16 devices in a mesh: dp: 2 (over y, z), sp: 8 (over x, core).
Axes of the slice: x: 4, y: 2, z: 1, core: 2. Of those that a mesh axis runs over, the one named last changes fastest.
The devices are a block of a 4x4x8 slice.
Arguments:
- tokens: bfloat16 [128, 4096], P('dp'), parts along dimension 0
- positions: int32 [128], P('dp'), parts along dimension 0
- k_cache: bfloat16 [128, 512, 8, 128], P('dp', 'sp'), parts along dimension 0
- v_cache: bfloat16 [128, 512, 8, 128], P('dp', 'sp'), parts along dimension 0
- w_q: bfloat16 [4096, 4096], replicated
- w_k: bfloat16 [4096, 1024], replicated
- w_v: bfloat16 [4096, 1024], replicated
- w_o: bfloat16 [4096, 4096], replicated
- attn_norm: bfloat16 [4096], replicated
- q_norm: bfloat16 [128], replicated
- k_norm: bfloat16 [128], replicated
Outputs:
- output 1: bfloat16 [128, 4096], P('dp'), parts along dimension 0
- output 2: bfloat16 [128, 512, 8, 128], P('dp', 'sp'), parts along dimension 0
- output 3: bfloat16 [128, 512, 8, 128], P('dp', 'sp'), parts along dimension 0
- output 4: bfloat16 [128, 2, 8, 128], P('dp'), parts along dimension 0
There are 2 independent parts. The reference program is written for one: setup_inputs(seed, part) draws one part's arguments, and reference() takes and returns one part's arrays. A program takes and returns all parts, laid end to end along the dimension named above; an argument that names none is the same for every part.
All inputs are finite; a program needn't handle non-finite values.
Results may differ from the reference program's by a relative error of at most 0.00658311.
Values sent between devices are 32-bit elements.
A program may use at most 768 MiB of HBM per device.

```python
import jax
import jax.numpy as jnp
from jax import lax

NUM_SEQS = 64
MODEL_DIM = 4096
Q_HEADS = 32
KV_HEADS = 8
HEAD_DIM = 128
CACHE_LEN = 512

Q_PER_KV = Q_HEADS // KV_HEADS
NORM_EPS = 1e-6
ROPE_THETA = 1000000.0
NEG_FILL = -1e30


def setup_inputs(seed: int = 0, part: int = 0) -> dict:
    part_keys = jax.random.split(jax.random.fold_in(jax.random.key(seed), part), 5)
    shared = jax.random.split(jax.random.key(seed + 1), 7)
    cache_shape = (NUM_SEQS, CACHE_LEN, KV_HEADS, HEAD_DIM)
    tokens = jax.random.normal(part_keys[0], (NUM_SEQS, MODEL_DIM), jnp.float32)
    pos_draw = jax.random.randint(part_keys[1], (NUM_SEQS,), CACHE_LEN // 4, CACHE_LEN, dtype=jnp.int32)
    positions = pos_draw.at[0].set(CACHE_LEN - 1).at[1].set(CACHE_LEN // 4)
    k_cache = jax.random.normal(part_keys[2], cache_shape, jnp.float32)
    coarse = jax.random.normal(part_keys[3], (NUM_SEQS, 16, KV_HEADS, HEAD_DIM), jnp.float32)
    v_noise = jax.random.normal(part_keys[4], cache_shape, jnp.float32)
    v_cache = 1.5 * jnp.repeat(coarse, CACHE_LEN // 16, axis=1) + 0.5 * v_noise
    w_q = jax.random.normal(shared[0], (MODEL_DIM, Q_HEADS * HEAD_DIM), jnp.float32) * MODEL_DIM ** -0.5
    w_k = jax.random.normal(shared[1], (MODEL_DIM, KV_HEADS * HEAD_DIM), jnp.float32) * MODEL_DIM ** -0.5
    w_v = jax.random.normal(shared[2], (MODEL_DIM, KV_HEADS * HEAD_DIM), jnp.float32) * MODEL_DIM ** -0.5
    w_o = jax.random.normal(shared[3], (Q_HEADS * HEAD_DIM, MODEL_DIM), jnp.float32) * (Q_HEADS * HEAD_DIM) ** -0.5
    attn_norm = jax.random.uniform(shared[4], (MODEL_DIM,), jnp.float32, 0.5, 1.5)
    q_norm = jax.random.uniform(shared[5], (HEAD_DIM,), jnp.float32, 0.5, 2.0)
    k_norm = jax.random.uniform(shared[6], (HEAD_DIM,), jnp.float32, 0.5, 2.0)
    return {
        'tokens': tokens.astype(jnp.bfloat16),
        'positions': positions,
        'k_cache': k_cache.astype(jnp.bfloat16),
        'v_cache': v_cache.astype(jnp.bfloat16),
        'w_q': w_q.astype(jnp.bfloat16),
        'w_k': w_k.astype(jnp.bfloat16),
        'w_v': w_v.astype(jnp.bfloat16),
        'w_o': w_o.astype(jnp.bfloat16),
        'attn_norm': attn_norm.astype(jnp.bfloat16),
        'q_norm': q_norm.astype(jnp.bfloat16),
        'k_norm': k_norm.astype(jnp.bfloat16),
    }


def rms_scale(values, gain):
    return values * lax.rsqrt(jnp.mean(values * values, axis=-1, keepdims=True) + NORM_EPS) * gain.astype(jnp.float32)


def rope_table(positions):
    inv_freq = ROPE_THETA ** (-jnp.arange(HEAD_DIM // 2, dtype=jnp.float32) * 2.0 / HEAD_DIM)
    angles = positions.astype(jnp.float32)[:, None] * inv_freq[None, :]
    return jnp.cos(angles)[:, None, :], jnp.sin(angles)[:, None, :]


def norm_rope(proj, gain, cos_table, sin_table):
    normed = rms_scale(proj.astype(jnp.float32), gain)
    first_half = normed[..., :HEAD_DIM // 2]
    second_half = normed[..., HEAD_DIM // 2:]
    rotated = jnp.concatenate([first_half * cos_table - second_half * sin_table, second_half * cos_table + first_half * sin_table], axis=-1)
    return rotated.astype(jnp.bfloat16)


def reference(tokens, positions, k_cache, v_cache, w_q, w_k, w_v, w_o, attn_norm, q_norm, k_norm):
    tokens_f = tokens.astype(jnp.float32)
    hidden = rms_scale(tokens_f, attn_norm).astype(jnp.bfloat16)
    q_proj = jnp.dot(hidden, w_q, preferred_element_type=jnp.float32).astype(jnp.bfloat16).reshape(NUM_SEQS, Q_HEADS, HEAD_DIM)
    k_proj = jnp.dot(hidden, w_k, preferred_element_type=jnp.float32).astype(jnp.bfloat16).reshape(NUM_SEQS, KV_HEADS, HEAD_DIM)
    v_new = jnp.dot(hidden, w_v, preferred_element_type=jnp.float32).astype(jnp.bfloat16).reshape(NUM_SEQS, KV_HEADS, HEAD_DIM)
    cos_table, sin_table = rope_table(positions)
    q_rot = norm_rope(q_proj, q_norm, cos_table, sin_table)
    k_rot = norm_rope(k_proj, k_norm, cos_table, sin_table)
    slot_ids = jnp.arange(CACHE_LEN)
    write_mask = (slot_ids[None, :] == positions[:, None])[:, :, None, None]
    k_out = jnp.where(write_mask, k_rot[:, None], k_cache)
    v_out = jnp.where(write_mask, v_new[:, None], v_cache)
    score_scale = HEAD_DIM ** -0.5

    def one_seq(items):
        q_one, k_one, v_one, pos_one = items
        q_grp = q_one.reshape(KV_HEADS, Q_PER_KV, HEAD_DIM).astype(jnp.float32)
        scores = jnp.einsum('kgd,tkd->kgt', q_grp, k_one.astype(jnp.float32)) * score_scale
        live_mask = (slot_ids <= pos_one)[None, None, :]
        global_peak = jnp.max(jnp.where(live_mask, scores, NEG_FILL), axis=-1, keepdims=True)
        weights = jnp.where(live_mask, jnp.exp(scores - global_peak), 0.0)
        total_sum = jnp.sum(weights, axis=-1, keepdims=True)
        mixed = jnp.einsum('kgt,tkd->kgd', weights.astype(jnp.bfloat16).astype(jnp.float32), v_one.astype(jnp.float32))
        return (mixed / total_sum).astype(jnp.bfloat16).reshape(Q_HEADS * HEAD_DIM)

    attn_out = lax.map(one_seq, (q_rot, k_out, v_out, positions))
    block_out = (tokens_f + jnp.dot(attn_out, w_o, preferred_element_type=jnp.float32)).astype(jnp.bfloat16)
    new_kv = jnp.stack([k_rot, v_new], axis=1)
    return (block_out, k_out, v_out, new_kv)
```

```python
import functools

import jax
import jax.numpy as jnp
from jax import lax
from jax.experimental import pallas as pl
from jax.experimental.pallas import tpu as pltpu
from jax.sharding import PartitionSpec as P

NORM_EPS = 1e-6
ROPE_THETA = 1000000.0
NEG_FILL = -1e30
MESH = pl.DeviceIdType.MESH
W_COLS = 512
W_SLOTS = 5
STAT_ROWS = 8


def rope_table(positions, head_dim):
    inv_freq = ROPE_THETA ** (-jnp.arange(head_dim // 2, dtype=jnp.float32) * 2.0 / head_dim)
    angles = positions.astype(jnp.float32)[:, None] * inv_freq[None, :]
    cos, sin = jnp.cos(angles), jnp.sin(angles)
    return jnp.concatenate([cos, cos], axis=-1), jnp.concatenate([-sin, sin], axis=-1)


def norm_rope(proj, gain, cos_full, sin_full):
    values = proj.astype(jnp.bfloat16).astype(jnp.float32)
    scale = lax.rsqrt(jnp.mean(values * values, axis=-1, keepdims=True) + NORM_EPS)
    normed = values * scale * gain
    turned = pltpu.roll(normed, normed.shape[-1] // 2, 1)
    return (normed * cos_full + turned * sin_full).astype(jnp.bfloat16).astype(jnp.float32)


def local_kernel(pos_ref, tok_ref, cos_ref, sin_ref, an_ref, qn_ref, kn_ref, wq_ref, wk_ref, wv_ref, kc_ref, vc_ref,
                 ko_ref, vo_ref, new_ref, part_ref,
                 hid, wbuf, kbuf, vbuf, qf, kf, vf, mstat, lstat, wsem, ksem, vsem, kosem, vosem):
    seqs, model = tok_ref.shape
    head_dim = qn_ref.shape[-1]
    slots, kv_heads = kbuf.shape[1], kbuf.shape[2]
    groups = ksem.shape[0]
    per_group = seqs // groups
    q_heads = wq_ref.shape[1] // head_dim
    start = lax.axis_index('sp') * slots
    n_k = wk_ref.shape[1] // W_COLS
    n_q = wq_ref.shape[1] // W_COLS
    n_all = 2 * n_k + n_q
    heads_per = W_COLS // head_dim

    def w_copy(ref, col, n):
        slot = n % W_SLOTS if isinstance(n, int) else lax.rem(n, W_SLOTS)
        off = col * W_COLS if isinstance(col, int) else pl.multiple_of(col * W_COLS, W_COLS)
        return pltpu.make_async_copy(ref.at[:, pl.ds(off, W_COLS)], wbuf.at[slot], wsem.at[slot])

    def w_start(n):
        if n < n_k:
            w_copy(wk_ref, n, n).start()
        elif n < 2 * n_k:
            w_copy(wv_ref, n - n_k, n).start()
        else:
            w_copy(wq_ref, n - 2 * n_k, n).start()

    def cache_in(ref, buf, sem, g):
        rows = pl.ds(g * per_group, per_group)
        return pltpu.make_async_copy(ref.at[rows], buf.at[rows], sem.at[g])

    for n in range(W_SLOTS):
        w_start(n)

    blk = 512
    total = jnp.zeros((seqs, 1), jnp.float32)
    for i in range(model // blk):
        xf = tok_ref[:, i * blk:(i + 1) * blk].astype(jnp.float32)
        total = total + jnp.sum(xf * xf, axis=-1, keepdims=True)
    inv = lax.rsqrt(total / model + NORM_EPS)
    for i in range(model // blk):
        xf = tok_ref[:, i * blk:(i + 1) * blk].astype(jnp.float32)
        gain = an_ref[:, i * blk:(i + 1) * blk].astype(jnp.float32)
        hid[:, i * blk:(i + 1) * blk] = (xf * inv * gain).astype(jnp.bfloat16)

    cos_full, sin_full = cos_ref[...], sin_ref[...]

    def project(n):
        slot = n % W_SLOTS if isinstance(n, int) else lax.rem(n, W_SLOTS)
        w_copy(wq_ref, 0, n).wait()
        return jnp.dot(hid[...], wbuf[slot], preferred_element_type=jnp.float32)

    k_gain = kn_ref[...].astype(jnp.float32)
    q_gain = qn_ref[...].astype(jnp.float32)
    for n in range(2 * n_k):
        y = project(n)
        if n + W_SLOTS < n_all:
            w_start(n + W_SLOTS)
        for hh in range(heads_per):
            piece = y[:, hh * head_dim:(hh + 1) * head_dim]
            if n < n_k:
                row = (n * heads_per + hh) * seqs
                kf[row:row + seqs, :] = norm_rope(piece, k_gain, cos_full, sin_full)
            else:
                row = ((n - n_k) * heads_per + hh) * seqs
                vf[row:row + seqs, :] = piece.astype(jnp.bfloat16).astype(jnp.float32)

    def q_step(i, carry):
        n = i + 2 * n_k
        y = project(n)

        @pl.when(n + W_SLOTS < n_all)
        def _():
            w_copy(wq_ref, i + W_SLOTS, n + W_SLOTS).start()

        @pl.when(n + W_SLOTS >= n_all)
        def _():
            g = n + W_SLOTS - n_all
            cache_in(kc_ref, kbuf, ksem, g).start()
            cache_in(vc_ref, vbuf, vsem, g).start()

        for hh in range(heads_per):
            row = pl.multiple_of(i * (heads_per * seqs) + hh * seqs, seqs)
            qf[pl.ds(row, seqs), :] = norm_rope(y[:, hh * head_dim:(hh + 1) * head_dim], q_gain, cos_full, sin_full)
        return carry

    lax.fori_loop(0, n_q, q_step, 0)
    for g in range(W_SLOTS, groups):
        cache_in(kc_ref, kbuf, ksem, g).start()
        cache_in(vc_ref, vbuf, vsem, g).start()

    half = q_heads // 2
    cols = slots * kv_heads
    row_id = lax.broadcasted_iota(jnp.int32, (q_heads, cols), 0)
    col_id = lax.broadcasted_iota(jnp.int32, (q_heads, cols), 1)
    q_per_kv = q_heads // kv_heads
    head_ok = ((row_id % half) * 2) // q_per_kv == col_id % kv_heads
    slot_key = jnp.where(head_ok, col_id // kv_heads, slots * 1024)
    lane = lax.broadcasted_iota(jnp.int32, (q_heads, 128), 1)
    score_scale = head_dim ** -0.5
    part_rows = part_ref.shape[1]
    mstat[...] = jnp.zeros_like(mstat)
    lstat[...] = jnp.zeros_like(lstat)

    def group_step(g, carry):
        cache_in(kc_ref, kbuf, ksem, g).wait()
        cache_in(vc_ref, vbuf, vsem, g).wait()
        m_acc, l_acc = mstat[...], lstat[...]
        for bb in range(per_group):
            b = g * per_group + bb
            local = pos_ref[b] - start
            k_new = kf[pl.ds(b, kv_heads, stride=seqs), :].astype(jnp.bfloat16)
            v_new = vf[pl.ds(b, kv_heads, stride=seqs), :].astype(jnp.bfloat16)
            new_ref[b, 0] = k_new
            new_ref[b, 1] = v_new

            @pl.when((local >= 0) & (local < slots))
            def _():
                kbuf[b, local] = k_new
                vbuf[b, local] = v_new

            q_even = qf[pl.ds(b, half, stride=2 * seqs), :]
            q_odd = qf[pl.ds(b + seqs, half, stride=2 * seqs), :]
            q_b = jnp.concatenate([q_even, q_odd], axis=0).astype(jnp.bfloat16)
            k_b = kbuf[b].reshape(cols, head_dim)
            v_b = vbuf[b].reshape(cols, head_dim)
            s = lax.dot_general(q_b, k_b, (((1,), (1,)), ((), ())), preferred_element_type=jnp.float32) * score_scale
            live = slot_key <= local
            s = jnp.where(live, s, NEG_FILL)
            m = jnp.max(s, axis=-1, keepdims=True)
            e = jnp.where(live, jnp.exp(s - m), 0.0)
            l = jnp.sum(e, axis=-1, keepdims=True)
            o = jnp.dot(e.astype(jnp.bfloat16), v_b, preferred_element_type=jnp.float32)
            for par in range(2):
                for i in range(half):
                    part_ref[i, pl.ds(b + par * seqs, 1), :] = o[par * half + i:par * half + i + 1, :]
            m_acc = jnp.where(lane == b, m, m_acc)
            l_acc = jnp.where(lane == b, l, l_acc)
        mstat[...] = m_acc
        lstat[...] = l_acc
        rows = pl.ds(g * per_group, per_group)
        pltpu.make_async_copy(kbuf.at[rows], ko_ref.at[rows], kosem.at[g]).start()
        pltpu.make_async_copy(vbuf.at[rows], vo_ref.at[rows], vosem.at[g]).start()
        return carry

    lax.fori_loop(0, groups, group_step, 0)

    for i in range(half):
        base = 2 * seqs
        part_ref[i, base:base + 1, :] = mstat[i:i + 1, :]
        part_ref[i, base + 1:base + 2, :] = mstat[half + i:half + i + 1, :]
        part_ref[i, base + 2:base + 3, :] = lstat[i:i + 1, :]
        part_ref[i, base + 3:base + 4, :] = lstat[half + i:half + i + 1, :]
        part_ref[i, base + 4:base + 8, :] = jnp.zeros((4, 128), jnp.float32)
    for g in range(groups):
        rows = pl.ds(g * per_group, per_group)
        pltpu.make_async_copy(kbuf.at[rows], ko_ref.at[rows], kosem.at[g]).wait()
        pltpu.make_async_copy(vbuf.at[rows], vo_ref.at[rows], vosem.at[g]).wait()


def local_stage(tokens, positions, cos_t, sin_t, k_cache, v_cache, w_q, w_k, w_v, attn_norm, q_norm, k_norm):
    seqs, model = tokens.shape
    slots, kv_heads, head_dim = k_cache.shape[1:]
    q_heads = w_q.shape[1] // head_dim
    groups = 8
    vmem = pl.BlockSpec(memory_space=pltpu.VMEM)
    anyspec = pl.BlockSpec(memory_space=pl.ANY)
    part_shape = (q_heads // 2, 2 * seqs + STAT_ROWS, head_dim)
    return pl.pallas_call(
        local_kernel,
        name='local_stage',
        out_shape=(
            jax.ShapeDtypeStruct(k_cache.shape, k_cache.dtype),
            jax.ShapeDtypeStruct(v_cache.shape, v_cache.dtype),
            jax.ShapeDtypeStruct((seqs, 2, kv_heads, head_dim), jnp.bfloat16),
            jax.ShapeDtypeStruct(part_shape, jnp.float32),
        ),
        in_specs=[pl.BlockSpec(memory_space=pltpu.SMEM)] + [vmem] * 6 + [anyspec] * 5,
        out_specs=(anyspec, anyspec, vmem, vmem),
        scratch_shapes=[
            pltpu.VMEM((seqs, model), jnp.bfloat16),
            pltpu.VMEM((W_SLOTS, model, W_COLS), jnp.bfloat16),
            pltpu.VMEM(k_cache.shape, k_cache.dtype),
            pltpu.VMEM(v_cache.shape, v_cache.dtype),
            pltpu.VMEM((q_heads * seqs, head_dim), jnp.float32),
            pltpu.VMEM((kv_heads * seqs, head_dim), jnp.float32),
            pltpu.VMEM((kv_heads * seqs, head_dim), jnp.float32),
            pltpu.VMEM((q_heads, 128), jnp.float32),
            pltpu.VMEM((q_heads, 128), jnp.float32),
            pltpu.SemaphoreType.DMA((W_SLOTS,)),
            pltpu.SemaphoreType.DMA((groups,)),
            pltpu.SemaphoreType.DMA((groups,)),
            pltpu.SemaphoreType.DMA((groups,)),
            pltpu.SemaphoreType.DMA((groups,)),
        ],
        compiler_params=pltpu.CompilerParams(vmem_limit_bytes=56 * 1024 * 1024),
    )(positions, tokens, cos_t, sin_t, attn_norm[None, :], q_norm[None, :], k_norm[None, :], w_q, w_k, w_v, k_cache, v_cache)


def combine(pieces, seqs, rows_out, final=False):
    stats = [jnp.transpose(s, (1, 0))[:seqs] for _, s in pieces]
    peak = functools.reduce(jnp.maximum, [t[:, 0:2] for t in stats])
    factors = [jnp.exp(t[:, 0:2] - peak) for t in stats]
    total = functools.reduce(jnp.add, [f * t[:, 2:4] for f, t in zip(factors, stats)])
    outs = []
    for hh in range(2):
        acc = None
        for (o, _), f in zip(pieces, factors):
            term = o[hh * seqs:(hh + 1) * seqs] * f[:, hh:hh + 1]
            acc = term if acc is None else acc + term
        if final:
            acc = acc / total[:, hh:hh + 1]
        outs.append(acc)
    if final:
        return outs, None
    both = jnp.concatenate([peak, total, jnp.zeros((seqs, 4), jnp.float32)], axis=1)
    both = jnp.concatenate([both, jnp.zeros((128 - seqs, 8), jnp.float32)], axis=0)
    return outs, jnp.transpose(both, (1, 0))


def tail_kernel(part_ref, wo_ref, tok_ref, out_ref, mine, pin, acc, rel, fin, att, wov, res,
                psem, wsem, s0, r0, s1, r1, s2, r2, s3, r3, s4, r4):
    seqs, model = tok_ref.shape
    me = lax.axis_index('sp')
    n = lax.axis_size('sp')
    chips = n // 2
    core, chip = lax.rem(me, 2), me // 2
    c_right, c_left, c_opp = lax.rem(chip + 1, chips), lax.rem(chip + chips - 1, chips), lax.rem(chip + 2, chips)
    partner = chip * 2 + 1 - core
    right, left = c_right * 2 + core, c_left * 2 + core
    body = 2 * seqs
    k_rows = wov.shape[1]

    load = pltpu.make_async_copy(part_ref, mine, psem)
    load.start()

    def wo_copy(k):
        return pltpu.make_async_copy(wo_ref.at[pl.ds(pl.multiple_of(k * k_rows, k_rows), k_rows)], wov.at[k], wsem.at[k])

    barrier = pltpu.get_barrier_semaphore()
    for peer in (partner, right, left):
        pl.semaphore_signal(barrier, inc=1, device_id={'sp': peer}, device_id_type=MESH)
    for k in range(wov.shape[0]):
        wo_copy(k).start()
    load.wait()
    pl.semaphore_wait(barrier, 3)

    def send(src, dst, ss, rs, peer):
        copy = pltpu.make_async_remote_copy(src_ref=src, dst_ref=dst, send_sem=ss, recv_sem=rs,
                                            device_id={'sp': peer}, device_id_type=MESH)
        copy.start()
        return copy

    order = (c_opp, c_right, c_left, chip)
    halves = 2 * chips
    sends = []
    pair = []
    for i, c in enumerate(order):
        copy = send(mine.at[pl.ds((1 - core) * halves + 2 * c, 2)], pin.at[i], s0.at[i], r0.at[i], partner)
        pair.append(copy)

    def put(dst, outs, stat):
        for hh in range(2):
            dst[hh * seqs:(hh + 1) * seqs, :] = outs[hh]
        dst[body:body + STAT_ROWS, :] = stat

    def read(ref):
        return ref[0:body, :], ref[body:body + STAT_ROWS, :]

    def merge_pair(i):
        pair[i].wait_recv()
        for h in range(2):
            own = mine.at[core * halves + 2 * order[i] + h]
            put(acc.at[i, h], *combine([read(own), read(pin.at[i, h])], seqs, body))

    merge_pair(0)
    sends.append(send(acc.at[0, 1], rel.at[1], s1.at[1], r1.at[1], right))
    sends.append(send(acc.at[0, 0], rel.at[0], s1.at[0], r1.at[0], left))
    relay_b, relay_a = sends[0], sends[1]
    merge_pair(1)
    fin_left_a = send(acc.at[1, 0], fin.at[0, 0], s2.at[0], r2.at[0], right)
    merge_pair(2)
    fin_right_b = send(acc.at[2, 1], fin.at[1, 1], s2.at[1], r2.at[1], left)
    merge_pair(3)
    relay_b.wait_recv()
    put(fin.at[2, 1], *combine([read(acc.at[1, 1]), read(rel.at[1])], seqs, body))
    fin_left_b = send(fin.at[2, 1], fin.at[0, 1], s2.at[2], r2.at[2], right)
    relay_a.wait_recv()
    put(fin.at[2, 0], *combine([read(acc.at[2, 0]), read(rel.at[0])], seqs, body))
    fin_right_a = send(fin.at[2, 0], fin.at[1, 0], s2.at[3], r2.at[3], left)

    mine_k = core * chips + chip
    for h, (from_left, from_right) in ((0, (fin_left_a, fin_right_a)), (1, (fin_left_b, fin_right_b))):
        from_left.wait_recv()
        from_right.wait_recv()
        outs, _ = combine([read(acc.at[3, h]), read(fin.at[0, h]), read(fin.at[1, h])], seqs, body, final=True)
        for hh in range(2):
            att[mine_k, h, hh * seqs:(hh + 1) * seqs, :] = outs[hh].astype(jnp.bfloat16).astype(jnp.float32)

    k_left, k_right, k_opp = core * chips + c_left, core * chips + c_right, core * chips + c_opp
    o_core = 1 - core
    to_right_b = send(att.at[mine_k, 1], att.at[mine_k, 1], s3.at[0], r3.at[0], right)
    to_left_a = send(att.at[mine_k, 0], att.at[mine_k, 0], s3.at[1], r3.at[1], left)
    to_right_a = send(att.at[mine_k, 0], att.at[mine_k, 0], s3.at[2], r3.at[2], right)
    to_left_b = send(att.at[mine_k, 1], att.at[mine_k, 1], s3.at[3], r3.at[3], left)
    to_partner = send(att.at[mine_k], att.at[mine_k], s3.at[4], r3.at[4], partner)

    cols = 512

    def multiply(k, first=False):
        wo_copy(k).wait()
        lhs = jnp.concatenate([att[k, h, hh * seqs:(hh + 1) * seqs, :] for h in range(2) for hh in range(2)], axis=1)
        lhs = lhs.astype(jnp.bfloat16)

        def tile(i, carry):
            off = pl.ds(pl.multiple_of(i * cols, cols), cols)
            y = jnp.dot(lhs, wov[k, :, off], preferred_element_type=jnp.float32)
            res[:, off] = y if first else res[:, off] + y
            return carry

        lax.fori_loop(0, model // cols, tile, 0)

    multiply(mine_k, first=True)
    to_right_b.wait_recv()
    fwd_right = send(att.at[k_left, 1], att.at[k_left, 1], s4.at[0], r4.at[0], right)
    p1 = send(att.at[k_left, 1], att.at[k_left, 1], s4.at[2], r4.at[2], partner)
    to_left_a.wait_recv()
    fwd_left = send(att.at[k_right, 0], att.at[k_right, 0], s4.at[1], r4.at[1], left)
    p2 = send(att.at[k_right, 0], att.at[k_right, 0], s4.at[3], r4.at[3], partner)
    to_partner.wait_recv()
    multiply(o_core * chips + chip)
    to_right_a.wait_recv()
    p3 = send(att.at[k_left, 0], att.at[k_left, 0], s4.at[4], r4.at[4], partner)
    to_left_b.wait_recv()
    p4 = send(att.at[k_right, 1], att.at[k_right, 1], s4.at[5], r4.at[5], partner)
    multiply(k_left)
    multiply(k_right)
    p1.wait_recv()
    p3.wait_recv()
    multiply(o_core * chips + c_left)
    p2.wait_recv()
    p4.wait_recv()
    multiply(o_core * chips + c_right)
    fwd_right.wait_recv()
    p5 = send(att.at[k_opp, 1], att.at[k_opp, 1], s4.at[6], r4.at[6], partner)
    fwd_left.wait_recv()
    p6 = send(att.at[k_opp, 0], att.at[k_opp, 0], s4.at[7], r4.at[7], partner)
    multiply(k_opp)
    p5.wait_recv()
    p6.wait_recv()
    multiply(o_core * chips + c_opp)
    out_ref[...] = (tok_ref[...].astype(jnp.float32) + res[...]).astype(jnp.bfloat16)
    for copy in pair + sends + [fin_left_a, fin_right_b, fin_left_b, fin_right_a, to_right_b, to_left_a, to_right_a,
                                to_left_b, to_partner, fwd_right, fwd_left, p1, p2, p3, p4, p5, p6]:
        copy.wait_send()


def tail_stage(part, w_o, tokens, group):
    seqs, model = tokens.shape
    halves, rows, head_dim = part.shape
    chips = group // 2
    vmem = pl.BlockSpec(memory_space=pltpu.VMEM)
    anyspec = pl.BlockSpec(memory_space=pl.ANY)
    dma = pltpu.SemaphoreType.DMA
    return pl.pallas_call(
        tail_kernel,
        name='tail_stage',
        out_shape=jax.ShapeDtypeStruct((seqs, model), jnp.bfloat16),
        in_specs=[anyspec, anyspec, vmem],
        out_specs=vmem,
        scratch_shapes=[
            pltpu.VMEM(part.shape, jnp.float32),
            pltpu.VMEM((chips, 2, rows, head_dim), jnp.float32),
            pltpu.VMEM((chips, 2, rows, head_dim), jnp.float32),
            pltpu.VMEM((2, rows, head_dim), jnp.float32),
            pltpu.VMEM((3, 2, rows, head_dim), jnp.float32),
            pltpu.VMEM((group, 2, 2 * seqs, head_dim), jnp.float32),
            pltpu.VMEM((group, w_o.shape[0] // group, model), jnp.bfloat16),
            pltpu.VMEM((seqs, model), jnp.float32),
            dma, dma((group,)),
            dma((chips,)), dma((chips,)), dma((2,)), dma((2,)), dma((4,)), dma((4,)), dma((5,)), dma((5,)), dma((8,)), dma((8,)),
        ],
        compiler_params=pltpu.CompilerParams(collective_id=0, has_side_effects=True, vmem_limit_bytes=56 * 1024 * 1024),
    )(part, w_o, tokens)


def solution(mesh):
    cache_spec = P('dp', 'sp', None, None)
    group = mesh.shape['sp']

    def device_step(tokens, positions, k_cache, v_cache, w_q, w_k, w_v, w_o, attn_norm, q_norm, k_norm):
        cos_t, sin_t = rope_table(positions, q_norm.shape[0])
        k_upd, v_upd, new_kv, part = local_stage(tokens, positions, cos_t, sin_t, k_cache, v_cache, w_q, w_k, w_v, attn_norm, q_norm, k_norm)
        block_out = tail_stage(part, w_o, tokens, group)
        return block_out, k_upd, v_upd, new_kv

    return jax.shard_map(device_step, mesh=mesh, in_specs=(P('dp', None), P('dp'), cache_spec, cache_spec, P(), P(), P(), P(), P(), P(), P()), out_specs=(P('dp', None), cache_spec, cache_spec, P('dp', None, None, None)), check_vma=False)
```

```python
import functools

import jax
import jax.numpy as jnp
import numpy as np
from jax import lax
from jax.experimental import pallas as pl
from jax.experimental.pallas import tpu as pltpu
from jax.sharding import PartitionSpec as P

NORM_EPS = 1e-6
ROPE_THETA = 1000000.0
NEG_FILL = -1e30
MESH = pl.DeviceIdType.MESH
W_ROWS = 512
W_SLOTS = 3
STAT_ROWS = 8


def rope_frequencies(head_dim):
    inv_freq = ROPE_THETA ** (-np.arange(head_dim // 2, dtype=np.float64) * 2.0 / head_dim)
    return np.concatenate([inv_freq, inv_freq])[None, :].astype(np.float32)


def norm_rope(proj, gain, cos_full, sin_full):
    values = proj.astype(jnp.bfloat16).astype(jnp.float32)
    scale = lax.rsqrt(jnp.mean(values * values, axis=-1, keepdims=True) + NORM_EPS)
    normed = values * scale * gain
    turned = pltpu.roll(normed, normed.shape[-1] // 2, 1)
    return (normed * cos_full + turned * sin_full).astype(jnp.bfloat16).astype(jnp.float32)


def local_kernel(pos_in, tok_in, freq_in, an_in, qn_in, kn_in, wq_ref, wk_ref, wv_ref, kc_ref, vc_ref,
                 ko_ref, vo_ref, new_out, part_ref,
                 pos_ref, tok_ref, freq_ref, an_ref, qn_ref, kn_ref, new_ref, insem, newsem, hid, wqb, wkb, wvb, yq, yk, yv, cosb, sinb, kbuf, vbuf, qf, kf, vf, mstat, lstat, wsem, ksem, vsem, kosem, vosem):
    seqs, model = tok_ref.shape
    head_dim = qn_ref.shape[-1]
    slots, kv_heads = kbuf.shape[1], kbuf.shape[2]
    groups = ksem.shape[0]
    per_group = seqs // groups
    q_heads = wq_ref.shape[1] // head_dim
    start = lax.axis_index('sp') * slots
    steps = model // W_ROWS
    weights = ((wk_ref, wkb, yk), (wv_ref, wvb, yv), (wq_ref, wqb, yq))

    def w_copies(i):
        slot = lax.rem(i, W_SLOTS)
        rows = pl.ds(pl.multiple_of(i * W_ROWS, W_ROWS), W_ROWS)
        return [pltpu.make_async_copy(ref.at[rows], buf.at[slot], wsem.at[j, slot]) for j, (ref, buf, _) in enumerate(weights)]

    def cache_in(ref, buf, sem, g):
        rows = pl.ds(g * per_group, per_group)
        return pltpu.make_async_copy(ref.at[rows], buf.at[rows], sem.at[g])

    smalls = [pltpu.make_async_copy(src, dst, insem.at[j]) for j, (src, dst) in enumerate((
        (tok_in, tok_ref), (pos_in, pos_ref), (freq_in, freq_ref), (an_in, an_ref), (qn_in, qn_ref), (kn_in, kn_ref)))]
    for copy in smalls:
        copy.start()
    for n in range(W_SLOTS):
        for copy in w_copies(jnp.int32(n)):
            copy.start()
    for copy in smalls:
        copy.wait()

    lanes = an_ref.shape[1]
    total = jnp.zeros((seqs, 1), jnp.float32)
    for i in range(model // lanes):
        xf = tok_ref[:, i * lanes:(i + 1) * lanes].astype(jnp.float32)
        total = total + jnp.sum(xf * xf, axis=-1, keepdims=True)
    inv = lax.rsqrt(total / model + NORM_EPS)
    per_step = W_ROWS // lanes
    for i in range(model // lanes):
        xf = tok_ref[:, i * lanes:(i + 1) * lanes].astype(jnp.float32)
        gain = an_ref[i:i + 1, :].astype(jnp.float32)
        hid[i // per_step, :, (i % per_step) * lanes:(i % per_step + 1) * lanes] = (xf * inv * gain).astype(jnp.bfloat16)

    for b in range(seqs):
        cosb[b:b + 1, :] = jnp.full((1, head_dim), pos_ref[b], jnp.int32).astype(jnp.float32)
    angles = cosb[...] * freq_ref[...]
    sign = jnp.where(lax.broadcasted_iota(jnp.int32, angles.shape, 1) < head_dim // 2, -1.0, 1.0)
    sinb[...] = jnp.sin(angles) * sign
    cosb[...] = jnp.cos(angles)
    for y in (yq, yk, yv):
        y[...] = jnp.zeros_like(y)

    def w_step(i, carry):
        slot = lax.rem(i, W_SLOTS)
        lhs = hid[i]
        for copy, (_, buf, y) in zip(w_copies(i), weights):
            copy.wait()
            y[...] += jnp.dot(lhs, buf[slot], preferred_element_type=jnp.float32)

        @pl.when(i + W_SLOTS < steps)
        def _():
            for copy in w_copies(i + W_SLOTS):
                copy.start()

        @pl.when(i + W_SLOTS >= steps)
        def _():
            g = i + W_SLOTS - steps
            cache_in(kc_ref, kbuf, ksem, g).start()
            cache_in(vc_ref, vbuf, vsem, g).start()

        return carry

    lax.fori_loop(0, steps, w_step, 0)
    for g in range(W_SLOTS, groups):
        cache_in(kc_ref, kbuf, ksem, g).start()
        cache_in(vc_ref, vbuf, vsem, g).start()

    cos_full, sin_full = cosb[...], sinb[...]
    k_gain = kn_ref[...].astype(jnp.float32)
    q_gain = qn_ref[...].astype(jnp.float32)
    for h in range(kv_heads):
        cols = slice(h * head_dim, (h + 1) * head_dim)
        rows = slice(h * seqs, (h + 1) * seqs)
        kf[rows, :] = norm_rope(yk[:, cols], k_gain, cos_full, sin_full)
        vf[rows, :] = yv[:, cols].astype(jnp.bfloat16).astype(jnp.float32)
    for h in range(q_heads):
        qf[h * seqs:(h + 1) * seqs, :] = norm_rope(yq[:, h * head_dim:(h + 1) * head_dim], q_gain, cos_full, sin_full)

    half = q_heads // 2
    cols = slots * kv_heads
    row_id = lax.broadcasted_iota(jnp.int32, (q_heads, cols), 0)
    col_id = lax.broadcasted_iota(jnp.int32, (q_heads, cols), 1)
    q_per_kv = q_heads // kv_heads
    head_ok = ((row_id % half) * 2) // q_per_kv == col_id % kv_heads
    slot_key = jnp.where(head_ok, col_id // kv_heads, slots * 1024)
    lane = lax.broadcasted_iota(jnp.int32, (q_heads, 128), 1)
    score_scale = head_dim ** -0.5
    part_rows = part_ref.shape[1]
    mstat[...] = jnp.zeros_like(mstat)
    lstat[...] = jnp.zeros_like(lstat)

    def group_step(g, carry):
        cache_in(kc_ref, kbuf, ksem, g).wait()
        cache_in(vc_ref, vbuf, vsem, g).wait()
        m_acc, l_acc = mstat[...], lstat[...]
        for bb in range(per_group):
            b = g * per_group + bb
            local = pos_ref[b] - start
            k_new = kf[pl.ds(b, kv_heads, stride=seqs), :].astype(jnp.bfloat16)
            v_new = vf[pl.ds(b, kv_heads, stride=seqs), :].astype(jnp.bfloat16)
            new_ref[b, 0] = k_new
            new_ref[b, 1] = v_new

            @pl.when((local >= 0) & (local < slots))
            def _():
                kbuf[b, local] = k_new
                vbuf[b, local] = v_new

            q_even = qf[pl.ds(b, half, stride=2 * seqs), :]
            q_odd = qf[pl.ds(b + seqs, half, stride=2 * seqs), :]
            q_b = jnp.concatenate([q_even, q_odd], axis=0).astype(jnp.bfloat16)
            k_b = kbuf[b].reshape(cols, head_dim)
            v_b = vbuf[b].reshape(cols, head_dim)
            s = lax.dot_general(q_b, k_b, (((1,), (1,)), ((), ())), preferred_element_type=jnp.float32) * score_scale
            live = slot_key <= local
            s = jnp.where(live, s, NEG_FILL)
            m = jnp.max(s, axis=-1, keepdims=True)
            e = jnp.where(live, jnp.exp(s - m), 0.0)
            l = jnp.sum(e, axis=-1, keepdims=True)
            o = jnp.dot(e.astype(jnp.bfloat16), v_b, preferred_element_type=jnp.float32)
            for par in range(2):
                for i in range(half):
                    part_ref[i, pl.ds(b + par * seqs, 1), :] = o[par * half + i:par * half + i + 1, :]
            m_acc = jnp.where(lane == b, m, m_acc)
            l_acc = jnp.where(lane == b, l, l_acc)
        mstat[...] = m_acc
        lstat[...] = l_acc
        rows = pl.ds(g * per_group, per_group)
        pltpu.make_async_copy(kbuf.at[rows], ko_ref.at[rows], kosem.at[g]).start()
        pltpu.make_async_copy(vbuf.at[rows], vo_ref.at[rows], vosem.at[g]).start()
        pltpu.make_async_copy(new_ref.at[rows], new_out.at[rows], newsem.at[g]).start()
        return carry

    lax.fori_loop(0, groups, group_step, 0)

    for i in range(half):
        base = 2 * seqs
        part_ref[i, base:base + 1, :] = mstat[i:i + 1, :]
        part_ref[i, base + 1:base + 2, :] = mstat[half + i:half + i + 1, :]
        part_ref[i, base + 2:base + 3, :] = lstat[i:i + 1, :]
        part_ref[i, base + 3:base + 4, :] = lstat[half + i:half + i + 1, :]
        part_ref[i, base + 4:base + 8, :] = jnp.zeros((4, 128), jnp.float32)
    for g in range(groups):
        rows = pl.ds(g * per_group, per_group)
        pltpu.make_async_copy(kbuf.at[rows], ko_ref.at[rows], kosem.at[g]).wait()
        pltpu.make_async_copy(vbuf.at[rows], vo_ref.at[rows], vosem.at[g]).wait()
        pltpu.make_async_copy(new_ref.at[rows], new_out.at[rows], newsem.at[g]).wait()


def in_hbm(*arrays):
    return [pltpu.with_memory_space_constraint(jnp.asarray(a), pltpu.HBM) for a in arrays]


def local_stage(tokens, positions, k_cache, v_cache, w_q, w_k, w_v, attn_norm, q_norm, k_norm):
    seqs, model = tokens.shape
    slots, kv_heads, head_dim = k_cache.shape[1:]
    q_heads = w_q.shape[1] // head_dim
    groups = 8
    vmem = pl.BlockSpec(memory_space=pltpu.VMEM)
    anyspec = pl.BlockSpec(memory_space=pl.ANY)
    hbm = pl.BlockSpec(memory_space=pltpu.HBM)
    part_shape = (q_heads // 2, 2 * seqs + STAT_ROWS, head_dim)
    return pl.pallas_call(
        local_kernel,
        name='local_stage',
        out_shape=(
            jax.ShapeDtypeStruct(k_cache.shape, k_cache.dtype),
            jax.ShapeDtypeStruct(v_cache.shape, v_cache.dtype),
            jax.ShapeDtypeStruct((seqs, 2, kv_heads, head_dim), jnp.bfloat16),
            pltpu.VMEM(part_shape, jnp.float32),
        ),
        in_specs=[hbm] * 11,
        out_specs=(anyspec, anyspec, anyspec, vmem),
        scratch_shapes=[
            pltpu.SMEM(positions.shape, jnp.int32),
            pltpu.VMEM(tokens.shape, tokens.dtype),
            pltpu.VMEM((1, head_dim), jnp.float32),
            pltpu.VMEM((model // 128, 128), attn_norm.dtype),
            pltpu.VMEM((1, head_dim), q_norm.dtype),
            pltpu.VMEM((1, head_dim), k_norm.dtype),
            pltpu.VMEM((seqs, 2, kv_heads, head_dim), jnp.bfloat16),
            pltpu.SemaphoreType.DMA((6,)),
            pltpu.SemaphoreType.DMA((groups,)),
            pltpu.VMEM((model // W_ROWS, seqs, W_ROWS), jnp.bfloat16),
            pltpu.VMEM((W_SLOTS, W_ROWS, w_q.shape[1]), jnp.bfloat16),
            pltpu.VMEM((W_SLOTS, W_ROWS, w_k.shape[1]), jnp.bfloat16),
            pltpu.VMEM((W_SLOTS, W_ROWS, w_v.shape[1]), jnp.bfloat16),
            pltpu.VMEM((seqs, w_q.shape[1]), jnp.float32),
            pltpu.VMEM((seqs, w_k.shape[1]), jnp.float32),
            pltpu.VMEM((seqs, w_v.shape[1]), jnp.float32),
            pltpu.VMEM((seqs, head_dim), jnp.float32),
            pltpu.VMEM((seqs, head_dim), jnp.float32),
            pltpu.VMEM(k_cache.shape, k_cache.dtype),
            pltpu.VMEM(v_cache.shape, v_cache.dtype),
            pltpu.VMEM((q_heads * seqs, head_dim), jnp.float32),
            pltpu.VMEM((kv_heads * seqs, head_dim), jnp.float32),
            pltpu.VMEM((kv_heads * seqs, head_dim), jnp.float32),
            pltpu.VMEM((q_heads, 128), jnp.float32),
            pltpu.VMEM((q_heads, 128), jnp.float32),
            pltpu.SemaphoreType.DMA((3, W_SLOTS)),
            pltpu.SemaphoreType.DMA((groups,)),
            pltpu.SemaphoreType.DMA((groups,)),
            pltpu.SemaphoreType.DMA((groups,)),
            pltpu.SemaphoreType.DMA((groups,)),
        ],
        compiler_params=pltpu.CompilerParams(vmem_limit_bytes=46 * 1024 * 1024),
    )(*in_hbm(positions, tokens, rope_frequencies(head_dim), attn_norm.reshape(-1, 128), q_norm[None, :], k_norm[None, :]), w_q, w_k, w_v, k_cache, v_cache)


def combine(pieces, seqs, rows_out, final=False):
    stats = [jnp.transpose(s, (1, 0))[:seqs] for _, s in pieces]
    peak = functools.reduce(jnp.maximum, [t[:, 0:2] for t in stats])
    factors = [jnp.exp(t[:, 0:2] - peak) for t in stats]
    total = functools.reduce(jnp.add, [f * t[:, 2:4] for f, t in zip(factors, stats)])
    outs = []
    for hh in range(2):
        acc = None
        for (o, _), f in zip(pieces, factors):
            term = o[hh * seqs:(hh + 1) * seqs] * f[:, hh:hh + 1]
            acc = term if acc is None else acc + term
        if final:
            acc = acc / total[:, hh:hh + 1]
        outs.append(acc)
    if final:
        return outs, None
    both = jnp.concatenate([peak, total, jnp.zeros((seqs, 4), jnp.float32)], axis=1)
    both = jnp.concatenate([both, jnp.zeros((128 - seqs, 8), jnp.float32)], axis=0)
    return outs, jnp.transpose(both, (1, 0))


def tail_kernel(mine, wo_ref, tok_in, out_ref, tok_ref, toksem, pin, acc, rel, fin, att, wov, res,
                wsem, s0, r0, s1, r1, s2, r2, s3, r3, s4, r4):
    seqs, model = tok_ref.shape
    tok_copy = pltpu.make_async_copy(tok_in, tok_ref, toksem)
    tok_copy.start()
    me = lax.axis_index('sp')
    n = lax.axis_size('sp')
    chips = n // 2
    core, chip = lax.rem(me, 2), me // 2
    c_right, c_left, c_opp = lax.rem(chip + 1, chips), lax.rem(chip + chips - 1, chips), lax.rem(chip + 2, chips)
    partner = chip * 2 + 1 - core
    right, left = c_right * 2 + core, c_left * 2 + core
    body = 2 * seqs
    k_rows = wov.shape[1]

    def wo_copy(k):
        return pltpu.make_async_copy(wo_ref.at[pl.ds(pl.multiple_of(k * k_rows, k_rows), k_rows)], wov.at[k], wsem.at[k])

    barrier = pltpu.get_barrier_semaphore()
    for peer in (partner, right, left):
        pl.semaphore_signal(barrier, inc=1, device_id={'sp': peer}, device_id_type=MESH)
    pl.semaphore_wait(barrier, 3)

    def send(src, dst, ss, rs, peer):
        copy = pltpu.make_async_remote_copy(src_ref=src, dst_ref=dst, send_sem=ss, recv_sem=rs,
                                            device_id={'sp': peer}, device_id_type=MESH)
        copy.start()
        return copy

    order = (c_opp, c_right, c_left, chip)
    halves = 2 * chips
    sends = []
    pair = []
    for i, c in enumerate(order):
        copy = send(mine.at[pl.ds((1 - core) * halves + 2 * c, 2)], pin.at[i], s0.at[i], r0.at[i], partner)
        pair.append(copy)

    for k in range(2):
        wo_copy(k).start()

    def put(dst, outs, stat):
        for hh in range(2):
            dst[hh * seqs:(hh + 1) * seqs, :] = outs[hh]
        dst[body:body + STAT_ROWS, :] = stat

    def read(ref):
        return ref[0:body, :], ref[body:body + STAT_ROWS, :]

    def merge_pair(i):
        pair[i].wait_recv()
        for h in range(2):
            own = mine.at[core * halves + 2 * order[i] + h]
            put(acc.at[i, h], *combine([read(own), read(pin.at[i, h])], seqs, body))

    merge_pair(0)
    sends.append(send(acc.at[0, 1], rel.at[1], s1.at[1], r1.at[1], right))
    sends.append(send(acc.at[0, 0], rel.at[0], s1.at[0], r1.at[0], left))
    relay_b, relay_a = sends[0], sends[1]
    for k in range(2, 4):
        wo_copy(k).start()
    merge_pair(1)
    fin_left_a = send(acc.at[1, 0], fin.at[0, 0], s2.at[0], r2.at[0], right)
    merge_pair(2)
    fin_right_b = send(acc.at[2, 1], fin.at[1, 1], s2.at[1], r2.at[1], left)
    merge_pair(3)
    for k in range(4, 8):
        wo_copy(k).start()
    relay_b.wait_recv()
    put(fin.at[2, 1], *combine([read(acc.at[1, 1]), read(rel.at[1])], seqs, body))
    fin_left_b = send(fin.at[2, 1], fin.at[0, 1], s2.at[2], r2.at[2], right)
    relay_a.wait_recv()
    put(fin.at[2, 0], *combine([read(acc.at[2, 0]), read(rel.at[0])], seqs, body))
    fin_right_a = send(fin.at[2, 0], fin.at[1, 0], s2.at[3], r2.at[3], left)

    mine_k = core * chips + chip
    for h, (from_left, from_right) in ((0, (fin_left_a, fin_right_a)), (1, (fin_left_b, fin_right_b))):
        from_left.wait_recv()
        from_right.wait_recv()
        outs, _ = combine([read(acc.at[3, h]), read(fin.at[0, h]), read(fin.at[1, h])], seqs, body, final=True)
        for hh in range(2):
            att[mine_k, h, hh * seqs:(hh + 1) * seqs, :] = outs[hh].astype(jnp.bfloat16).astype(jnp.float32)

    k_left, k_right, k_opp = core * chips + c_left, core * chips + c_right, core * chips + c_opp
    o_core = 1 - core
    to_right_b = send(att.at[mine_k, 1], att.at[mine_k, 1], s3.at[0], r3.at[0], right)
    to_left_a = send(att.at[mine_k, 0], att.at[mine_k, 0], s3.at[1], r3.at[1], left)
    to_right_a = send(att.at[mine_k, 0], att.at[mine_k, 0], s3.at[2], r3.at[2], right)
    to_left_b = send(att.at[mine_k, 1], att.at[mine_k, 1], s3.at[3], r3.at[3], left)
    to_partner = send(att.at[mine_k], att.at[mine_k], s3.at[4], r3.at[4], partner)

    cols = 512

    def multiply(k, first=False):
        wo_copy(k).wait()
        lhs = jnp.concatenate([att[k, h, hh * seqs:(hh + 1) * seqs, :] for h in range(2) for hh in range(2)], axis=1)
        lhs = lhs.astype(jnp.bfloat16)

        def tile(i, carry):
            off = pl.ds(pl.multiple_of(i * cols, cols), cols)
            y = jnp.dot(lhs, wov[k, :, off], preferred_element_type=jnp.float32)
            res[:, off] = y if first else res[:, off] + y
            return carry

        lax.fori_loop(0, model // cols, tile, 0)

    multiply(mine_k, first=True)
    to_right_b.wait_recv()
    fwd_right = send(att.at[k_left, 1], att.at[k_left, 1], s4.at[0], r4.at[0], right)
    p1 = send(att.at[k_left, 1], att.at[k_left, 1], s4.at[2], r4.at[2], partner)
    to_left_a.wait_recv()
    fwd_left = send(att.at[k_right, 0], att.at[k_right, 0], s4.at[1], r4.at[1], left)
    p2 = send(att.at[k_right, 0], att.at[k_right, 0], s4.at[3], r4.at[3], partner)
    to_partner.wait_recv()
    multiply(o_core * chips + chip)
    to_right_a.wait_recv()
    p3 = send(att.at[k_left, 0], att.at[k_left, 0], s4.at[4], r4.at[4], partner)
    to_left_b.wait_recv()
    p4 = send(att.at[k_right, 1], att.at[k_right, 1], s4.at[5], r4.at[5], partner)
    multiply(k_left)
    multiply(k_right)
    p1.wait_recv()
    p3.wait_recv()
    multiply(o_core * chips + c_left)
    p2.wait_recv()
    p4.wait_recv()
    multiply(o_core * chips + c_right)
    fwd_right.wait_recv()
    p5 = send(att.at[k_opp, 1], att.at[k_opp, 1], s4.at[6], r4.at[6], partner)
    fwd_left.wait_recv()
    p6 = send(att.at[k_opp, 0], att.at[k_opp, 0], s4.at[7], r4.at[7], partner)
    multiply(k_opp)
    p5.wait_recv()
    p6.wait_recv()
    multiply(o_core * chips + c_opp)
    tok_copy.wait()
    out_ref[...] = (tok_ref[...].astype(jnp.float32) + res[...]).astype(jnp.bfloat16)
    for copy in pair + sends + [fin_left_a, fin_right_b, fin_left_b, fin_right_a, to_right_b, to_left_a, to_right_a,
                                to_left_b, to_partner, fwd_right, fwd_left, p1, p2, p3, p4, p5, p6]:
        copy.wait_send()


def tail_stage(part, w_o, tokens, group):
    seqs, model = tokens.shape
    halves, rows, head_dim = part.shape
    chips = group // 2
    vmem = pl.BlockSpec(memory_space=pltpu.VMEM)
    hbm = pl.BlockSpec(memory_space=pltpu.HBM)
    dma = pltpu.SemaphoreType.DMA
    return pl.pallas_call(
        tail_kernel,
        name='tail_stage',
        out_shape=pltpu.VMEM((seqs, model), jnp.bfloat16),
        in_specs=[vmem, hbm, hbm],
        out_specs=vmem,
        scratch_shapes=[
            pltpu.VMEM((seqs, model), tokens.dtype),
            dma,
            pltpu.VMEM((chips, 2, rows, head_dim), jnp.float32),
            pltpu.VMEM((chips, 2, rows, head_dim), jnp.float32),
            pltpu.VMEM((2, rows, head_dim), jnp.float32),
            pltpu.VMEM((3, 2, rows, head_dim), jnp.float32),
            pltpu.VMEM((group, 2, 2 * seqs, head_dim), jnp.float32),
            pltpu.VMEM((group, w_o.shape[0] // group, model), jnp.bfloat16),
            pltpu.VMEM((seqs, model), jnp.float32),
            dma((group,)),
            dma((chips,)), dma((chips,)), dma((2,)), dma((2,)), dma((4,)), dma((4,)), dma((5,)), dma((5,)), dma((8,)), dma((8,)),
        ],
        compiler_params=pltpu.CompilerParams(collective_id=0, has_side_effects=True, vmem_limit_bytes=44 * 1024 * 1024),
    )(part, *in_hbm(w_o, tokens))


def solution(mesh):
    cache_spec = P('dp', 'sp', None, None)
    group = mesh.shape['sp']

    def device_step(tokens, positions, k_cache, v_cache, w_q, w_k, w_v, w_o, attn_norm, q_norm, k_norm):
        k_upd, v_upd, new_kv, part = local_stage(tokens, positions, k_cache, v_cache, w_q, w_k, w_v, attn_norm, q_norm, k_norm)
        block_out = tail_stage(part, w_o, tokens, group)
        return block_out, k_upd, v_upd, new_kv

    return jax.shard_map(device_step, mesh=mesh, in_specs=(P('dp', None), P('dp'), cache_spec, cache_spec, P(), P(), P(), P(), P(), P(), P()), out_specs=(P('dp', None), cache_spec, cache_spec, P('dp', None, None, None)), check_vma=False)
```

```python
import functools

import jax
import jax.numpy as jnp
import numpy as np
from jax import lax
from jax.experimental import pallas as pl
from jax.experimental.pallas import tpu as pltpu
from jax.sharding import PartitionSpec as P

NORM_EPS = 1e-6
ROPE_THETA = 1000000.0
NEG_FILL = -1e30
MESH = pl.DeviceIdType.MESH
W_ROWS = 512
W_SLOTS = 3
STAT_ROWS = 8


def rope_frequencies(head_dim):
    inv_freq = ROPE_THETA ** (-np.arange(head_dim // 2, dtype=np.float64) * 2.0 / head_dim)
    return np.concatenate([inv_freq, inv_freq])[None, :].astype(np.float32)


def norm_rope(proj, gain, cos_full, sin_full):
    values = proj.astype(jnp.bfloat16).astype(jnp.float32)
    scale = lax.rsqrt(jnp.mean(values * values, axis=-1, keepdims=True) + NORM_EPS)
    normed = values * scale * gain
    turned = pltpu.roll(normed, normed.shape[-1] // 2, 1)
    return (normed * cos_full + turned * sin_full).astype(jnp.bfloat16).astype(jnp.float32)


def local_kernel(pos_in, tok_in, freq_in, an_in, qn_in, kn_in, wq_ref, wk_ref, wv_ref, kc_ref, vc_ref,
                 ko_ref, vo_ref, new_out, part_ref,
                 pos_ref, tok_ref, freq_ref, an_ref, qn_ref, kn_ref, new_ref, insem, newsem, hid, wqb, wkb, wvb, yq, yk, yv, cosb, sinb, kbuf, vbuf, qf, kf, vf, mstat, lstat, sbuf, ebuf, obuf, wsem, ksem, vsem, kosem, vosem):
    seqs, model = tok_ref.shape
    head_dim = qn_ref.shape[-1]
    slots, kv_heads = kbuf.shape[1], kbuf.shape[2]
    groups = ksem.shape[0]
    per_group = seqs // groups
    q_heads = wq_ref.shape[1] // head_dim
    start = lax.axis_index('sp') * slots
    steps = model // W_ROWS
    weights = ((wk_ref, wkb, yk), (wv_ref, wvb, yv), (wq_ref, wqb, yq))

    def w_copies(i):
        slot = lax.rem(i, W_SLOTS)
        rows = pl.ds(pl.multiple_of(i * W_ROWS, W_ROWS), W_ROWS)
        return [pltpu.make_async_copy(ref.at[rows], buf.at[slot], wsem.at[j, slot]) for j, (ref, buf, _) in enumerate(weights)]

    def cache_in(ref, buf, sem, g):
        rows = pl.ds(g * per_group, per_group)
        return pltpu.make_async_copy(ref.at[rows], buf.at[rows], sem.at[g])

    smalls = [pltpu.make_async_copy(src, dst, insem.at[j]) for j, (src, dst) in enumerate((
        (tok_in, tok_ref), (pos_in, pos_ref), (freq_in, freq_ref), (an_in, an_ref), (qn_in, qn_ref), (kn_in, kn_ref)))]
    for copy in smalls:
        copy.start()
    for n in range(W_SLOTS):
        for copy in w_copies(jnp.int32(n)):
            copy.start()
    for copy in smalls:
        copy.wait()

    lanes = an_ref.shape[1]
    total = jnp.zeros((seqs, 1), jnp.float32)
    for i in range(model // lanes):
        xf = tok_ref[:, i * lanes:(i + 1) * lanes].astype(jnp.float32)
        total = total + jnp.sum(xf * xf, axis=-1, keepdims=True)
    inv = lax.rsqrt(total / model + NORM_EPS)
    per_step = W_ROWS // lanes
    for i in range(model // lanes):
        xf = tok_ref[:, i * lanes:(i + 1) * lanes].astype(jnp.float32)
        gain = an_ref[i:i + 1, :].astype(jnp.float32)
        hid[i // per_step, :, (i % per_step) * lanes:(i % per_step + 1) * lanes] = (xf * inv * gain).astype(jnp.bfloat16)

    for b in range(seqs):
        cosb[b:b + 1, :] = jnp.full((1, head_dim), pos_ref[b], jnp.int32).astype(jnp.float32)
    angles = cosb[...] * freq_ref[...]
    sign = jnp.where(lax.broadcasted_iota(jnp.int32, angles.shape, 1) < head_dim // 2, -1.0, 1.0)
    sinb[...] = jnp.sin(angles) * sign
    cosb[...] = jnp.cos(angles)
    for y in (yq, yk, yv):
        y[...] = jnp.zeros_like(y)

    def w_step(i, carry):
        slot = lax.rem(i, W_SLOTS)
        lhs = hid[i]
        for copy, (_, buf, y) in zip(w_copies(i), weights):
            copy.wait()
            y[...] += jnp.dot(lhs, buf[slot], preferred_element_type=jnp.float32)

        @pl.when(i + W_SLOTS < steps)
        def _():
            for copy in w_copies(i + W_SLOTS):
                copy.start()

        @pl.when(i + W_SLOTS >= steps)
        def _():
            g = i + W_SLOTS - steps
            cache_in(kc_ref, kbuf, ksem, g).start()
            cache_in(vc_ref, vbuf, vsem, g).start()

        return carry

    lax.fori_loop(0, steps, w_step, 0)
    for g in range(W_SLOTS, groups):
        cache_in(kc_ref, kbuf, ksem, g).start()
        cache_in(vc_ref, vbuf, vsem, g).start()

    cos_full, sin_full = cosb[...], sinb[...]
    k_gain = kn_ref[...].astype(jnp.float32)
    q_gain = qn_ref[...].astype(jnp.float32)
    for h in range(kv_heads):
        cols = slice(h * head_dim, (h + 1) * head_dim)
        rows = slice(h * seqs, (h + 1) * seqs)
        kf[rows, :] = norm_rope(yk[:, cols], k_gain, cos_full, sin_full)
        vf[rows, :] = yv[:, cols].astype(jnp.bfloat16).astype(jnp.float32)
    for h in range(q_heads):
        qf[h * seqs:(h + 1) * seqs, :] = norm_rope(yq[:, h * head_dim:(h + 1) * head_dim], q_gain, cos_full, sin_full)

    half = q_heads // 2
    cols = slots * kv_heads
    row_id = lax.broadcasted_iota(jnp.int32, (q_heads, cols), 0)
    col_id = lax.broadcasted_iota(jnp.int32, (q_heads, cols), 1)
    q_per_kv = q_heads // kv_heads
    head_ok = ((row_id % half) * 2) // q_per_kv == col_id % kv_heads
    slot_key = jnp.where(head_ok, col_id // kv_heads, slots * 1024)
    lane = lax.broadcasted_iota(jnp.int32, (q_heads, 128), 1)
    score_scale = head_dim ** -0.5
    part_rows = part_ref.shape[1]
    mstat[...] = jnp.zeros_like(mstat)
    lstat[...] = jnp.zeros_like(lstat)

    def group_step(g, carry):
        cache_in(kc_ref, kbuf, ksem, g).wait()
        cache_in(vc_ref, vbuf, vsem, g).wait()
        m_acc, l_acc = mstat[...], lstat[...]
        members = [g * per_group + bb for bb in range(per_group)]
        for b in members:
            local = pos_ref[b] - start
            here = (local >= 0) & (local < slots)
            at = jnp.clip(local, 0, slots - 1)
            k_new = kf[pl.ds(b, kv_heads, stride=seqs), :]
            v_new = vf[pl.ds(b, kv_heads, stride=seqs), :]
            new_ref[b, 0] = k_new.astype(jnp.bfloat16)
            new_ref[b, 1] = v_new.astype(jnp.bfloat16)
            kbuf[b, at] = jnp.where(here, k_new, kbuf[b, at].astype(jnp.float32)).astype(jnp.bfloat16)
            vbuf[b, at] = jnp.where(here, v_new, vbuf[b, at].astype(jnp.float32)).astype(jnp.bfloat16)
        for bb, b in enumerate(members):
            q_even = qf[pl.ds(b, half, stride=2 * seqs), :]
            q_odd = qf[pl.ds(b + seqs, half, stride=2 * seqs), :]
            q_b = jnp.concatenate([q_even, q_odd], axis=0).astype(jnp.bfloat16)
            k_b = kbuf[b].reshape(cols, head_dim)
            sbuf[bb] = lax.dot_general(q_b, k_b, (((1,), (1,)), ((), ())), preferred_element_type=jnp.float32)
        for bb, b in enumerate(members):
            live = slot_key <= pos_ref[b] - start
            s = jnp.where(live, sbuf[bb] * score_scale, NEG_FILL)
            m = jnp.max(s, axis=-1, keepdims=True)
            e = jnp.where(live, jnp.exp(s - m), 0.0)
            l = jnp.sum(e, axis=-1, keepdims=True)
            ebuf[bb] = e.astype(jnp.bfloat16)
            m_acc = jnp.where(lane == b, m, m_acc)
            l_acc = jnp.where(lane == b, l, l_acc)
        for bb, b in enumerate(members):
            obuf[bb] = jnp.dot(ebuf[bb], vbuf[b].reshape(cols, head_dim), preferred_element_type=jnp.float32)
        for bb, b in enumerate(members):
            for par in range(2):
                for i in range(half):
                    part_ref[i, pl.ds(b + par * seqs, 1), :] = obuf[bb, par * half + i:par * half + i + 1, :]
        mstat[...] = m_acc
        lstat[...] = l_acc
        rows = pl.ds(g * per_group, per_group)
        pltpu.make_async_copy(kbuf.at[rows], ko_ref.at[rows], kosem.at[g]).start()
        pltpu.make_async_copy(vbuf.at[rows], vo_ref.at[rows], vosem.at[g]).start()
        pltpu.make_async_copy(new_ref.at[rows], new_out.at[rows], newsem.at[g]).start()
        return carry

    lax.fori_loop(0, groups, group_step, 0)

    for i in range(half):
        base = 2 * seqs
        part_ref[i, base:base + 1, :] = mstat[i:i + 1, :]
        part_ref[i, base + 1:base + 2, :] = mstat[half + i:half + i + 1, :]
        part_ref[i, base + 2:base + 3, :] = lstat[i:i + 1, :]
        part_ref[i, base + 3:base + 4, :] = lstat[half + i:half + i + 1, :]
        part_ref[i, base + 4:base + 8, :] = jnp.zeros((4, 128), jnp.float32)
    for g in range(groups):
        rows = pl.ds(g * per_group, per_group)
        pltpu.make_async_copy(kbuf.at[rows], ko_ref.at[rows], kosem.at[g]).wait()
        pltpu.make_async_copy(vbuf.at[rows], vo_ref.at[rows], vosem.at[g]).wait()
        pltpu.make_async_copy(new_ref.at[rows], new_out.at[rows], newsem.at[g]).wait()


def in_hbm(*arrays):
    return [pltpu.with_memory_space_constraint(jnp.asarray(a), pltpu.HBM) for a in arrays]


def local_stage(tokens, positions, k_cache, v_cache, w_q, w_k, w_v, attn_norm, q_norm, k_norm):
    seqs, model = tokens.shape
    slots, kv_heads, head_dim = k_cache.shape[1:]
    q_heads = w_q.shape[1] // head_dim
    groups = 8
    vmem = pl.BlockSpec(memory_space=pltpu.VMEM)
    anyspec = pl.BlockSpec(memory_space=pl.ANY)
    hbm = pl.BlockSpec(memory_space=pltpu.HBM)
    part_shape = (q_heads // 2, 2 * seqs + STAT_ROWS, head_dim)
    return pl.pallas_call(
        local_kernel,
        name='local_stage',
        out_shape=(
            jax.ShapeDtypeStruct(k_cache.shape, k_cache.dtype),
            jax.ShapeDtypeStruct(v_cache.shape, v_cache.dtype),
            jax.ShapeDtypeStruct((seqs, 2, kv_heads, head_dim), jnp.bfloat16),
            pltpu.VMEM(part_shape, jnp.float32),
        ),
        in_specs=[hbm] * 11,
        out_specs=(anyspec, anyspec, anyspec, vmem),
        scratch_shapes=[
            pltpu.SMEM(positions.shape, jnp.int32),
            pltpu.VMEM(tokens.shape, tokens.dtype),
            pltpu.VMEM((1, head_dim), jnp.float32),
            pltpu.VMEM((model // 128, 128), attn_norm.dtype),
            pltpu.VMEM((1, head_dim), q_norm.dtype),
            pltpu.VMEM((1, head_dim), k_norm.dtype),
            pltpu.VMEM((seqs, 2, kv_heads, head_dim), jnp.bfloat16),
            pltpu.SemaphoreType.DMA((6,)),
            pltpu.SemaphoreType.DMA((groups,)),
            pltpu.VMEM((model // W_ROWS, seqs, W_ROWS), jnp.bfloat16),
            pltpu.VMEM((W_SLOTS, W_ROWS, w_q.shape[1]), jnp.bfloat16),
            pltpu.VMEM((W_SLOTS, W_ROWS, w_k.shape[1]), jnp.bfloat16),
            pltpu.VMEM((W_SLOTS, W_ROWS, w_v.shape[1]), jnp.bfloat16),
            pltpu.VMEM((seqs, w_q.shape[1]), jnp.float32),
            pltpu.VMEM((seqs, w_k.shape[1]), jnp.float32),
            pltpu.VMEM((seqs, w_v.shape[1]), jnp.float32),
            pltpu.VMEM((seqs, head_dim), jnp.float32),
            pltpu.VMEM((seqs, head_dim), jnp.float32),
            pltpu.VMEM(k_cache.shape, k_cache.dtype),
            pltpu.VMEM(v_cache.shape, v_cache.dtype),
            pltpu.VMEM((q_heads * seqs, head_dim), jnp.float32),
            pltpu.VMEM((kv_heads * seqs, head_dim), jnp.float32),
            pltpu.VMEM((kv_heads * seqs, head_dim), jnp.float32),
            pltpu.VMEM((q_heads, 128), jnp.float32),
            pltpu.VMEM((q_heads, 128), jnp.float32),
            pltpu.VMEM((seqs // groups, q_heads, slots * kv_heads), jnp.float32),
            pltpu.VMEM((seqs // groups, q_heads, slots * kv_heads), jnp.bfloat16),
            pltpu.VMEM((seqs // groups, q_heads, head_dim), jnp.float32),
            pltpu.SemaphoreType.DMA((3, W_SLOTS)),
            pltpu.SemaphoreType.DMA((groups,)),
            pltpu.SemaphoreType.DMA((groups,)),
            pltpu.SemaphoreType.DMA((groups,)),
            pltpu.SemaphoreType.DMA((groups,)),
        ],
        compiler_params=pltpu.CompilerParams(vmem_limit_bytes=46 * 1024 * 1024),
    )(*in_hbm(positions, tokens, rope_frequencies(head_dim), attn_norm.reshape(-1, 128), q_norm[None, :], k_norm[None, :]), w_q, w_k, w_v, k_cache, v_cache)


def combine(pieces, seqs, rows_out, final=False):
    stats = [jnp.transpose(s, (1, 0))[:seqs] for _, s in pieces]
    peak = functools.reduce(jnp.maximum, [t[:, 0:2] for t in stats])
    factors = [jnp.exp(t[:, 0:2] - peak) for t in stats]
    total = functools.reduce(jnp.add, [f * t[:, 2:4] for f, t in zip(factors, stats)])
    outs = []
    for hh in range(2):
        acc = None
        for (o, _), f in zip(pieces, factors):
            term = o[hh * seqs:(hh + 1) * seqs] * f[:, hh:hh + 1]
            acc = term if acc is None else acc + term
        if final:
            acc = acc / total[:, hh:hh + 1]
        outs.append(acc)
    if final:
        return outs, None
    both = jnp.concatenate([peak, total, jnp.zeros((seqs, 4), jnp.float32)], axis=1)
    both = jnp.concatenate([both, jnp.zeros((128 - seqs, 8), jnp.float32)], axis=0)
    return outs, jnp.transpose(both, (1, 0))


def tail_kernel(mine, wo_ref, tok_in, out_ref, tok_ref, toksem, pin, acc, rel, fin, att, wov, res,
                wsem, s0, r0, s1, r1, s2, r2, s3, r3, s4, r4):
    seqs, model = tok_ref.shape
    tok_copy = pltpu.make_async_copy(tok_in, tok_ref, toksem)
    tok_copy.start()
    me = lax.axis_index('sp')
    n = lax.axis_size('sp')
    chips = n // 2
    core, chip = lax.rem(me, 2), me // 2
    c_right, c_left, c_opp = lax.rem(chip + 1, chips), lax.rem(chip + chips - 1, chips), lax.rem(chip + 2, chips)
    partner = chip * 2 + 1 - core
    right, left = c_right * 2 + core, c_left * 2 + core
    body = 2 * seqs
    k_rows = wov.shape[1]

    def wo_copy(k):
        return pltpu.make_async_copy(wo_ref.at[pl.ds(pl.multiple_of(k * k_rows, k_rows), k_rows)], wov.at[k], wsem.at[k])

    barrier = pltpu.get_barrier_semaphore()
    for peer in (partner, right, left):
        pl.semaphore_signal(barrier, inc=1, device_id={'sp': peer}, device_id_type=MESH)
    pl.semaphore_wait(barrier, 3)

    def send(src, dst, ss, rs, peer):
        copy = pltpu.make_async_remote_copy(src_ref=src, dst_ref=dst, send_sem=ss, recv_sem=rs,
                                            device_id={'sp': peer}, device_id_type=MESH)
        copy.start()
        return copy

    order = (c_opp, c_right, c_left, chip)
    halves = 2 * chips
    sends = []
    pair = []
    for i, c in enumerate(order):
        copy = send(mine.at[pl.ds((1 - core) * halves + 2 * c, 2)], pin.at[i], s0.at[i], r0.at[i], partner)
        pair.append(copy)

    for k in range(2):
        wo_copy(k).start()

    def put(dst, outs, stat):
        for hh in range(2):
            dst[hh * seqs:(hh + 1) * seqs, :] = outs[hh]
        dst[body:body + STAT_ROWS, :] = stat

    def read(ref):
        return ref[0:body, :], ref[body:body + STAT_ROWS, :]

    def merge_pair(i):
        pair[i].wait_recv()
        for h in range(2):
            own = mine.at[core * halves + 2 * order[i] + h]
            put(acc.at[i, h], *combine([read(own), read(pin.at[i, h])], seqs, body))

    merge_pair(0)
    sends.append(send(acc.at[0, 1], rel.at[1], s1.at[1], r1.at[1], right))
    sends.append(send(acc.at[0, 0], rel.at[0], s1.at[0], r1.at[0], left))
    relay_b, relay_a = sends[0], sends[1]
    for k in range(2, 4):
        wo_copy(k).start()
    merge_pair(1)
    fin_left_a = send(acc.at[1, 0], fin.at[0, 0], s2.at[0], r2.at[0], right)
    merge_pair(2)
    fin_right_b = send(acc.at[2, 1], fin.at[1, 1], s2.at[1], r2.at[1], left)
    merge_pair(3)
    for k in range(4, 8):
        wo_copy(k).start()
    relay_b.wait_recv()
    put(fin.at[2, 1], *combine([read(acc.at[1, 1]), read(rel.at[1])], seqs, body))
    fin_left_b = send(fin.at[2, 1], fin.at[0, 1], s2.at[2], r2.at[2], right)
    relay_a.wait_recv()
    put(fin.at[2, 0], *combine([read(acc.at[2, 0]), read(rel.at[0])], seqs, body))
    fin_right_a = send(fin.at[2, 0], fin.at[1, 0], s2.at[3], r2.at[3], left)

    mine_k = core * chips + chip
    for h, (from_left, from_right) in ((0, (fin_left_a, fin_right_a)), (1, (fin_left_b, fin_right_b))):
        from_left.wait_recv()
        from_right.wait_recv()
        outs, _ = combine([read(acc.at[3, h]), read(fin.at[0, h]), read(fin.at[1, h])], seqs, body, final=True)
        for hh in range(2):
            att[mine_k, h, hh * seqs:(hh + 1) * seqs, :] = outs[hh].astype(jnp.bfloat16).astype(jnp.float32)

    k_left, k_right, k_opp = core * chips + c_left, core * chips + c_right, core * chips + c_opp
    o_core = 1 - core
    to_right_b = send(att.at[mine_k, 1], att.at[mine_k, 1], s3.at[0], r3.at[0], right)
    to_left_a = send(att.at[mine_k, 0], att.at[mine_k, 0], s3.at[1], r3.at[1], left)
    to_right_a = send(att.at[mine_k, 0], att.at[mine_k, 0], s3.at[2], r3.at[2], right)
    to_left_b = send(att.at[mine_k, 1], att.at[mine_k, 1], s3.at[3], r3.at[3], left)
    to_partner = send(att.at[mine_k], att.at[mine_k], s3.at[4], r3.at[4], partner)

    cols = 512

    def multiply(k, first=False):
        wo_copy(k).wait()
        lhs = jnp.concatenate([att[k, h, hh * seqs:(hh + 1) * seqs, :] for h in range(2) for hh in range(2)], axis=1)
        lhs = lhs.astype(jnp.bfloat16)

        for i in range(model // cols):
            off = slice(i * cols, (i + 1) * cols)
            y = jnp.dot(lhs, wov[k, :, off], preferred_element_type=jnp.float32)
            res[:, off] = y if first else res[:, off] + y

    multiply(mine_k, first=True)
    to_right_b.wait_recv()
    fwd_right = send(att.at[k_left, 1], att.at[k_left, 1], s4.at[0], r4.at[0], right)
    p1 = send(att.at[k_left, 1], att.at[k_left, 1], s4.at[2], r4.at[2], partner)
    to_left_a.wait_recv()
    fwd_left = send(att.at[k_right, 0], att.at[k_right, 0], s4.at[1], r4.at[1], left)
    p2 = send(att.at[k_right, 0], att.at[k_right, 0], s4.at[3], r4.at[3], partner)
    to_partner.wait_recv()
    multiply(o_core * chips + chip)
    to_right_a.wait_recv()
    p3 = send(att.at[k_left, 0], att.at[k_left, 0], s4.at[4], r4.at[4], partner)
    to_left_b.wait_recv()
    p4 = send(att.at[k_right, 1], att.at[k_right, 1], s4.at[5], r4.at[5], partner)
    multiply(k_left)
    multiply(k_right)
    p1.wait_recv()
    p3.wait_recv()
    multiply(o_core * chips + c_left)
    p2.wait_recv()
    p4.wait_recv()
    multiply(o_core * chips + c_right)
    fwd_right.wait_recv()
    p5 = send(att.at[k_opp, 1], att.at[k_opp, 1], s4.at[6], r4.at[6], partner)
    fwd_left.wait_recv()
    p6 = send(att.at[k_opp, 0], att.at[k_opp, 0], s4.at[7], r4.at[7], partner)
    multiply(k_opp)
    p5.wait_recv()
    p6.wait_recv()
    multiply(o_core * chips + c_opp)
    tok_copy.wait()
    out_ref[...] = (tok_ref[...].astype(jnp.float32) + res[...]).astype(jnp.bfloat16)
    for copy in pair + sends + [fin_left_a, fin_right_b, fin_left_b, fin_right_a, to_right_b, to_left_a, to_right_a,
                                to_left_b, to_partner, fwd_right, fwd_left, p1, p2, p3, p4, p5, p6]:
        copy.wait_send()


def tail_stage(part, w_o, tokens, group):
    seqs, model = tokens.shape
    halves, rows, head_dim = part.shape
    chips = group // 2
    vmem = pl.BlockSpec(memory_space=pltpu.VMEM)
    hbm = pl.BlockSpec(memory_space=pltpu.HBM)
    dma = pltpu.SemaphoreType.DMA
    return pl.pallas_call(
        tail_kernel,
        name='tail_stage',
        out_shape=pltpu.VMEM((seqs, model), jnp.bfloat16),
        in_specs=[vmem, hbm, hbm],
        out_specs=vmem,
        scratch_shapes=[
            pltpu.VMEM((seqs, model), tokens.dtype),
            dma,
            pltpu.VMEM((chips, 2, rows, head_dim), jnp.float32),
            pltpu.VMEM((chips, 2, rows, head_dim), jnp.float32),
            pltpu.VMEM((2, rows, head_dim), jnp.float32),
            pltpu.VMEM((3, 2, rows, head_dim), jnp.float32),
            pltpu.VMEM((group, 2, 2 * seqs, head_dim), jnp.float32),
            pltpu.VMEM((group, w_o.shape[0] // group, model), jnp.bfloat16),
            pltpu.VMEM((seqs, model), jnp.float32),
            dma((group,)),
            dma((chips,)), dma((chips,)), dma((2,)), dma((2,)), dma((4,)), dma((4,)), dma((5,)), dma((5,)), dma((8,)), dma((8,)),
        ],
        compiler_params=pltpu.CompilerParams(collective_id=0, has_side_effects=True, vmem_limit_bytes=44 * 1024 * 1024),
    )(part, *in_hbm(w_o, tokens))


def solution(mesh):
    cache_spec = P('dp', 'sp', None, None)
    group = mesh.shape['sp']

    def device_step(tokens, positions, k_cache, v_cache, w_q, w_k, w_v, w_o, attn_norm, q_norm, k_norm):
        k_upd, v_upd, new_kv, part = local_stage(tokens, positions, k_cache, v_cache, w_q, w_k, w_v, attn_norm, q_norm, k_norm)
        block_out = tail_stage(part, w_o, tokens, group)
        return block_out, k_upd, v_upd, new_kv

    return jax.shard_map(device_step, mesh=mesh, in_specs=(P('dp', None), P('dp'), cache_spec, cache_spec, P(), P(), P(), P(), P(), P(), P()), out_specs=(P('dp', None), cache_spec, cache_spec, P('dp', None, None, None)), check_vma=False)
```

```python
import functools

import jax
import jax.numpy as jnp
import numpy as np
from jax import lax
from jax.experimental import pallas as pl
from jax.experimental.pallas import tpu as pltpu
from jax.sharding import PartitionSpec as P

NORM_EPS = 1e-6
ROPE_THETA = 1000000.0
NEG_FILL = -1e30
MESH = pl.DeviceIdType.MESH
STAT_ROWS = 8


def in_hbm(*arrays):
    return [pltpu.with_memory_space_constraint(jnp.asarray(a), pltpu.HBM) for a in arrays]


def rope_frequencies(head_dim):
    inv_freq = ROPE_THETA ** (-np.arange(head_dim // 2, dtype=np.float64) * 2.0 / head_dim)
    return np.concatenate([inv_freq, inv_freq])[None, :].astype(np.float32)


def norm_rope(proj, gain, cos_full, sin_full):
    values = proj.astype(jnp.bfloat16).astype(jnp.float32)
    scale = lax.rsqrt(jnp.mean(values * values, axis=-1, keepdims=True) + NORM_EPS)
    normed = values * scale * gain
    turned = pltpu.roll(normed, normed.shape[-1] // 2, 1)
    return (normed * cos_full + turned * sin_full).astype(jnp.bfloat16).astype(jnp.float32)


def ring_place():
    me = lax.axis_index('sp')
    chips = lax.axis_size('sp') // 2
    core, chip = lax.rem(me, 2), me // 2
    c_right, c_left, c_opp = lax.rem(chip + 1, chips), lax.rem(chip + chips - 1, chips), lax.rem(chip + 2, chips)
    return chips, core, chip, c_right, c_left, c_opp, chip * 2 + 1 - core, c_right * 2 + core, c_left * 2 + core


def enter(peers):
    barrier = pltpu.get_barrier_semaphore()
    for peer in peers:
        pl.semaphore_signal(barrier, inc=1, device_id={'sp': peer}, device_id_type=MESH)
    return lambda: pl.semaphore_wait(barrier, len(peers))


def send(src, dst, ss, rs, peer):
    copy = pltpu.make_async_remote_copy(src_ref=src, dst_ref=dst, send_sem=ss, recv_sem=rs,
                                        device_id={'sp': peer}, device_id_type=MESH)
    copy.start()
    return copy


def project_kernel(pos_in, tok_in, freq_in, an_in, qn_in, kn_in, wq_ref, wk_ref, wv_ref, kc_ref, vc_ref,
                   qf, kf, vf, kbuf, vbuf,
                   pos_ref, tok_ref, freq_ref, an_ref, qn_ref, kn_ref, hid, wbuf, cosb, sinb, insem, wsem, csem, ss, rs):
    seqs, model = tok_ref.shape
    head_dim = qn_ref.shape[-1]
    blocks, _, blk = hid.shape
    width = wbuf.shape[-1]
    heads = width // head_dim
    chips, core, chip, c_right, c_left, c_opp, partner, right, left = ring_place()
    mine_k = core * chips + chip

    smalls = [pltpu.make_async_copy(src, dst, insem.at[j]) for j, (src, dst) in enumerate((
        (tok_in, tok_ref), (pos_in, pos_ref), (freq_in, freq_ref), (an_in, an_ref), (qn_in, qn_ref), (kn_in, kn_ref)))]
    for copy in smalls:
        copy.start()
    bulk = []
    for j, (ref, col) in enumerate(((wq_ref, mine_k), (wk_ref, core), (wv_ref, core))):
        for i in range(blocks):
            src = ref.at[pl.ds(i * blk, blk), pl.ds(pl.multiple_of(col * width, width), width)]
            bulk.append(pltpu.make_async_copy(src, wbuf.at[j, i], wsem.at[j, i]))
    pieces = csem.shape[1]
    per = seqs // pieces
    for g in range(pieces):
        for j, (ref, buf) in enumerate(((kc_ref, kbuf), (vc_ref, vbuf))):
            rows = pl.ds(g * per, per)
            bulk.append(pltpu.make_async_copy(ref.at[rows], buf.at[rows], csem.at[j, g]))
    issued = 0

    def issue(count):
        nonlocal issued
        for copy in bulk[issued:issued + count]:
            copy.start()
        issued += count

    issue(6)
    arrived = enter((partner, right, left))
    for copy in smalls:
        copy.wait()

    lanes = an_ref.shape[1]
    total = jnp.zeros((seqs, lanes), jnp.float32)
    for i in range(model // lanes):
        xf = tok_ref[:, i * lanes:(i + 1) * lanes].astype(jnp.float32)
        total = total + xf * xf
    inv = lax.rsqrt(jnp.sum(total, axis=-1, keepdims=True) / model + NORM_EPS)
    per_blk = blk // lanes
    for i in range(model // lanes):
        xf = tok_ref[:, i * lanes:(i + 1) * lanes].astype(jnp.float32)
        gain = an_ref[i:i + 1, :].astype(jnp.float32)
        hid[i // per_blk, :, (i % per_blk) * lanes:(i % per_blk + 1) * lanes] = (xf * inv * gain).astype(jnp.bfloat16)

    for b in range(seqs):
        cosb[b:b + 1, :] = jnp.full((1, head_dim), pos_ref[b], jnp.int32).astype(jnp.float32)
    angles = cosb[...] * freq_ref[...]
    sign = jnp.where(lax.broadcasted_iota(jnp.int32, angles.shape, 1) < head_dim // 2, -1.0, 1.0)
    sinb[...] = jnp.sin(angles) * sign
    cosb[...] = jnp.cos(angles)
    cos_full, sin_full = cosb[...], sinb[...]

    def project(j, more):
        y = None
        for i in range(blocks):
            bulk[j * blocks + i].wait()
            issue(more)
            part = jnp.dot(hid[i], wbuf[j, i], preferred_element_type=jnp.float32)
            y = part if y is None else y + part
        return [y[:, h * head_dim:(h + 1) * head_dim] for h in range(heads)]

    def put(dst, base, values):
        for h, value in enumerate(values):
            dst[pl.ds(pl.multiple_of(base + h * seqs, seqs), seqs), :] = value

    half_rows = heads // 2 * seqs

    def q_half(k, h):
        return qf.at[pl.ds(pl.multiple_of(k * heads * seqs + h * half_rows, half_rows), half_rows)]

    q_gain = qn_ref[...].astype(jnp.float32)
    put(qf, mine_k * heads * seqs, [norm_rope(p, q_gain, cos_full, sin_full) for p in project(0, 1)])
    arrived()
    count = 0
    sent = []

    def push(ref, peer):
        nonlocal count
        sent.append(send(ref, ref, ss.at[count], rs.at[count], peer))
        count += 1
        return sent[-1]

    to_right_b = push(q_half(mine_k, 1), right)
    to_left_a = push(q_half(mine_k, 0), left)
    to_right_a = push(q_half(mine_k, 0), right)
    to_left_b = push(q_half(mine_k, 1), left)
    push(q_half(mine_k, 0), partner)
    push(q_half(mine_k, 1), partner)

    kv_rows = heads * seqs
    kv_base = core * kv_rows
    kv_part = pl.ds(pl.multiple_of(kv_base, kv_rows), kv_rows)
    k_gain = kn_ref[...].astype(jnp.float32)
    put(kf, kv_base, [norm_rope(p, k_gain, cos_full, sin_full) for p in project(1, 2)])
    push(kf.at[kv_part], partner)
    put(vf, kv_base, [p.astype(jnp.bfloat16).astype(jnp.float32) for p in project(2, 3)])
    push(vf.at[kv_part], partner)
    issue(len(bulk) - issued)

    k_left, k_right, k_opp = core * chips + c_left, core * chips + c_right, core * chips + c_opp
    to_right_b.wait_recv()
    fwd_right = push(q_half(k_left, 1), right)
    to_left_a.wait_recv()
    fwd_left = push(q_half(k_right, 0), left)
    push(q_half(k_left, 1), partner)
    push(q_half(k_right, 0), partner)
    to_right_a.wait_recv()
    push(q_half(k_left, 0), partner)
    to_left_b.wait_recv()
    push(q_half(k_right, 1), partner)
    fwd_right.wait_recv()
    push(q_half(k_opp, 1), partner)
    fwd_left.wait_recv()
    push(q_half(k_opp, 0), partner)
    waited = (to_right_b, to_left_a, to_right_a, to_left_b, fwd_right, fwd_left)
    for copy in sent:
        if not any(copy is w for w in waited):
            copy.wait_recv()
        copy.wait_send()
    for copy in bulk[3 * blocks:]:
        copy.wait()


def project_stage(tokens, positions, k_cache, v_cache, w_q, w_k, w_v, attn_norm, q_norm, k_norm, group):
    seqs, model = tokens.shape
    kv_heads, head_dim = k_cache.shape[2:]
    q_heads = w_q.shape[1] // head_dim
    width = w_q.shape[1] // group
    blocks = 4
    vmem = pl.BlockSpec(memory_space=pltpu.VMEM)
    hbm = pl.BlockSpec(memory_space=pltpu.HBM)
    dma = pltpu.SemaphoreType.DMA
    return pl.pallas_call(
        project_kernel,
        name='project_stage',
        out_shape=(
            pltpu.VMEM((q_heads * seqs, head_dim), jnp.float32),
            pltpu.VMEM((kv_heads * seqs, head_dim), jnp.float32),
            pltpu.VMEM((kv_heads * seqs, head_dim), jnp.float32),
            pltpu.VMEM(k_cache.shape, k_cache.dtype),
            pltpu.VMEM(v_cache.shape, v_cache.dtype),
        ),
        in_specs=[hbm] * 11,
        out_specs=(vmem,) * 5,
        scratch_shapes=[
            pltpu.SMEM(positions.shape, jnp.int32),
            pltpu.VMEM(tokens.shape, tokens.dtype),
            pltpu.VMEM((1, head_dim), jnp.float32),
            pltpu.VMEM((model // 128, 128), attn_norm.dtype),
            pltpu.VMEM((1, head_dim), q_norm.dtype),
            pltpu.VMEM((1, head_dim), k_norm.dtype),
            pltpu.VMEM((blocks, seqs, model // blocks), jnp.bfloat16),
            pltpu.VMEM((3, blocks, model // blocks, width), jnp.bfloat16),
            pltpu.VMEM((seqs, head_dim), jnp.float32),
            pltpu.VMEM((seqs, head_dim), jnp.float32),
            dma((6,)), dma((3, blocks)), dma((2, 8)), dma((16,)), dma((16,)),
        ],
        compiler_params=pltpu.CompilerParams(collective_id=1, has_side_effects=True, vmem_limit_bytes=24 * 1024 * 1024),
    )(*in_hbm(positions, tokens, rope_frequencies(head_dim), attn_norm.reshape(-1, 128), q_norm[None, :], k_norm[None, :],
              w_q, w_k, w_v, k_cache, v_cache))


def attend_kernel(pos_in, qf, kf, vf, k_in, v_in, ko_ref, vo_ref, new_out, part_ref, kbuf, vbuf,
                  pos_ref, new_ref, mstat, lstat, sbuf, ebuf, obuf, possem, newsem, kosem, vosem):
    seqs, slots, kv_heads, head_dim = kbuf.shape
    groups = kosem.shape[0]
    per_group = seqs // groups
    q_heads = qf.shape[0] // seqs
    start = lax.axis_index('sp') * slots
    pos_copy = pltpu.make_async_copy(pos_in, pos_ref, possem)
    pos_copy.start()
    pos_copy.wait()

    half = q_heads // 2
    cols = slots * kv_heads
    row_id = lax.broadcasted_iota(jnp.int32, (q_heads, cols), 0)
    col_id = lax.broadcasted_iota(jnp.int32, (q_heads, cols), 1)
    q_per_kv = q_heads // kv_heads
    head_ok = ((row_id % half) * 2) // q_per_kv == col_id % kv_heads
    slot_key = jnp.where(head_ok, col_id // kv_heads, slots * 1024)
    lane = lax.broadcasted_iota(jnp.int32, (q_heads, 128), 1)
    score_scale = head_dim ** -0.5
    part_rows = part_ref.shape[1]
    mstat[...] = jnp.zeros_like(mstat)
    lstat[...] = jnp.zeros_like(lstat)

    def group_step(g, carry):
        m_acc, l_acc = mstat[...], lstat[...]
        members = [g * per_group + bb for bb in range(per_group)]
        for b in members:
            local = pos_ref[b] - start
            here = (local >= 0) & (local < slots)
            at = jnp.clip(local, 0, slots - 1)
            k_new = kf[pl.ds(b, kv_heads, stride=seqs), :]
            v_new = vf[pl.ds(b, kv_heads, stride=seqs), :]
            new_ref[b, 0] = k_new.astype(jnp.bfloat16)
            new_ref[b, 1] = v_new.astype(jnp.bfloat16)
            kbuf[b, at] = jnp.where(here, k_new, kbuf[b, at].astype(jnp.float32)).astype(jnp.bfloat16)
            vbuf[b, at] = jnp.where(here, v_new, vbuf[b, at].astype(jnp.float32)).astype(jnp.bfloat16)
        for bb, b in enumerate(members):
            q_even = qf[pl.ds(b, half, stride=2 * seqs), :]
            q_odd = qf[pl.ds(b + seqs, half, stride=2 * seqs), :]
            q_b = jnp.concatenate([q_even, q_odd], axis=0).astype(jnp.bfloat16)
            k_b = kbuf[b].reshape(cols, head_dim)
            sbuf[bb] = lax.dot_general(q_b, k_b, (((1,), (1,)), ((), ())), preferred_element_type=jnp.float32)
        for bb, b in enumerate(members):
            live = slot_key <= pos_ref[b] - start
            s = jnp.where(live, sbuf[bb] * score_scale, NEG_FILL)
            m = jnp.max(s, axis=-1, keepdims=True)
            e = jnp.where(live, jnp.exp(s - m), 0.0)
            l = jnp.sum(e, axis=-1, keepdims=True)
            ebuf[bb] = e.astype(jnp.bfloat16)
            m_acc = jnp.where(lane == b, m, m_acc)
            l_acc = jnp.where(lane == b, l, l_acc)
        for bb, b in enumerate(members):
            obuf[bb] = jnp.dot(ebuf[bb], vbuf[b].reshape(cols, head_dim), preferred_element_type=jnp.float32)
        for bb, b in enumerate(members):
            for par in range(2):
                for i in range(half):
                    part_ref[i, pl.ds(b + par * seqs, 1), :] = obuf[bb, par * half + i:par * half + i + 1, :]
        mstat[...] = m_acc
        lstat[...] = l_acc
        rows = pl.ds(g * per_group, per_group)
        pltpu.make_async_copy(kbuf.at[rows], ko_ref.at[rows], kosem.at[g]).start()
        pltpu.make_async_copy(vbuf.at[rows], vo_ref.at[rows], vosem.at[g]).start()
        pltpu.make_async_copy(new_ref.at[rows], new_out.at[rows], newsem.at[g]).start()
        return carry

    lax.fori_loop(0, groups, group_step, 0)

    for i in range(half):
        base = 2 * seqs
        part_ref[i, base:base + 1, :] = mstat[i:i + 1, :]
        part_ref[i, base + 1:base + 2, :] = mstat[half + i:half + i + 1, :]
        part_ref[i, base + 2:base + 3, :] = lstat[i:i + 1, :]
        part_ref[i, base + 3:base + 4, :] = lstat[half + i:half + i + 1, :]
        part_ref[i, base + 4:base + 8, :] = jnp.zeros((4, 128), jnp.float32)
    for g in range(groups):
        rows = pl.ds(g * per_group, per_group)
        pltpu.make_async_copy(kbuf.at[rows], ko_ref.at[rows], kosem.at[g]).wait()
        pltpu.make_async_copy(vbuf.at[rows], vo_ref.at[rows], vosem.at[g]).wait()
        pltpu.make_async_copy(new_ref.at[rows], new_out.at[rows], newsem.at[g]).wait()


def attend_stage(positions, qf, kf, vf, k_vm, v_vm):
    seqs, slots, kv_heads, head_dim = k_vm.shape
    q_heads = qf.shape[0] // seqs
    groups = 8
    vmem = pl.BlockSpec(memory_space=pltpu.VMEM)
    anyspec = pl.BlockSpec(memory_space=pl.ANY)
    hbm = pl.BlockSpec(memory_space=pltpu.HBM)
    dma = pltpu.SemaphoreType.DMA
    outs = pl.pallas_call(
        attend_kernel,
        name='attend_stage',
        out_shape=(
            jax.ShapeDtypeStruct(k_vm.shape, k_vm.dtype),
            jax.ShapeDtypeStruct(v_vm.shape, v_vm.dtype),
            jax.ShapeDtypeStruct((seqs, 2, kv_heads, head_dim), jnp.bfloat16),
            pltpu.VMEM((q_heads // 2, 2 * seqs + STAT_ROWS, head_dim), jnp.float32),
            pltpu.VMEM(k_vm.shape, k_vm.dtype),
            pltpu.VMEM(v_vm.shape, v_vm.dtype),
        ),
        in_specs=[hbm] + [vmem] * 5,
        out_specs=(anyspec, anyspec, anyspec, vmem, vmem, vmem),
        input_output_aliases={4: 4, 5: 5},
        scratch_shapes=[
            pltpu.SMEM(positions.shape, jnp.int32),
            pltpu.VMEM((seqs, 2, kv_heads, head_dim), jnp.bfloat16),
            pltpu.VMEM((q_heads, 128), jnp.float32),
            pltpu.VMEM((q_heads, 128), jnp.float32),
            pltpu.VMEM((seqs // groups, q_heads, slots * kv_heads), jnp.float32),
            pltpu.VMEM((seqs // groups, q_heads, slots * kv_heads), jnp.bfloat16),
            pltpu.VMEM((seqs // groups, q_heads, head_dim), jnp.float32),
            dma, dma((groups,)), dma((groups,)), dma((groups,)),
        ],
        compiler_params=pltpu.CompilerParams(vmem_limit_bytes=16 * 1024 * 1024),
    )(*in_hbm(positions), qf, kf, vf, k_vm, v_vm)
    return outs[:4]


def combine(pieces, seqs, rows_out, final=False):
    stats = [jnp.transpose(s, (1, 0))[:seqs] for _, s in pieces]
    peak = functools.reduce(jnp.maximum, [t[:, 0:2] for t in stats])
    factors = [jnp.exp(t[:, 0:2] - peak) for t in stats]
    total = functools.reduce(jnp.add, [f * t[:, 2:4] for f, t in zip(factors, stats)])
    outs = []
    for hh in range(2):
        acc = None
        for (o, _), f in zip(pieces, factors):
            term = o[hh * seqs:(hh + 1) * seqs] * f[:, hh:hh + 1]
            acc = term if acc is None else acc + term
        if final:
            acc = acc / total[:, hh:hh + 1]
        outs.append(acc)
    if final:
        return outs, None
    both = jnp.concatenate([peak, total, jnp.zeros((seqs, 4), jnp.float32)], axis=1)
    both = jnp.concatenate([both, jnp.zeros((128 - seqs, 8), jnp.float32)], axis=0)
    return outs, jnp.transpose(both, (1, 0))


def tail_kernel(mine, wo_ref, tok_in, out_ref, tok_ref, toksem, pin, acc, rel, fin, att, wov, res,
                wsem, s0, r0, s1, r1, s2, r2, s3, r3, s4, r4):
    seqs, model = tok_ref.shape
    tok_copy = pltpu.make_async_copy(tok_in, tok_ref, toksem)
    tok_copy.start()
    me = lax.axis_index('sp')
    n = lax.axis_size('sp')
    chips = n // 2
    core, chip = lax.rem(me, 2), me // 2
    c_right, c_left, c_opp = lax.rem(chip + 1, chips), lax.rem(chip + chips - 1, chips), lax.rem(chip + 2, chips)
    partner = chip * 2 + 1 - core
    right, left = c_right * 2 + core, c_left * 2 + core
    body = 2 * seqs
    k_rows = wov.shape[1]

    def wo_copy(k):
        return pltpu.make_async_copy(wo_ref.at[pl.ds(pl.multiple_of(k * k_rows, k_rows), k_rows)], wov.at[k], wsem.at[k])

    barrier = pltpu.get_barrier_semaphore()
    for peer in (partner, right, left):
        pl.semaphore_signal(barrier, inc=1, device_id={'sp': peer}, device_id_type=MESH)
    pl.semaphore_wait(barrier, 3)

    order = (c_opp, c_right, c_left, chip)
    halves = 2 * chips
    sends = []
    pair = []
    for i, c in enumerate(order):
        copy = send(mine.at[pl.ds((1 - core) * halves + 2 * c, 2)], pin.at[i], s0.at[i], r0.at[i], partner)
        pair.append(copy)

    for k in range(2):
        wo_copy(k).start()

    def put(dst, outs, stat):
        for hh in range(2):
            dst[hh * seqs:(hh + 1) * seqs, :] = outs[hh]
        dst[body:body + STAT_ROWS, :] = stat

    def read(ref):
        return ref[0:body, :], ref[body:body + STAT_ROWS, :]

    def merge_pair(i):
        pair[i].wait_recv()
        for h in range(2):
            own = mine.at[core * halves + 2 * order[i] + h]
            put(acc.at[i, h], *combine([read(own), read(pin.at[i, h])], seqs, body))

    merge_pair(0)
    sends.append(send(acc.at[0, 1], rel.at[1], s1.at[1], r1.at[1], right))
    sends.append(send(acc.at[0, 0], rel.at[0], s1.at[0], r1.at[0], left))
    relay_b, relay_a = sends[0], sends[1]
    for k in range(2, 4):
        wo_copy(k).start()
    merge_pair(1)
    fin_left_a = send(acc.at[1, 0], fin.at[0, 0], s2.at[0], r2.at[0], right)
    merge_pair(2)
    fin_right_b = send(acc.at[2, 1], fin.at[1, 1], s2.at[1], r2.at[1], left)
    merge_pair(3)
    for k in range(4, 8):
        wo_copy(k).start()
    relay_b.wait_recv()
    put(fin.at[2, 1], *combine([read(acc.at[1, 1]), read(rel.at[1])], seqs, body))
    fin_left_b = send(fin.at[2, 1], fin.at[0, 1], s2.at[2], r2.at[2], right)
    relay_a.wait_recv()
    put(fin.at[2, 0], *combine([read(acc.at[2, 0]), read(rel.at[0])], seqs, body))
    fin_right_a = send(fin.at[2, 0], fin.at[1, 0], s2.at[3], r2.at[3], left)

    mine_k = core * chips + chip
    for h, (from_left, from_right) in ((0, (fin_left_a, fin_right_a)), (1, (fin_left_b, fin_right_b))):
        from_left.wait_recv()
        from_right.wait_recv()
        outs, _ = combine([read(acc.at[3, h]), read(fin.at[0, h]), read(fin.at[1, h])], seqs, body, final=True)
        for hh in range(2):
            att[mine_k, h, hh * seqs:(hh + 1) * seqs, :] = outs[hh].astype(jnp.bfloat16).astype(jnp.float32)

    k_left, k_right, k_opp = core * chips + c_left, core * chips + c_right, core * chips + c_opp
    o_core = 1 - core
    to_right_b = send(att.at[mine_k, 1], att.at[mine_k, 1], s3.at[0], r3.at[0], right)
    to_left_a = send(att.at[mine_k, 0], att.at[mine_k, 0], s3.at[1], r3.at[1], left)
    to_right_a = send(att.at[mine_k, 0], att.at[mine_k, 0], s3.at[2], r3.at[2], right)
    to_left_b = send(att.at[mine_k, 1], att.at[mine_k, 1], s3.at[3], r3.at[3], left)
    to_partner = send(att.at[mine_k], att.at[mine_k], s3.at[4], r3.at[4], partner)

    cols = 512

    def multiply(k, first=False):
        wo_copy(k).wait()
        lhs = jnp.concatenate([att[k, h, hh * seqs:(hh + 1) * seqs, :] for h in range(2) for hh in range(2)], axis=1)
        lhs = lhs.astype(jnp.bfloat16)

        for i in range(model // cols):
            off = slice(i * cols, (i + 1) * cols)
            y = jnp.dot(lhs, wov[k, :, off], preferred_element_type=jnp.float32)
            res[:, off] = y if first else res[:, off] + y

    multiply(mine_k, first=True)
    to_right_b.wait_recv()
    fwd_right = send(att.at[k_left, 1], att.at[k_left, 1], s4.at[0], r4.at[0], right)
    p1 = send(att.at[k_left, 1], att.at[k_left, 1], s4.at[2], r4.at[2], partner)
    to_left_a.wait_recv()
    fwd_left = send(att.at[k_right, 0], att.at[k_right, 0], s4.at[1], r4.at[1], left)
    p2 = send(att.at[k_right, 0], att.at[k_right, 0], s4.at[3], r4.at[3], partner)
    to_partner.wait_recv()
    multiply(o_core * chips + chip)
    to_right_a.wait_recv()
    p3 = send(att.at[k_left, 0], att.at[k_left, 0], s4.at[4], r4.at[4], partner)
    to_left_b.wait_recv()
    p4 = send(att.at[k_right, 1], att.at[k_right, 1], s4.at[5], r4.at[5], partner)
    multiply(k_left)
    multiply(k_right)
    p1.wait_recv()
    p3.wait_recv()
    multiply(o_core * chips + c_left)
    p2.wait_recv()
    p4.wait_recv()
    multiply(o_core * chips + c_right)
    fwd_right.wait_recv()
    p5 = send(att.at[k_opp, 1], att.at[k_opp, 1], s4.at[6], r4.at[6], partner)
    fwd_left.wait_recv()
    p6 = send(att.at[k_opp, 0], att.at[k_opp, 0], s4.at[7], r4.at[7], partner)
    multiply(k_opp)
    p5.wait_recv()
    p6.wait_recv()
    multiply(o_core * chips + c_opp)
    tok_copy.wait()
    out_ref[...] = (tok_ref[...].astype(jnp.float32) + res[...]).astype(jnp.bfloat16)
    for copy in pair + sends + [fin_left_a, fin_right_b, fin_left_b, fin_right_a, to_right_b, to_left_a, to_right_a,
                                to_left_b, to_partner, fwd_right, fwd_left, p1, p2, p3, p4, p5, p6]:
        copy.wait_send()


def tail_stage(part, w_o, tokens, group):
    seqs, model = tokens.shape
    halves, rows, head_dim = part.shape
    chips = group // 2
    vmem = pl.BlockSpec(memory_space=pltpu.VMEM)
    hbm = pl.BlockSpec(memory_space=pltpu.HBM)
    dma = pltpu.SemaphoreType.DMA
    return pl.pallas_call(
        tail_kernel,
        name='tail_stage',
        out_shape=pltpu.VMEM((seqs, model), jnp.bfloat16),
        in_specs=[vmem, hbm, hbm],
        out_specs=vmem,
        scratch_shapes=[
            pltpu.VMEM((seqs, model), tokens.dtype),
            dma,
            pltpu.VMEM((chips, 2, rows, head_dim), jnp.float32),
            pltpu.VMEM((chips, 2, rows, head_dim), jnp.float32),
            pltpu.VMEM((2, rows, head_dim), jnp.float32),
            pltpu.VMEM((3, 2, rows, head_dim), jnp.float32),
            pltpu.VMEM((group, 2, 2 * seqs, head_dim), jnp.float32),
            pltpu.VMEM((group, w_o.shape[0] // group, model), jnp.bfloat16),
            pltpu.VMEM((seqs, model), jnp.float32),
            dma((group,)),
            dma((chips,)), dma((chips,)), dma((2,)), dma((2,)), dma((4,)), dma((4,)), dma((5,)), dma((5,)), dma((8,)), dma((8,)),
        ],
        compiler_params=pltpu.CompilerParams(collective_id=0, has_side_effects=True, vmem_limit_bytes=44 * 1024 * 1024),
    )(part, *in_hbm(w_o, tokens))


def solution(mesh):
    cache_spec = P('dp', 'sp', None, None)
    group = mesh.shape['sp']

    def device_step(tokens, positions, k_cache, v_cache, w_q, w_k, w_v, w_o, attn_norm, q_norm, k_norm):
        shared = project_stage(tokens, positions, k_cache, v_cache, w_q, w_k, w_v, attn_norm, q_norm, k_norm, group)
        k_upd, v_upd, new_kv, part = attend_stage(positions, *shared)
        block_out = tail_stage(part, w_o, tokens, group)
        return block_out, k_upd, v_upd, new_kv

    return jax.shard_map(device_step, mesh=mesh, in_specs=(P('dp', None), P('dp'), cache_spec, cache_spec, P(), P(), P(), P(), P(), P(), P()), out_specs=(P('dp', None), cache_spec, cache_spec, P('dp', None, None, None)), check_vma=False)
```

```python
import functools

import jax
import jax.numpy as jnp
import numpy as np
from jax import lax
from jax.experimental import pallas as pl
from jax.experimental.pallas import tpu as pltpu
from jax.sharding import PartitionSpec as P

NORM_EPS = 1e-6
ROPE_THETA = 1000000.0
NEG_FILL = -1e30
MESH = pl.DeviceIdType.MESH
STAT_ROWS = 8


def in_hbm(*arrays):
    return [pltpu.with_memory_space_constraint(jnp.asarray(a), pltpu.HBM) for a in arrays]


def rope_frequencies(head_dim):
    inv_freq = ROPE_THETA ** (-np.arange(head_dim // 2, dtype=np.float64) * 2.0 / head_dim)
    return np.concatenate([inv_freq, inv_freq])[None, :].astype(np.float32)


def norm_rope(proj, gain, cos_full, sin_full):
    values = proj.astype(jnp.bfloat16).astype(jnp.float32)
    scale = lax.rsqrt(jnp.mean(values * values, axis=-1, keepdims=True) + NORM_EPS)
    normed = values * scale * gain
    turned = pltpu.roll(normed, normed.shape[-1] // 2, 1)
    return (normed * cos_full + turned * sin_full).astype(jnp.bfloat16).astype(jnp.float32)


def ring_place():
    me = lax.axis_index('sp')
    chips = lax.axis_size('sp') // 2
    core, chip = lax.rem(me, 2), me // 2
    c_right, c_left, c_opp = lax.rem(chip + 1, chips), lax.rem(chip + chips - 1, chips), lax.rem(chip + 2, chips)
    return chips, core, chip, c_right, c_left, c_opp, chip * 2 + 1 - core, c_right * 2 + core, c_left * 2 + core


def enter(peers):
    barrier = pltpu.get_barrier_semaphore()
    for peer in peers:
        pl.semaphore_signal(barrier, inc=1, device_id={'sp': peer}, device_id_type=MESH)
    return lambda: pl.semaphore_wait(barrier, len(peers))


def send(src, dst, ss, rs, peer):
    copy = pltpu.make_async_remote_copy(src_ref=src, dst_ref=dst, send_sem=ss, recv_sem=rs,
                                        device_id={'sp': peer}, device_id_type=MESH)
    copy.start()
    return copy


def project_kernel(pos_in, tok_in, freq_in, an_in, qn_in, kn_in, wq_ref, wk_ref, wv_ref, kc_ref, vc_ref,
                   qf, kf, vf, kbuf, vbuf,
                   pos_ref, tok_ref, freq_ref, an_ref, qn_ref, kn_ref, hid, wbuf, cosb, sinb, insem, wsem, csem, ss, rs):
    seqs, model = tok_ref.shape
    head_dim = qn_ref.shape[-1]
    blocks, _, blk = hid.shape
    width = wbuf.shape[-1]
    heads = width // head_dim
    chips, core, chip, c_right, c_left, c_opp, partner, right, left = ring_place()
    mine_k = core * chips + chip

    smalls = [pltpu.make_async_copy(src, dst, insem.at[j]) for j, (src, dst) in enumerate((
        (tok_in, tok_ref), (pos_in, pos_ref), (freq_in, freq_ref), (an_in, an_ref), (qn_in, qn_ref), (kn_in, kn_ref)))]
    for copy in smalls:
        copy.start()
    bulk = []
    k_left, k_right, k_opp = core * chips + c_left, core * chips + c_right, core * chips + c_opp
    for j, (ref, col) in enumerate(((wq_ref, mine_k), (wq_ref, k_opp), (wk_ref, core), (wv_ref, core))):
        for i in range(blocks):
            src = ref.at[pl.ds(i * blk, blk), pl.ds(pl.multiple_of(col * width, width), width)]
            bulk.append(pltpu.make_async_copy(src, wbuf.at[j, i], wsem.at[j, i]))
    pieces = csem.shape[1]
    per = seqs // pieces
    for g in range(pieces):
        for j, (ref, buf) in enumerate(((kc_ref, kbuf), (vc_ref, vbuf))):
            rows = pl.ds(g * per, per)
            bulk.append(pltpu.make_async_copy(ref.at[rows], buf.at[rows], csem.at[j, g]))
    issued = 0

    def issue(count):
        nonlocal issued
        for copy in bulk[issued:issued + count]:
            copy.start()
        issued += count

    issue(7)
    arrived = enter((partner, right, left))
    for copy in smalls:
        copy.wait()

    lanes = an_ref.shape[1]
    total = jnp.zeros((seqs, lanes), jnp.float32)
    for i in range(model // lanes):
        xf = tok_ref[:, i * lanes:(i + 1) * lanes].astype(jnp.float32)
        total = total + xf * xf
    inv = lax.rsqrt(jnp.sum(total, axis=-1, keepdims=True) / model + NORM_EPS)
    per_blk = blk // lanes
    for i in range(model // lanes):
        xf = tok_ref[:, i * lanes:(i + 1) * lanes].astype(jnp.float32)
        gain = an_ref[i:i + 1, :].astype(jnp.float32)
        hid[i // per_blk, :, (i % per_blk) * lanes:(i % per_blk + 1) * lanes] = (xf * inv * gain).astype(jnp.bfloat16)

    for b in range(seqs):
        cosb[b:b + 1, :] = jnp.full((1, head_dim), pos_ref[b], jnp.int32).astype(jnp.float32)
    angles = cosb[...] * freq_ref[...]
    sign = jnp.where(lax.broadcasted_iota(jnp.int32, angles.shape, 1) < head_dim // 2, -1.0, 1.0)
    sinb[...] = jnp.sin(angles) * sign
    cosb[...] = jnp.cos(angles)
    cos_full, sin_full = cosb[...], sinb[...]

    def project(j, more):
        y = None
        for i in range(blocks):
            bulk[j * blocks + i].wait()
            issue(more)
            part = jnp.dot(hid[i], wbuf[j, i], preferred_element_type=jnp.float32)
            y = part if y is None else y + part
        return [y[:, h * head_dim:(h + 1) * head_dim] for h in range(heads)]

    def put(dst, base, values):
        for h, value in enumerate(values):
            dst[pl.ds(pl.multiple_of(base + h * seqs, seqs), seqs), :] = value

    half_rows = heads // 2 * seqs

    def q_half(k, h):
        return qf.at[pl.ds(pl.multiple_of(k * heads * seqs + h * half_rows, half_rows), half_rows)]

    q_gain = qn_ref[...].astype(jnp.float32)
    put(qf, mine_k * heads * seqs, [norm_rope(p, q_gain, cos_full, sin_full) for p in project(0, 1)])
    arrived()
    count = 0
    sent = []

    def push(ref, peer):
        nonlocal count
        sent.append(send(ref, ref, ss.at[count], rs.at[count], peer))
        count += 1
        return sent[-1]

    own = [[push(q_half(mine_k, h), peer) for peer in (right, left)] for h in range(2)]
    push(q_half(mine_k, 0), partner)
    push(q_half(mine_k, 1), partner)
    put(qf, k_opp * heads * seqs, [norm_rope(p, q_gain, cos_full, sin_full) for p in project(1, 2)])
    push(q_half(k_opp, 0), partner)
    push(q_half(k_opp, 1), partner)

    kv_rows = heads * seqs
    kv_base = core * kv_rows
    kv_part = pl.ds(pl.multiple_of(kv_base, kv_rows), kv_rows)
    k_gain = kn_ref[...].astype(jnp.float32)
    put(kf, kv_base, [norm_rope(p, k_gain, cos_full, sin_full) for p in project(2, 2)])
    push(kf.at[kv_part], partner)
    put(vf, kv_base, [p.astype(jnp.bfloat16).astype(jnp.float32) for p in project(3, 2)])
    push(vf.at[kv_part], partner)
    issue(len(bulk) - issued)

    for h in range(2):
        for from_peer, k in zip(own[h], (k_left, k_right)):
            from_peer.wait_recv()
            push(q_half(k, h), partner)
    waited = own[0] + own[1]
    for copy in sent:
        if not any(copy is w for w in waited):
            copy.wait_recv()
        copy.wait_send()
    for copy in bulk[4 * blocks:]:
        copy.wait()


def project_stage(tokens, positions, k_cache, v_cache, w_q, w_k, w_v, attn_norm, q_norm, k_norm, group):
    seqs, model = tokens.shape
    kv_heads, head_dim = k_cache.shape[2:]
    q_heads = w_q.shape[1] // head_dim
    width = w_q.shape[1] // group
    blocks = 4
    vmem = pl.BlockSpec(memory_space=pltpu.VMEM)
    hbm = pl.BlockSpec(memory_space=pltpu.HBM)
    dma = pltpu.SemaphoreType.DMA
    return pl.pallas_call(
        project_kernel,
        name='project_stage',
        out_shape=(
            pltpu.VMEM((q_heads * seqs, head_dim), jnp.float32),
            pltpu.VMEM((kv_heads * seqs, head_dim), jnp.float32),
            pltpu.VMEM((kv_heads * seqs, head_dim), jnp.float32),
            pltpu.VMEM(k_cache.shape, k_cache.dtype),
            pltpu.VMEM(v_cache.shape, v_cache.dtype),
        ),
        in_specs=[hbm] * 11,
        out_specs=(vmem,) * 5,
        scratch_shapes=[
            pltpu.SMEM(positions.shape, jnp.int32),
            pltpu.VMEM(tokens.shape, tokens.dtype),
            pltpu.VMEM((1, head_dim), jnp.float32),
            pltpu.VMEM((model // 128, 128), attn_norm.dtype),
            pltpu.VMEM((1, head_dim), q_norm.dtype),
            pltpu.VMEM((1, head_dim), k_norm.dtype),
            pltpu.VMEM((blocks, seqs, model // blocks), jnp.bfloat16),
            pltpu.VMEM((4, blocks, model // blocks, width), jnp.bfloat16),
            pltpu.VMEM((seqs, head_dim), jnp.float32),
            pltpu.VMEM((seqs, head_dim), jnp.float32),
            dma((6,)), dma((4, blocks)), dma((2, 8)), dma((16,)), dma((16,)),
        ],
        compiler_params=pltpu.CompilerParams(collective_id=1, has_side_effects=True, vmem_limit_bytes=24 * 1024 * 1024),
    )(*in_hbm(positions, tokens, rope_frequencies(head_dim), attn_norm.reshape(-1, 128), q_norm[None, :], k_norm[None, :],
              w_q, w_k, w_v, k_cache, v_cache))


def attend_kernel(pos_in, qf, kf, vf, k_in, v_in, ko_ref, vo_ref, new_out, part_ref, kbuf, vbuf,
                  pos_ref, new_ref, mstat, lstat, sbuf, ebuf, obuf, possem, newsem, kosem, vosem):
    seqs, slots, kv_heads, head_dim = kbuf.shape
    groups = kosem.shape[0]
    per_group = seqs // groups
    q_heads = qf.shape[0] // seqs
    start = lax.axis_index('sp') * slots
    pos_copy = pltpu.make_async_copy(pos_in, pos_ref, possem)
    pos_copy.start()
    pos_copy.wait()

    def write_step(g, carry):
        for bb in range(per_group):
            b = g * per_group + bb
            local = pos_ref[b] - start
            here = (local >= 0) & (local < slots)
            at = jnp.clip(local, 0, slots - 1)
            k_new = kf[pl.ds(b, kv_heads, stride=seqs), :]
            v_new = vf[pl.ds(b, kv_heads, stride=seqs), :]
            new_ref[b, 0] = k_new.astype(jnp.bfloat16)
            new_ref[b, 1] = v_new.astype(jnp.bfloat16)
            kbuf[b, at] = jnp.where(here, k_new, kbuf[b, at].astype(jnp.float32)).astype(jnp.bfloat16)
            vbuf[b, at] = jnp.where(here, v_new, vbuf[b, at].astype(jnp.float32)).astype(jnp.bfloat16)
        for copy in writes(g):
            copy.start()
        return carry

    def writes(g):
        rows = pl.ds(g * per_group, per_group)
        return (pltpu.make_async_copy(kbuf.at[rows], ko_ref.at[rows], kosem.at[g]),
                pltpu.make_async_copy(vbuf.at[rows], vo_ref.at[rows], vosem.at[g]),
                pltpu.make_async_copy(new_ref.at[rows], new_out.at[rows], newsem.at[g]))

    lax.fori_loop(0, groups, write_step, 0)

    cols = slots * kv_heads
    row_id = lax.broadcasted_iota(jnp.int32, (q_heads, cols), 0)
    col_id = lax.broadcasted_iota(jnp.int32, (q_heads, cols), 1)
    head_ok = row_id // (q_heads // kv_heads) == col_id % kv_heads
    slot_key = jnp.where(head_ok, col_id // kv_heads, slots * 1024)
    lane = lax.broadcasted_iota(jnp.int32, (q_heads, 128), 1)
    score_scale = head_dim ** -0.5
    mstat[...] = jnp.zeros_like(mstat)
    lstat[...] = jnp.zeros_like(lstat)

    def group_step(g, carry):
        m_acc, l_acc = mstat[...], lstat[...]
        members = [g * per_group + bb for bb in range(per_group)]
        for bb, b in enumerate(members):
            q_b = qf[pl.ds(b, q_heads, stride=seqs), :].astype(jnp.bfloat16)
            k_b = kbuf[b].reshape(cols, head_dim)
            sbuf[bb] = lax.dot_general(q_b, k_b, (((1,), (1,)), ((), ())), preferred_element_type=jnp.float32)
        for bb, b in enumerate(members):
            live = slot_key <= pos_ref[b] - start
            s = jnp.where(live, sbuf[bb] * score_scale, NEG_FILL)
            m = jnp.max(s, axis=-1, keepdims=True)
            e = jnp.where(live, jnp.exp(s - m), 0.0)
            l = jnp.sum(e, axis=-1, keepdims=True)
            ebuf[bb] = e.astype(jnp.bfloat16)
            m_acc = jnp.where(lane == b, m, m_acc)
            l_acc = jnp.where(lane == b, l, l_acc)
        for bb, b in enumerate(members):
            obuf[bb] = jnp.dot(ebuf[bb], vbuf[b].reshape(cols, head_dim), preferred_element_type=jnp.float32)
        for bb, b in enumerate(members):
            for h in range(q_heads):
                part_ref[h, pl.ds(b, 1), :] = obuf[bb, h:h + 1, :]
        mstat[...] = m_acc
        lstat[...] = l_acc
        return carry

    lax.fori_loop(0, groups, group_step, 0)

    for h in range(q_heads):
        part_ref[h, seqs:seqs + 1, :] = mstat[h:h + 1, :]
        part_ref[h, seqs + 1:seqs + 2, :] = lstat[h:h + 1, :]
        part_ref[h, seqs + 2:seqs + STAT_ROWS, :] = jnp.zeros((STAT_ROWS - 2, 128), jnp.float32)
    for g in range(groups):
        for copy in writes(g):
            copy.wait()


def attend_stage(positions, qf, kf, vf, k_vm, v_vm):
    seqs, slots, kv_heads, head_dim = k_vm.shape
    q_heads = qf.shape[0] // seqs
    groups = 8
    vmem = pl.BlockSpec(memory_space=pltpu.VMEM)
    anyspec = pl.BlockSpec(memory_space=pl.ANY)
    hbm = pl.BlockSpec(memory_space=pltpu.HBM)
    dma = pltpu.SemaphoreType.DMA
    outs = pl.pallas_call(
        attend_kernel,
        name='attend_stage',
        out_shape=(
            jax.ShapeDtypeStruct(k_vm.shape, k_vm.dtype),
            jax.ShapeDtypeStruct(v_vm.shape, v_vm.dtype),
            jax.ShapeDtypeStruct((seqs, 2, kv_heads, head_dim), jnp.bfloat16),
            pltpu.VMEM((q_heads, seqs + STAT_ROWS, head_dim), jnp.float32),
            pltpu.VMEM(k_vm.shape, k_vm.dtype),
            pltpu.VMEM(v_vm.shape, v_vm.dtype),
        ),
        in_specs=[hbm] + [vmem] * 5,
        out_specs=(anyspec, anyspec, anyspec, vmem, vmem, vmem),
        input_output_aliases={4: 4, 5: 5},
        scratch_shapes=[
            pltpu.SMEM(positions.shape, jnp.int32),
            pltpu.VMEM((seqs, 2, kv_heads, head_dim), jnp.bfloat16),
            pltpu.VMEM((q_heads, 128), jnp.float32),
            pltpu.VMEM((q_heads, 128), jnp.float32),
            pltpu.VMEM((seqs // groups, q_heads, slots * kv_heads), jnp.float32),
            pltpu.VMEM((seqs // groups, q_heads, slots * kv_heads), jnp.bfloat16),
            pltpu.VMEM((seqs // groups, q_heads, head_dim), jnp.float32),
            dma, dma((groups,)), dma((groups,)), dma((groups,)),
        ],
        compiler_params=pltpu.CompilerParams(vmem_limit_bytes=16 * 1024 * 1024),
    )(*in_hbm(positions), qf, kf, vf, k_vm, v_vm)
    return outs[:4]


def merge(pieces, seqs, final=False):
    stats = [jnp.transpose(ref[seqs:seqs + STAT_ROWS, :], (1, 0))[:seqs] for ref in pieces]
    peak = functools.reduce(jnp.maximum, [t[:, 0:1] for t in stats])
    factors = [jnp.exp(t[:, 0:1] - peak) for t in stats]
    total = functools.reduce(jnp.add, [f * t[:, 1:2] for f, t in zip(factors, stats)])
    rows = functools.reduce(jnp.add, [f * ref[0:seqs, :] for f, ref in zip(factors, pieces)])
    if final:
        return rows / total
    both = jnp.concatenate([peak, total, jnp.zeros((seqs, STAT_ROWS - 2), jnp.float32)], axis=1)
    both = jnp.concatenate([both, jnp.zeros((128 - seqs, STAT_ROWS), jnp.float32)], axis=0)
    return rows, jnp.transpose(both, (1, 0))


def tail_kernel(mine, wo_ref, tok_in, out_ref, tok_ref, toksem, pin, away, kept, in1, out2, in2, att, wov, res,
                wsem, s0, r0, s1, r1, s2, r2, s3, r3, s4, r4, s5, r5):
    seqs, model = tok_ref.shape
    per = away.shape[1]
    tok_copy = pltpu.make_async_copy(tok_in, tok_ref, toksem)
    tok_copy.start()
    chips, core, chip, _, _, _, partner, _, _ = ring_place()
    near, far = chip + 1 - 2 * lax.rem(chip, 2), chips - 1 - chip
    first = (near * 2 + core, far * 2 + core)
    second = (first[1], first[0])
    sel = (lax.rem((chip + 1) // 2, 2), chip // 2)
    keep = [2 * c + sel[c] for c in range(2)]
    give = [2 * c + 1 - sel[c] for c in range(2)]
    arrived = enter((partner, first[0], first[1]))
    k_rows = wov.shape[1]

    def wo_copy(k):
        return pltpu.make_async_copy(wo_ref.at[pl.ds(pl.multiple_of(k * k_rows, k_rows), k_rows)], wov.at[k], wsem.at[k])

    arrived()
    sent = []

    def push(src, dst, ss, rs, peer):
        sent.append(send(src, dst, ss, rs, peer))
        return sent[-1]

    order = give + keep
    heads = per * 4
    pair = [push(mine.at[pl.ds((1 - core) * heads + q * per, per)], pin.at[i], s0.at[i], r0.at[i], partner)
            for i, q in enumerate(order)]
    for k in range(2):
        wo_copy(k).start()

    def put(dst, merged):
        rows, stat = merged
        dst[0:seqs, :] = rows
        dst[seqs:seqs + STAT_ROWS, :] = stat

    pair[0].wait_recv()
    pair[1].wait_recv()
    step1 = [[], []]
    for i in range(per):
        for c in range(2):
            put(away.at[c, i], merge([mine.at[core * heads + give[c] * per + i], pin.at[c, i]], seqs))
        for c in range(2):
            step1[c].append(push(away.at[c, i], in1.at[c, i], s1.at[c, i], r1.at[c, i], first[c]))
    for k in range(2, 8):
        wo_copy(k).start()
    pair[2].wait_recv()
    pair[3].wait_recv()
    for i in range(per):
        for c in range(2):
            put(kept.at[c, i], merge([mine.at[core * heads + keep[c] * per + i], pin.at[2 + c, i]], seqs))
    step2 = [[], []]
    for i in range(per):
        for c in range(2):
            step1[c][i].wait_recv()
        for c in range(2):
            put(out2.at[c, i], merge([kept.at[c, i], in1.at[c, i]], seqs))
        for c in range(2):
            step2[c].append(push(out2.at[c, i], in2.at[c, i], s2.at[c, i], r2.at[c, i], second[c]))
    step3, own = [[], []], [[], []]
    blocks = [core * 4 + keep[c] for c in range(2)]

    def rows_of(k, i):
        return att.at[k, pl.ds(i * seqs, seqs)]

    for i in range(per):
        for c in range(2):
            step2[c][i].wait_recv()
        for c in range(2):
            done = merge([out2.at[c, i], in2.at[c, i]], seqs, final=True)
            att[blocks[c], i * seqs:(i + 1) * seqs, :] = done.astype(jnp.bfloat16).astype(jnp.float32)
        for c in range(2):
            piece = rows_of(blocks[c], i)
            step3[c].append(push(piece, piece, s3.at[c, i], r3.at[c, i], first[c]))
            own[c].append(push(piece, piece, s4.at[c, i], r4.at[c, i], partner))

    cols = 512

    def multiply(k, fresh=False):
        wo_copy(k).wait()
        lhs = jnp.concatenate([att[k, i * seqs:(i + 1) * seqs, :] for i in range(per)], axis=1).astype(jnp.bfloat16)
        for i in range(model // cols):
            off = slice(i * cols, (i + 1) * cols)
            y = jnp.dot(lhs, wov[k, :, off], preferred_element_type=jnp.float32)
            res[:, off] = y if fresh else res[:, off] + y

    other = (1 - core) * 4
    multiply(blocks[0], fresh=True)
    multiply(blocks[1])
    for c in range(2):
        for i in range(per):
            own[c][i].wait_recv()
        multiply(other + keep[c])
    passed = [[], []]
    for i in range(per):
        for c in range(2):
            step3[c][i].wait_recv()
            piece = rows_of(core * 4 + give[c], i)
            passed[c].append(push(piece, piece, s5.at[c, i], r5.at[c, i], partner))
    for c in range(2):
        multiply(core * 4 + give[c])
    for c in range(2):
        for i in range(per):
            passed[c][i].wait_recv()
        multiply(other + give[c])
    tok_copy.wait()
    out_ref[...] = (tok_ref[...].astype(jnp.float32) + res[...]).astype(jnp.bfloat16)
    for copy in sent:
        copy.wait_send()


def tail_stage(part, w_o, tokens, group):
    seqs, model = tokens.shape
    q_heads, rows, head_dim = part.shape
    per = q_heads // group
    vmem = pl.BlockSpec(memory_space=pltpu.VMEM)
    hbm = pl.BlockSpec(memory_space=pltpu.HBM)
    dma = pltpu.SemaphoreType.DMA
    sums = pltpu.VMEM((2, per, rows, head_dim), jnp.float32)
    return pl.pallas_call(
        tail_kernel,
        name='tail_stage',
        out_shape=pltpu.VMEM((seqs, model), jnp.bfloat16),
        in_specs=[vmem, hbm, hbm],
        out_specs=vmem,
        scratch_shapes=[
            pltpu.VMEM((seqs, model), tokens.dtype),
            dma,
            pltpu.VMEM((4, per, rows, head_dim), jnp.float32),
            sums, sums, sums, sums, sums,
            pltpu.VMEM((group, per * seqs, head_dim), jnp.float32),
            pltpu.VMEM((group, w_o.shape[0] // group, model), jnp.bfloat16),
            pltpu.VMEM((seqs, model), jnp.float32),
            dma((group,)), dma((4,)), dma((4,)),
        ] + [dma((2, per))] * 10,
        compiler_params=pltpu.CompilerParams(collective_id=0, has_side_effects=True, vmem_limit_bytes=44 * 1024 * 1024),
    )(part, *in_hbm(w_o, tokens))


def solution(mesh):
    cache_spec = P('dp', 'sp', None, None)
    group = mesh.shape['sp']

    def device_step(tokens, positions, k_cache, v_cache, w_q, w_k, w_v, w_o, attn_norm, q_norm, k_norm):
        shared = project_stage(tokens, positions, k_cache, v_cache, w_q, w_k, w_v, attn_norm, q_norm, k_norm, group)
        k_upd, v_upd, new_kv, part = attend_stage(positions, *shared)
        block_out = tail_stage(part, w_o, tokens, group)
        return block_out, k_upd, v_upd, new_kv

    return jax.shard_map(device_step, mesh=mesh, in_specs=(P('dp', None), P('dp'), cache_spec, cache_spec, P(), P(), P(), P(), P(), P(), P()), out_specs=(P('dp', None), cache_spec, cache_spec, P('dp', None, None, None)), check_vma=False)
```

```python
import functools

import jax
import jax.numpy as jnp
import numpy as np
from jax import lax
from jax.experimental import pallas as pl
from jax.experimental.pallas import tpu as pltpu
from jax.sharding import PartitionSpec as P

NORM_EPS = 1e-6
ROPE_THETA = 1000000.0
NEG_FILL = -1e30
MESH = pl.DeviceIdType.MESH
STAT_ROWS = 8


def in_hbm(*arrays):
    return [pltpu.with_memory_space_constraint(jnp.asarray(a), pltpu.HBM) for a in arrays]


def rope_frequencies(head_dim):
    inv_freq = ROPE_THETA ** (-np.arange(head_dim // 2, dtype=np.float64) * 2.0 / head_dim)
    return np.concatenate([inv_freq, inv_freq])[None, :].astype(np.float32)


def norm_rope(proj, gain, cos_full, sin_full):
    values = proj.astype(jnp.bfloat16).astype(jnp.float32)
    scale = lax.rsqrt(jnp.mean(values * values, axis=-1, keepdims=True) + NORM_EPS)
    normed = values * scale * gain
    turned = pltpu.roll(normed, normed.shape[-1] // 2, 1)
    return (normed * cos_full + turned * sin_full).astype(jnp.bfloat16).astype(jnp.float32)


def ring_place():
    me = lax.axis_index('sp')
    chips = lax.axis_size('sp') // 2
    core, chip = lax.rem(me, 2), me // 2
    c_right, c_left, c_opp = lax.rem(chip + 1, chips), lax.rem(chip + chips - 1, chips), lax.rem(chip + 2, chips)
    return chips, core, chip, c_right, c_left, c_opp, chip * 2 + 1 - core, c_right * 2 + core, c_left * 2 + core


def enter(peers):
    barrier = pltpu.get_barrier_semaphore()
    for peer in peers:
        pl.semaphore_signal(barrier, inc=1, device_id={'sp': peer}, device_id_type=MESH)
    return lambda: pl.semaphore_wait(barrier, len(peers))


def send(src, dst, ss, rs, peer):
    copy = pltpu.make_async_remote_copy(src_ref=src, dst_ref=dst, send_sem=ss, recv_sem=rs,
                                        device_id={'sp': peer}, device_id_type=MESH)
    copy.start()
    return copy


def project_kernel(pos_in, tok_in, freq_in, an_in, qn_in, kn_in, wq_ref, wk_ref, wv_ref, kc_ref, vc_ref,
                   qf, kf, vf, kbuf, vbuf,
                   pos_ref, tok_ref, freq_ref, an_ref, qn_ref, kn_ref, hid, wbuf, cosb, sinb, insem, wsem, csem, ss, rs):
    seqs, model = tok_ref.shape
    head_dim = qn_ref.shape[-1]
    blocks, _, blk = hid.shape
    width = wbuf.shape[-1]
    heads = width // head_dim
    chips, core, chip, c_right, c_left, c_opp, partner, right, left = ring_place()
    mine_k = core * chips + chip

    smalls = [pltpu.make_async_copy(src, dst, insem.at[j]) for j, (src, dst) in enumerate((
        (tok_in, tok_ref), (pos_in, pos_ref), (freq_in, freq_ref), (an_in, an_ref), (qn_in, qn_ref), (kn_in, kn_ref)))]
    for copy in smalls:
        copy.start()
    bulk = []
    k_left, k_right, k_opp = core * chips + c_left, core * chips + c_right, core * chips + c_opp
    for j, (ref, col) in enumerate(((wq_ref, mine_k), (wq_ref, k_opp), (wk_ref, core), (wv_ref, core))):
        for i in range(blocks):
            src = ref.at[pl.ds(i * blk, blk), pl.ds(pl.multiple_of(col * width, width), width)]
            bulk.append(pltpu.make_async_copy(src, wbuf.at[j, i], wsem.at[j, i]))
    pieces = csem.shape[1]
    per = seqs // pieces
    for g in range(pieces):
        for j, (ref, buf) in enumerate(((kc_ref, kbuf), (vc_ref, vbuf))):
            rows = pl.ds(g * per, per)
            bulk.append(pltpu.make_async_copy(ref.at[rows], buf.at[rows], csem.at[j, g]))
    issued = 0

    def issue(count):
        nonlocal issued
        for copy in bulk[issued:issued + count]:
            copy.start()
        issued += count

    issue(8)
    arrived = enter((partner, right, left))
    for copy in smalls:
        copy.wait()

    lanes = an_ref.shape[1]
    total = jnp.zeros((seqs, lanes), jnp.float32)
    for i in range(model // lanes):
        xf = tok_ref[:, i * lanes:(i + 1) * lanes].astype(jnp.float32)
        total = total + xf * xf
    inv = lax.rsqrt(jnp.sum(total, axis=-1, keepdims=True) / model + NORM_EPS)
    per_blk = blk // lanes
    for i in range(model // lanes):
        xf = tok_ref[:, i * lanes:(i + 1) * lanes].astype(jnp.float32)
        gain = an_ref[i:i + 1, :].astype(jnp.float32)
        hid[i // per_blk, :, (i % per_blk) * lanes:(i % per_blk + 1) * lanes] = (xf * inv * gain).astype(jnp.bfloat16)

    for b in range(seqs):
        cosb[b:b + 1, :] = jnp.full((1, head_dim), pos_ref[b], jnp.int32).astype(jnp.float32)
    angles = cosb[...] * freq_ref[...]
    sign = jnp.where(lax.broadcasted_iota(jnp.int32, angles.shape, 1) < head_dim // 2, -1.0, 1.0)
    sinb[...] = jnp.sin(angles) * sign
    cosb[...] = jnp.cos(angles)
    cos_full, sin_full = cosb[...], sinb[...]

    def project(j, more):
        y = None
        for i in range(blocks):
            bulk[j * blocks + i].wait()
            issue(more)
            part = jnp.dot(hid[i], wbuf[j, i], preferred_element_type=jnp.float32)
            y = part if y is None else y + part
        return [y[:, h * head_dim:(h + 1) * head_dim] for h in range(heads)]

    def put(dst, base, values):
        for h, value in enumerate(values):
            dst[pl.ds(pl.multiple_of(base + h * seqs, seqs), seqs), :] = value

    half_rows = heads // 2 * seqs

    def q_half(k, h):
        return qf.at[pl.ds(pl.multiple_of(k * heads * seqs + h * half_rows, half_rows), half_rows)]

    q_gain = qn_ref[...].astype(jnp.float32)
    put(qf, mine_k * heads * seqs, [norm_rope(p, q_gain, cos_full, sin_full) for p in project(0, 2)])
    arrived()
    count = 0
    sent = []

    def push(ref, peer):
        nonlocal count
        sent.append(send(ref, ref, ss.at[count], rs.at[count], peer))
        count += 1
        return sent[-1]

    own = [[push(q_half(mine_k, h), peer) for peer in (right, left)] for h in range(2)]
    push(q_half(mine_k, 0), partner)
    push(q_half(mine_k, 1), partner)
    put(qf, k_opp * heads * seqs, [norm_rope(p, q_gain, cos_full, sin_full) for p in project(1, 4)])
    push(q_half(k_opp, 0), partner)
    push(q_half(k_opp, 1), partner)

    kv_rows = heads * seqs
    kv_base = core * kv_rows
    kv_part = pl.ds(pl.multiple_of(kv_base, kv_rows), kv_rows)
    k_gain = kn_ref[...].astype(jnp.float32)
    put(kf, kv_base, [norm_rope(p, k_gain, cos_full, sin_full) for p in project(2, 2)])
    push(kf.at[kv_part], partner)
    put(vf, kv_base, [p.astype(jnp.bfloat16).astype(jnp.float32) for p in project(3, 2)])
    push(vf.at[kv_part], partner)
    issue(len(bulk) - issued)

    for h in range(2):
        for from_peer, k in zip(own[h], (k_left, k_right)):
            from_peer.wait_recv()
            push(q_half(k, h), partner)
    waited = own[0] + own[1]
    for copy in sent:
        if not any(copy is w for w in waited):
            copy.wait_recv()
        copy.wait_send()
    for copy in bulk[4 * blocks:]:
        copy.wait()


def project_stage(tokens, positions, k_cache, v_cache, w_q, w_k, w_v, attn_norm, q_norm, k_norm, group):
    seqs, model = tokens.shape
    kv_heads, head_dim = k_cache.shape[2:]
    q_heads = w_q.shape[1] // head_dim
    width = w_q.shape[1] // group
    blocks = 4
    vmem = pl.BlockSpec(memory_space=pltpu.VMEM)
    hbm = pl.BlockSpec(memory_space=pltpu.HBM)
    dma = pltpu.SemaphoreType.DMA
    return pl.pallas_call(
        project_kernel,
        name='project_stage',
        out_shape=(
            pltpu.VMEM((q_heads * seqs, head_dim), jnp.float32),
            pltpu.VMEM((kv_heads * seqs, head_dim), jnp.float32),
            pltpu.VMEM((kv_heads * seqs, head_dim), jnp.float32),
            pltpu.VMEM(k_cache.shape, k_cache.dtype),
            pltpu.VMEM(v_cache.shape, v_cache.dtype),
        ),
        in_specs=[hbm] * 11,
        out_specs=(vmem,) * 5,
        scratch_shapes=[
            pltpu.SMEM(positions.shape, jnp.int32),
            pltpu.VMEM(tokens.shape, tokens.dtype),
            pltpu.VMEM((1, head_dim), jnp.float32),
            pltpu.VMEM((model // 128, 128), attn_norm.dtype),
            pltpu.VMEM((1, head_dim), q_norm.dtype),
            pltpu.VMEM((1, head_dim), k_norm.dtype),
            pltpu.VMEM((blocks, seqs, model // blocks), jnp.bfloat16),
            pltpu.VMEM((4, blocks, model // blocks, width), jnp.bfloat16),
            pltpu.VMEM((seqs, head_dim), jnp.float32),
            pltpu.VMEM((seqs, head_dim), jnp.float32),
            dma((6,)), dma((4, blocks)), dma((2, 8)), dma((16,)), dma((16,)),
        ],
        compiler_params=pltpu.CompilerParams(collective_id=1, has_side_effects=True, vmem_limit_bytes=24 * 1024 * 1024),
    )(*in_hbm(positions, tokens, rope_frequencies(head_dim), attn_norm.reshape(-1, 128), q_norm[None, :], k_norm[None, :],
              w_q, w_k, w_v, k_cache, v_cache))


def attend_kernel(pos_in, qf, kf, vf, k_in, v_in, ko_ref, vo_ref, new_out, part_ref, kbuf, vbuf,
                  pos_ref, new_ref, mstat, lstat, sbuf, ebuf, possem, newsem, kosem, vosem):
    seqs, slots, kv_heads, head_dim = kbuf.shape
    groups = kosem.shape[0]
    per_group = seqs // groups
    q_heads = qf.shape[0] // seqs
    start = lax.axis_index('sp') * slots
    pos_copy = pltpu.make_async_copy(pos_in, pos_ref, possem)
    pos_copy.start()
    pos_copy.wait()

    def write_step(g, carry):
        for bb in range(per_group):
            b = g * per_group + bb
            local = pos_ref[b] - start
            here = (local >= 0) & (local < slots)
            at = jnp.clip(local, 0, slots - 1)
            k_new = kf[pl.ds(b, kv_heads, stride=seqs), :]
            v_new = vf[pl.ds(b, kv_heads, stride=seqs), :]
            new_ref[b, 0] = k_new.astype(jnp.bfloat16)
            new_ref[b, 1] = v_new.astype(jnp.bfloat16)
            kbuf[b, at] = jnp.where(here, k_new, kbuf[b, at].astype(jnp.float32)).astype(jnp.bfloat16)
            vbuf[b, at] = jnp.where(here, v_new, vbuf[b, at].astype(jnp.float32)).astype(jnp.bfloat16)
        for copy in writes(g):
            copy.start()
        return carry

    def writes(g):
        rows = pl.ds(g * per_group, per_group)
        return (pltpu.make_async_copy(kbuf.at[rows], ko_ref.at[rows], kosem.at[g]),
                pltpu.make_async_copy(vbuf.at[rows], vo_ref.at[rows], vosem.at[g]),
                pltpu.make_async_copy(new_ref.at[rows], new_out.at[rows], newsem.at[g]))

    lax.fori_loop(0, groups, write_step, 0)

    cols = slots * kv_heads
    row_id = lax.broadcasted_iota(jnp.int32, (q_heads, cols), 0)
    col_id = lax.broadcasted_iota(jnp.int32, (q_heads, cols), 1)
    head_ok = row_id // (q_heads // kv_heads) == col_id % kv_heads
    slot_key = jnp.where(head_ok, col_id // kv_heads, slots * 1024)
    lane = lax.broadcasted_iota(jnp.int32, (q_heads, 128), 1)
    score_scale = head_dim ** -0.5
    mstat[...] = jnp.zeros_like(mstat)
    lstat[...] = jnp.zeros_like(lstat)

    def group_step(g, carry):
        m_acc, l_acc = mstat[...], lstat[...]
        members = [g * per_group + bb for bb in range(per_group)]
        for bb, b in enumerate(members):
            q_b = qf[pl.ds(b, q_heads, stride=seqs), :].astype(jnp.bfloat16)
            k_b = kbuf[b].reshape(cols, head_dim)
            sbuf[bb] = lax.dot_general(q_b, k_b, (((1,), (1,)), ((), ())), preferred_element_type=jnp.float32)
        for bb, b in enumerate(members):
            live = slot_key <= pos_ref[b] - start
            s = jnp.where(live, sbuf[bb] * score_scale, NEG_FILL)
            m = jnp.max(s, axis=-1, keepdims=True)
            e = jnp.where(live, jnp.exp(s - m), 0.0)
            l = jnp.sum(e, axis=-1, keepdims=True)
            ebuf[bb] = e.astype(jnp.bfloat16)
            m_acc = jnp.where(lane == b, m, m_acc)
            l_acc = jnp.where(lane == b, l, l_acc)
        for bb, b in enumerate(members):
            o = jnp.dot(ebuf[bb], vbuf[b].reshape(cols, head_dim), preferred_element_type=jnp.float32)
            part_ref[pl.ds(b, q_heads, stride=seqs + STAT_ROWS), :] = o
        mstat[...] = m_acc
        lstat[...] = l_acc
        return carry

    lax.fori_loop(0, groups, group_step, 0)

    for h in range(q_heads):
        row = h * (seqs + STAT_ROWS) + seqs
        part_ref[row:row + 1, :] = mstat[h:h + 1, :]
        part_ref[row + 1:row + 2, :] = lstat[h:h + 1, :]
        part_ref[row + 2:row + STAT_ROWS, :] = jnp.zeros((STAT_ROWS - 2, 128), jnp.float32)
    for g in range(groups):
        for copy in writes(g):
            copy.wait()


def attend_stage(positions, qf, kf, vf, k_vm, v_vm):
    seqs, slots, kv_heads, head_dim = k_vm.shape
    q_heads = qf.shape[0] // seqs
    groups = 4
    vmem = pl.BlockSpec(memory_space=pltpu.VMEM)
    anyspec = pl.BlockSpec(memory_space=pl.ANY)
    hbm = pl.BlockSpec(memory_space=pltpu.HBM)
    dma = pltpu.SemaphoreType.DMA
    outs = pl.pallas_call(
        attend_kernel,
        name='attend_stage',
        out_shape=(
            jax.ShapeDtypeStruct(k_vm.shape, k_vm.dtype),
            jax.ShapeDtypeStruct(v_vm.shape, v_vm.dtype),
            jax.ShapeDtypeStruct((seqs, 2, kv_heads, head_dim), jnp.bfloat16),
            pltpu.VMEM((q_heads * (seqs + STAT_ROWS), head_dim), jnp.float32),
            pltpu.VMEM(k_vm.shape, k_vm.dtype),
            pltpu.VMEM(v_vm.shape, v_vm.dtype),
        ),
        in_specs=[hbm] + [vmem] * 5,
        out_specs=(anyspec, anyspec, anyspec, vmem, vmem, vmem),
        input_output_aliases={4: 4, 5: 5},
        scratch_shapes=[
            pltpu.SMEM(positions.shape, jnp.int32),
            pltpu.VMEM((seqs, 2, kv_heads, head_dim), jnp.bfloat16),
            pltpu.VMEM((q_heads, 128), jnp.float32),
            pltpu.VMEM((q_heads, 128), jnp.float32),
            pltpu.VMEM((seqs // groups, q_heads, slots * kv_heads), jnp.float32),
            pltpu.VMEM((seqs // groups, q_heads, slots * kv_heads), jnp.bfloat16),
            dma, dma((groups,)), dma((groups,)), dma((groups,)),
        ],
        compiler_params=pltpu.CompilerParams(vmem_limit_bytes=16 * 1024 * 1024),
    )(*in_hbm(positions), qf, kf, vf, k_vm, v_vm)
    return outs[:4]


def merge(pieces, seqs, final=False):
    stats = [jnp.transpose(ref[seqs:seqs + STAT_ROWS, :], (1, 0))[:seqs] for ref in pieces]
    peak = functools.reduce(jnp.maximum, [t[:, 0:1] for t in stats])
    factors = [jnp.exp(t[:, 0:1] - peak) for t in stats]
    total = functools.reduce(jnp.add, [f * t[:, 1:2] for f, t in zip(factors, stats)])
    rows = functools.reduce(jnp.add, [f * ref[0:seqs, :] for f, ref in zip(factors, pieces)])
    if final:
        return rows / total
    both = jnp.concatenate([peak, total, jnp.zeros((seqs, STAT_ROWS - 2), jnp.float32)], axis=1)
    both = jnp.concatenate([both, jnp.zeros((128 - seqs, STAT_ROWS), jnp.float32)], axis=0)
    return rows, jnp.transpose(both, (1, 0))


def tail_kernel(mine, wo_ref, tok_in, out_ref, tok_ref, toksem, pin, away, kept, in1, out2, in2, att, wov, res,
                wsem, s0, r0, s1, r1, s2, r2, s3, r3, s4, r4, s5, r5):
    seqs, model = tok_ref.shape
    per = away.shape[1]
    tok_copy = pltpu.make_async_copy(tok_in, tok_ref, toksem)
    tok_copy.start()
    chips, core, chip, _, _, _, partner, _, _ = ring_place()
    near, far = chip + 1 - 2 * lax.rem(chip, 2), chips - 1 - chip
    first = (near * 2 + core, far * 2 + core)
    second = (first[1], first[0])
    sel = (lax.rem((chip + 1) // 2, 2), chip // 2)
    keep = [2 * c + sel[c] for c in range(2)]
    give = [2 * c + 1 - sel[c] for c in range(2)]
    arrived = enter((partner, first[0], first[1]))
    k_rows = wov.shape[1]

    def wo_copy(k):
        return pltpu.make_async_copy(wo_ref.at[pl.ds(pl.multiple_of(k * k_rows, k_rows), k_rows)], wov.at[k], wsem.at[k])

    other = (1 - core) * 4
    for k in [core * 4 + q for q in keep] + [other + q for q in keep] + [core * 4 + q for q in give] + [other + q for q in give]:
        wo_copy(k).start()
    arrived()
    sent = []

    def push(src, dst, ss, rs, peer):
        sent.append(send(src, dst, ss, rs, peer))
        return sent[-1]

    heads = per * 4
    size = seqs + STAT_ROWS

    def part_of(ref, h, count=1):
        return ref.at[pl.ds(pl.multiple_of(h * size, 8), count * size)]

    pair = [[push(part_of(mine, (1 - core) * heads + give[c] * per + i), pin.at[c, i], s0.at[c, i], r0.at[c, i], partner)
             for c in range(2)] for i in range(per)]
    pair_keep = [[push(part_of(mine, (1 - core) * heads + keep[c] * per + i), pin.at[2 + c, i], s0.at[2 + c, i], r0.at[2 + c, i], partner)
                  for c in range(2)] for i in range(per)]

    def put(dst, merged):
        rows, stat = merged
        dst[0:seqs, :] = rows
        dst[seqs:seqs + STAT_ROWS, :] = stat

    step1 = [[], []]
    for i in range(per):
        for c in range(2):
            pair[i][c].wait_recv()
        for c in range(2):
            put(away.at[c, i], merge([part_of(mine, core * heads + give[c] * per + i), pin.at[c, i]], seqs))
        for c in range(2):
            step1[c].append(push(away.at[c, i], in1.at[c, i], s1.at[c, i], r1.at[c, i], first[c]))
    for copies in pair_keep:
        for copy in copies:
            copy.wait_recv()
    for i in range(per):
        for c in range(2):
            put(kept.at[c, i], merge([part_of(mine, core * heads + keep[c] * per + i), pin.at[2 + c, i]], seqs))
    step2 = [[], []]
    for i in range(per):
        for c in range(2):
            step1[c][i].wait_recv()
        for c in range(2):
            put(out2.at[c, i], merge([kept.at[c, i], in1.at[c, i]], seqs))
        for c in range(2):
            step2[c].append(push(out2.at[c, i], in2.at[c, i], s2.at[c, i], r2.at[c, i], second[c]))
    step3, own = [[], []], [[], []]
    blocks = [core * 4 + keep[c] for c in range(2)]

    def rows_of(k, i):
        return att.at[k, pl.ds(i * seqs, seqs)]

    for i in range(per):
        for c in range(2):
            step2[c][i].wait_recv()
        for c in range(2):
            done = merge([out2.at[c, i], in2.at[c, i]], seqs, final=True)
            att[blocks[c], i * seqs:(i + 1) * seqs, :] = done.astype(jnp.bfloat16).astype(jnp.float32)
        for c in range(2):
            piece = rows_of(blocks[c], i)
            step3[c].append(push(piece, piece, s3.at[c, i], r3.at[c, i], first[c]))
            own[c].append(push(piece, piece, s4.at[c, i], r4.at[c, i], partner))

    cols = 512

    def multiply(k, fresh=False):
        wo_copy(k).wait()
        lhs = jnp.concatenate([att[k, i * seqs:(i + 1) * seqs, :] for i in range(per)], axis=1).astype(jnp.bfloat16)
        for i in range(model // cols):
            off = slice(i * cols, (i + 1) * cols)
            y = jnp.dot(lhs, wov[k, :, off], preferred_element_type=jnp.float32)
            res[:, off] = y if fresh else res[:, off] + y

    def multiply_pair(base, i, last=False):
        ks = [base + give[c] for c in range(2)]
        if i == 0:
            for k in ks:
                wo_copy(k).wait()
        part = slice(i * seqs, (i + 1) * seqs)
        depth = slice(i * (k_rows // per), (i + 1) * (k_rows // per))
        lhs = jnp.concatenate([att[k, part, :] for k in ks], axis=1).astype(jnp.bfloat16)
        for j in range(model // cols):
            off = slice(j * cols, (j + 1) * cols)
            rhs = jnp.concatenate([wov[k, depth, off] for k in ks], axis=0)
            y = res[:, off] + jnp.dot(lhs, rhs, preferred_element_type=jnp.float32)
            if last:
                out_ref[:, off] = (tok_ref[:, off].astype(jnp.float32) + y).astype(jnp.bfloat16)
            else:
                res[:, off] = y

    multiply(blocks[0], fresh=True)
    multiply(blocks[1])
    for c in range(2):
        for i in range(per):
            own[c][i].wait_recv()
        multiply(other + keep[c])
    tok_copy.wait()
    passed = []
    for i in range(per):
        for c in range(2):
            step3[c][i].wait_recv()
            piece = rows_of(core * 4 + give[c], i)
            passed.append(push(piece, piece, s5.at[c, i], r5.at[c, i], partner))
        multiply_pair(core * 4, i)
        if i > 0:
            for copy in passed[2 * i - 2:2 * i]:
                copy.wait_recv()
            multiply_pair(other, i - 1)
    for copy in passed[2 * per - 2:]:
        copy.wait_recv()
    multiply_pair(other, per - 1, last=True)
    for copy in sent:
        copy.wait_send()


def tail_stage(part, w_o, tokens, group):
    seqs, model = tokens.shape
    head_dim = part.shape[-1]
    rows = seqs + STAT_ROWS
    per = part.shape[0] // rows // group
    vmem = pl.BlockSpec(memory_space=pltpu.VMEM)
    hbm = pl.BlockSpec(memory_space=pltpu.HBM)
    dma = pltpu.SemaphoreType.DMA
    sums = pltpu.VMEM((2, per, rows, head_dim), jnp.float32)
    return pl.pallas_call(
        tail_kernel,
        name='tail_stage',
        out_shape=pltpu.VMEM((seqs, model), jnp.bfloat16),
        in_specs=[vmem, hbm, hbm],
        out_specs=vmem,
        scratch_shapes=[
            pltpu.VMEM((seqs, model), tokens.dtype),
            dma,
            pltpu.VMEM((4, per, rows, head_dim), jnp.float32),
            sums, sums, sums, sums, sums,
            pltpu.VMEM((group, per * seqs, head_dim), jnp.float32),
            pltpu.VMEM((group, w_o.shape[0] // group, model), jnp.bfloat16),
            pltpu.VMEM((seqs, model), jnp.float32),
            dma((group,)), dma((4, per)), dma((4, per)),
        ] + [dma((2, per))] * 10,
        compiler_params=pltpu.CompilerParams(collective_id=0, has_side_effects=True, vmem_limit_bytes=44 * 1024 * 1024),
    )(part, *in_hbm(w_o, tokens))


def solution(mesh):
    cache_spec = P('dp', 'sp', None, None)
    group = mesh.shape['sp']

    def device_step(tokens, positions, k_cache, v_cache, w_q, w_k, w_v, w_o, attn_norm, q_norm, k_norm):
        shared = project_stage(tokens, positions, k_cache, v_cache, w_q, w_k, w_v, attn_norm, q_norm, k_norm, group)
        k_upd, v_upd, new_kv, part = attend_stage(positions, *shared)
        block_out = tail_stage(part, w_o, tokens, group)
        return block_out, k_upd, v_upd, new_kv

    return jax.shard_map(device_step, mesh=mesh, in_specs=(P('dp', None), P('dp'), cache_spec, cache_spec, P(), P(), P(), P(), P(), P(), P()), out_specs=(P('dp', None), cache_spec, cache_spec, P('dp', None, None, None)), check_vma=False)
```

```python
import functools

import jax
import jax.numpy as jnp
import numpy as np
from jax import lax
from jax.experimental import pallas as pl
from jax.experimental.pallas import tpu as pltpu
from jax.sharding import PartitionSpec as P

NORM_EPS = 1e-6
ROPE_THETA = 1000000.0
NEG_FILL = -1e30
MESH = pl.DeviceIdType.MESH
STAT_ROWS = 8
PIECES = 2


def in_hbm(*arrays):
    return [pltpu.with_memory_space_constraint(jnp.asarray(a), pltpu.HBM) for a in arrays]


def rope_frequencies(head_dim):
    inv_freq = ROPE_THETA ** (-np.arange(head_dim // 2, dtype=np.float64) * 2.0 / head_dim)
    return np.concatenate([inv_freq, inv_freq])[None, :].astype(np.float32)


def norm_rope(proj, gain, cos_full, sin_full):
    values = proj.astype(jnp.bfloat16).astype(jnp.float32)
    scale = lax.rsqrt(jnp.mean(values * values, axis=-1, keepdims=True) + NORM_EPS)
    normed = values * scale * gain
    turned = pltpu.roll(normed, normed.shape[-1] // 2, 1)
    return (normed * cos_full + turned * sin_full).astype(jnp.bfloat16).astype(jnp.float32)


def ring_place():
    me = lax.axis_index('sp')
    chips = lax.axis_size('sp') // 2
    core, chip = lax.rem(me, 2), me // 2
    c_right, c_left, c_opp = lax.rem(chip + 1, chips), lax.rem(chip + chips - 1, chips), lax.rem(chip + 2, chips)
    return chips, core, chip, c_right, c_left, c_opp, chip * 2 + 1 - core, c_right * 2 + core, c_left * 2 + core


def enter(peers):
    barrier = pltpu.get_barrier_semaphore()
    for peer in peers:
        pl.semaphore_signal(barrier, inc=1, device_id={'sp': peer}, device_id_type=MESH)
    return lambda: pl.semaphore_wait(barrier, len(peers))


def send(src, dst, ss, rs, peer):
    copy = pltpu.make_async_remote_copy(src_ref=src, dst_ref=dst, send_sem=ss, recv_sem=rs,
                                        device_id={'sp': peer}, device_id_type=MESH)
    copy.start()
    return copy


def project_kernel(pos_in, tok_in, freq_in, an_in, qn_in, kn_in, wq_ref, wk_ref, wv_ref, kc_ref, vc_ref,
                   qf, kf, vf, kbuf, vbuf,
                   pos_ref, tok_ref, freq_ref, an_ref, qn_ref, kn_ref, hid, wbuf, cosb, sinb, insem, wsem, csem, ss, rs):
    seqs, model = tok_ref.shape
    head_dim = qn_ref.shape[-1]
    blocks, _, blk = hid.shape
    width = wbuf.shape[-1]
    heads = width // head_dim
    chips, core, chip, c_right, c_left, c_opp, partner, right, left = ring_place()
    mine_k = core * chips + chip

    smalls = [pltpu.make_async_copy(src, dst, insem.at[j]) for j, (src, dst) in enumerate((
        (tok_in, tok_ref), (pos_in, pos_ref), (freq_in, freq_ref), (an_in, an_ref), (qn_in, qn_ref), (kn_in, kn_ref)))]
    for copy in smalls:
        copy.start()
    bulk = []
    k_left, k_right, k_opp = core * chips + c_left, core * chips + c_right, core * chips + c_opp
    for j, (ref, col) in enumerate(((wq_ref, mine_k), (wq_ref, k_opp), (wk_ref, core), (wv_ref, core))):
        for i in range(blocks):
            src = ref.at[pl.ds(i * blk, blk), pl.ds(pl.multiple_of(col * width, width), width)]
            bulk.append(pltpu.make_async_copy(src, wbuf.at[j, i], wsem.at[j, i]))
    pieces = csem.shape[1]
    per = seqs // pieces
    for g in range(pieces):
        for j, (ref, buf) in enumerate(((kc_ref, kbuf), (vc_ref, vbuf))):
            rows = pl.ds(g * per, per)
            bulk.append(pltpu.make_async_copy(ref.at[rows], buf.at[rows], csem.at[j, g]))
    issued = 0

    def issue(count):
        nonlocal issued
        for copy in bulk[issued:issued + count]:
            copy.start()
        issued += count

    issue(8)
    arrived = enter((partner, right, left))
    for copy in smalls:
        copy.wait()

    lanes = an_ref.shape[1]
    total = jnp.zeros((seqs, lanes), jnp.float32)
    for i in range(model // lanes):
        xf = tok_ref[:, i * lanes:(i + 1) * lanes].astype(jnp.float32)
        total = total + xf * xf
    inv = lax.rsqrt(jnp.sum(total, axis=-1, keepdims=True) / model + NORM_EPS)
    per_blk = blk // lanes
    for i in range(model // lanes):
        xf = tok_ref[:, i * lanes:(i + 1) * lanes].astype(jnp.float32)
        gain = an_ref[i:i + 1, :].astype(jnp.float32)
        hid[i // per_blk, :, (i % per_blk) * lanes:(i % per_blk + 1) * lanes] = (xf * inv * gain).astype(jnp.bfloat16)

    for b in range(seqs):
        cosb[b:b + 1, :] = jnp.full((1, head_dim), pos_ref[b], jnp.int32).astype(jnp.float32)
    angles = cosb[...] * freq_ref[...]
    sign = jnp.where(lax.broadcasted_iota(jnp.int32, angles.shape, 1) < head_dim // 2, -1.0, 1.0)
    sinb[...] = jnp.sin(angles) * sign
    cosb[...] = jnp.cos(angles)
    cos_full, sin_full = cosb[...], sinb[...]

    def project(j, more):
        y = None
        for i in range(blocks):
            bulk[j * blocks + i].wait()
            issue(more)
            part = jnp.dot(hid[i], wbuf[j, i], preferred_element_type=jnp.float32)
            y = part if y is None else y + part
        return [y[:, h * head_dim:(h + 1) * head_dim] for h in range(heads)]

    def put(dst, base, values):
        for h, value in enumerate(values):
            dst[pl.ds(pl.multiple_of(base + h * seqs, seqs), seqs), :] = value

    def q_chunk(k):
        return qf.at[pl.ds(pl.multiple_of(k * heads * seqs, heads * seqs), heads * seqs)]

    q_gain = qn_ref[...].astype(jnp.float32)
    put(qf, mine_k * heads * seqs, [norm_rope(p, q_gain, cos_full, sin_full) for p in project(0, 2)])
    arrived()
    count = 0
    sent = []

    def push(ref, peer):
        nonlocal count
        sent.append(send(ref, ref, ss.at[count], rs.at[count], peer))
        count += 1
        return sent[-1]

    own = [push(q_chunk(mine_k), peer) for peer in (right, left)]
    push(q_chunk(mine_k), partner)
    put(qf, k_opp * heads * seqs, [norm_rope(p, q_gain, cos_full, sin_full) for p in project(1, 4)])
    push(q_chunk(k_opp), partner)

    kv_rows = heads * seqs
    kv_base = core * kv_rows
    kv_part = pl.ds(pl.multiple_of(kv_base, kv_rows), kv_rows)
    k_gain = kn_ref[...].astype(jnp.float32)
    put(kf, kv_base, [norm_rope(p, k_gain, cos_full, sin_full) for p in project(2, 2)])
    push(kf.at[kv_part], partner)
    put(vf, kv_base, [p.astype(jnp.bfloat16).astype(jnp.float32) for p in project(3, 2)])
    push(vf.at[kv_part], partner)
    issue(len(bulk) - issued)

    for from_peer, k in zip(own, (k_left, k_right)):
        from_peer.wait_recv()
        push(q_chunk(k), partner)
    for copy in sent:
        if not any(copy is w for w in own):
            copy.wait_recv()
        copy.wait_send()
    for copy in bulk[4 * blocks:]:
        copy.wait()


def project_stage(tokens, positions, k_cache, v_cache, w_q, w_k, w_v, attn_norm, q_norm, k_norm, group):
    seqs, model = tokens.shape
    kv_heads, head_dim = k_cache.shape[2:]
    q_heads = w_q.shape[1] // head_dim
    width = w_q.shape[1] // group
    blocks = 4
    vmem = pl.BlockSpec(memory_space=pltpu.VMEM)
    hbm = pl.BlockSpec(memory_space=pltpu.HBM)
    dma = pltpu.SemaphoreType.DMA
    return pl.pallas_call(
        project_kernel,
        name='project_stage',
        out_shape=(
            pltpu.VMEM((q_heads * seqs, head_dim), jnp.float32),
            pltpu.VMEM((kv_heads * seqs, head_dim), jnp.float32),
            pltpu.VMEM((kv_heads * seqs, head_dim), jnp.float32),
            pltpu.VMEM(k_cache.shape, k_cache.dtype),
            pltpu.VMEM(v_cache.shape, v_cache.dtype),
        ),
        in_specs=[hbm] * 11,
        out_specs=(vmem,) * 5,
        scratch_shapes=[
            pltpu.SMEM(positions.shape, jnp.int32),
            pltpu.VMEM(tokens.shape, tokens.dtype),
            pltpu.VMEM((1, head_dim), jnp.float32),
            pltpu.VMEM((model // 128, 128), attn_norm.dtype),
            pltpu.VMEM((1, head_dim), q_norm.dtype),
            pltpu.VMEM((1, head_dim), k_norm.dtype),
            pltpu.VMEM((blocks, seqs, model // blocks), jnp.bfloat16),
            pltpu.VMEM((4, blocks, model // blocks, width), jnp.bfloat16),
            pltpu.VMEM((seqs, head_dim), jnp.float32),
            pltpu.VMEM((seqs, head_dim), jnp.float32),
            dma((6,)), dma((4, blocks)), dma((2, 8)), dma((16,)), dma((16,)),
        ],
        compiler_params=pltpu.CompilerParams(collective_id=1, has_side_effects=True, vmem_limit_bytes=24 * 1024 * 1024),
    )(*in_hbm(positions, tokens, rope_frequencies(head_dim), attn_norm.reshape(-1, 128), q_norm[None, :], k_norm[None, :],
              w_q, w_k, w_v, k_cache, v_cache))


def attend_kernel(pos_in, qf, kf, vf, k_in, v_in, ko_ref, vo_ref, new_out, part_ref, kbuf, vbuf,
                  pos_ref, new_ref, mstat, lstat, sbuf, ebuf, possem, newsem, kosem, vosem):
    seqs, slots, kv_heads, head_dim = kbuf.shape
    groups = kosem.shape[0]
    per_group = seqs // groups
    q_heads = qf.shape[0] // seqs
    start = lax.axis_index('sp') * slots
    pos_copy = pltpu.make_async_copy(pos_in, pos_ref, possem)
    pos_copy.start()
    pos_copy.wait()

    def write_step(g, carry):
        for bb in range(per_group):
            b = g * per_group + bb
            local = pos_ref[b] - start
            here = (local >= 0) & (local < slots)
            at = jnp.clip(local, 0, slots - 1)
            k_new = kf[pl.ds(b, kv_heads, stride=seqs), :]
            v_new = vf[pl.ds(b, kv_heads, stride=seqs), :]
            new_ref[b, 0] = k_new.astype(jnp.bfloat16)
            new_ref[b, 1] = v_new.astype(jnp.bfloat16)
            kbuf[b, at] = jnp.where(here, k_new, kbuf[b, at].astype(jnp.float32)).astype(jnp.bfloat16)
            vbuf[b, at] = jnp.where(here, v_new, vbuf[b, at].astype(jnp.float32)).astype(jnp.bfloat16)
        for copy in writes(g):
            copy.start()
        return carry

    def writes(g):
        rows = pl.ds(g * per_group, per_group)
        return (pltpu.make_async_copy(kbuf.at[rows], ko_ref.at[rows], kosem.at[g]),
                pltpu.make_async_copy(vbuf.at[rows], vo_ref.at[rows], vosem.at[g]),
                pltpu.make_async_copy(new_ref.at[rows], new_out.at[rows], newsem.at[g]))

    lax.fori_loop(0, groups, write_step, 0)

    cols = slots * kv_heads
    row_id = lax.broadcasted_iota(jnp.int32, (q_heads, cols), 0)
    col_id = lax.broadcasted_iota(jnp.int32, (q_heads, cols), 1)
    head_ok = row_id // (q_heads // kv_heads) == col_id % kv_heads
    slot_key = jnp.where(head_ok, col_id // kv_heads, slots * 1024)
    lane = lax.broadcasted_iota(jnp.int32, (q_heads, 128), 1)
    score_scale = head_dim ** -0.5
    mstat[...] = jnp.zeros_like(mstat)
    lstat[...] = jnp.zeros_like(lstat)

    def group_step(g, carry):
        m_acc, l_acc = mstat[...], lstat[...]
        members = [g * per_group + bb for bb in range(per_group)]
        for bb, b in enumerate(members):
            q_b = qf[pl.ds(b, q_heads, stride=seqs), :].astype(jnp.bfloat16)
            k_b = kbuf[b].reshape(cols, head_dim)
            sbuf[bb] = lax.dot_general(q_b, k_b, (((1,), (1,)), ((), ())), preferred_element_type=jnp.float32)
        for bb, b in enumerate(members):
            live = slot_key <= pos_ref[b] - start
            s = jnp.where(live, sbuf[bb] * score_scale, NEG_FILL)
            m = jnp.max(s, axis=-1, keepdims=True)
            e = jnp.where(live, jnp.exp(s - m), 0.0)
            l = jnp.sum(e, axis=-1, keepdims=True)
            ebuf[bb] = e.astype(jnp.bfloat16)
            m_acc = jnp.where(lane == b, m, m_acc)
            l_acc = jnp.where(lane == b, l, l_acc)
        for bb, b in enumerate(members):
            o = jnp.dot(ebuf[bb], vbuf[b].reshape(cols, head_dim), preferred_element_type=jnp.float32)
            part_ref[pl.ds(b, q_heads, stride=seqs + STAT_ROWS), :] = o
        mstat[...] = m_acc
        lstat[...] = l_acc
        return carry

    lax.fori_loop(0, groups, group_step, 0)

    for h in range(q_heads):
        row = h * (seqs + STAT_ROWS) + seqs
        part_ref[row:row + 1, :] = mstat[h:h + 1, :]
        part_ref[row + 1:row + 2, :] = lstat[h:h + 1, :]
        part_ref[row + 2:row + STAT_ROWS, :] = jnp.zeros((STAT_ROWS - 2, 128), jnp.float32)
    for g in range(groups):
        for copy in writes(g):
            copy.wait()


def attend_stage(positions, qf, kf, vf, k_vm, v_vm):
    seqs, slots, kv_heads, head_dim = k_vm.shape
    q_heads = qf.shape[0] // seqs
    groups = 4
    vmem = pl.BlockSpec(memory_space=pltpu.VMEM)
    anyspec = pl.BlockSpec(memory_space=pl.ANY)
    hbm = pl.BlockSpec(memory_space=pltpu.HBM)
    dma = pltpu.SemaphoreType.DMA
    outs = pl.pallas_call(
        attend_kernel,
        name='attend_stage',
        out_shape=(
            jax.ShapeDtypeStruct(k_vm.shape, k_vm.dtype),
            jax.ShapeDtypeStruct(v_vm.shape, v_vm.dtype),
            jax.ShapeDtypeStruct((seqs, 2, kv_heads, head_dim), jnp.bfloat16),
            pltpu.VMEM((q_heads * (seqs + STAT_ROWS), head_dim), jnp.float32),
            pltpu.VMEM(k_vm.shape, k_vm.dtype),
            pltpu.VMEM(v_vm.shape, v_vm.dtype),
        ),
        in_specs=[hbm] + [vmem] * 5,
        out_specs=(anyspec, anyspec, anyspec, vmem, vmem, vmem),
        input_output_aliases={4: 4, 5: 5},
        scratch_shapes=[
            pltpu.SMEM(positions.shape, jnp.int32),
            pltpu.VMEM((seqs, 2, kv_heads, head_dim), jnp.bfloat16),
            pltpu.VMEM((q_heads, 128), jnp.float32),
            pltpu.VMEM((q_heads, 128), jnp.float32),
            pltpu.VMEM((seqs // groups, q_heads, slots * kv_heads), jnp.float32),
            pltpu.VMEM((seqs // groups, q_heads, slots * kv_heads), jnp.bfloat16),
            dma, dma((groups,)), dma((groups,)), dma((groups,)),
        ],
        compiler_params=pltpu.CompilerParams(vmem_limit_bytes=16 * 1024 * 1024),
    )(*in_hbm(positions), qf, kf, vf, k_vm, v_vm)
    return outs[:4]


def merge(pieces, seqs, final=False):
    stats = [jnp.transpose(ref[seqs:seqs + STAT_ROWS, :], (1, 0))[:seqs] for ref in pieces]
    peak = functools.reduce(jnp.maximum, [t[:, 0:1] for t in stats])
    factors = [jnp.exp(t[:, 0:1] - peak) for t in stats]
    total = functools.reduce(jnp.add, [f * t[:, 1:2] for f, t in zip(factors, stats)])
    rows = functools.reduce(jnp.add, [f * ref[0:seqs, :] for f, ref in zip(factors, pieces)])
    if final:
        return rows / total
    both = jnp.concatenate([peak, total, jnp.zeros((seqs, STAT_ROWS - 2), jnp.float32)], axis=1)
    both = jnp.concatenate([both, jnp.zeros((128 - seqs, STAT_ROWS), jnp.float32)], axis=0)
    return rows, jnp.transpose(both, (1, 0))


def tail_kernel(mine, wo_ref, tok_in, out_ref, tok_ref, toksem, pin, away, kept, in1, out2, in2, att, wov, res,
                wsem, s0, r0, s1, r1, s2, r2, s3, r3, s4, r4, s5, r5):
    seqs, model = tok_ref.shape
    size = seqs + STAT_ROWS
    per = away.shape[1] // size
    hp = per // PIECES
    tok_copy = pltpu.make_async_copy(tok_in, tok_ref, toksem)
    tok_copy.start()
    chips, core, chip, _, _, _, partner, _, _ = ring_place()
    near, far = chip + 1 - 2 * lax.rem(chip, 2), chips - 1 - chip
    first = (near * 2 + core, far * 2 + core)
    second = (first[1], first[0])
    sel = (lax.rem((chip + 1) // 2, 2), chip // 2)
    keep = [2 * c + sel[c] for c in range(2)]
    give = [2 * c + 1 - sel[c] for c in range(2)]
    arrived = enter((partner, first[0], first[1]))
    k_rows = wov.shape[1]

    def wo_copy(k):
        return pltpu.make_async_copy(wo_ref.at[pl.ds(pl.multiple_of(k * k_rows, k_rows), k_rows)], wov.at[k], wsem.at[k])

    other = (1 - core) * 4
    for k in [core * 4 + q for q in keep] + [other + q for q in keep] + [core * 4 + q for q in give] + [other + q for q in give]:
        wo_copy(k).start()
    arrived()
    sent = []

    def push(src, dst, ss, rs, peer):
        sent.append(send(src, dst, ss, rs, peer))
        return sent[-1]

    heads = per * 4

    def part_of(ref, h, count=1):
        return ref.at[pl.ds(pl.multiple_of(h * size, 8), count * size)]

    def piece_of(ref, i):
        return part_of(ref, i * hp, hp)

    def trade(q, slot, i):
        return push(part_of(mine, (1 - core) * heads + q * per + i * hp, hp), piece_of(pin.at[slot], i), s0.at[slot, i], r0.at[slot, i], partner)

    pair = [[trade(give[c], c, i) for c in range(2)] for i in range(PIECES)]
    pair_keep = [[trade(keep[c], 2 + c, i) for c in range(2)] for i in range(PIECES)]

    def put(dst, h, merged):
        rows, stat = merged
        dst[h * size:h * size + seqs, :] = rows
        dst[h * size + seqs:(h + 1) * size, :] = stat

    def members(i):
        return [(h, c) for h in range(i * hp, (i + 1) * hp) for c in range(2)]

    step1 = [[], []]
    for i in range(PIECES):
        for c in range(2):
            pair[i][c].wait_recv()
        for h, c in members(i):
            put(away.at[c], h, merge([part_of(mine, core * heads + give[c] * per + h), part_of(pin.at[c], h)], seqs))
        for c in range(2):
            step1[c].append(push(piece_of(away.at[c], i), piece_of(in1.at[c], i), s1.at[c, i], r1.at[c, i], first[c]))
    for copies in pair_keep:
        for copy in copies:
            copy.wait_recv()
    for i in range(PIECES):
        for h, c in members(i):
            put(kept.at[c], h, merge([part_of(mine, core * heads + keep[c] * per + h), part_of(pin.at[2 + c], h)], seqs))
    step2 = [[], []]
    for i in range(PIECES):
        for c in range(2):
            step1[c][i].wait_recv()
        for h, c in members(i):
            put(out2.at[c], h, merge([part_of(kept.at[c], h), part_of(in1.at[c], h)], seqs))
        for c in range(2):
            step2[c].append(push(piece_of(out2.at[c], i), piece_of(in2.at[c], i), s2.at[c, i], r2.at[c, i], second[c]))
    step3, own = [[], []], [[], []]
    blocks = [core * 4 + keep[c] for c in range(2)]

    def rows_of(k, i):
        return att.at[k, pl.ds(i * hp * seqs, hp * seqs)]

    for i in range(PIECES):
        for c in range(2):
            step2[c][i].wait_recv()
        for h, c in members(i):
            done = merge([part_of(out2.at[c], h), part_of(in2.at[c], h)], seqs, final=True)
            att[blocks[c], h * seqs:(h + 1) * seqs, :] = done.astype(jnp.bfloat16).astype(jnp.float32)
        for c in range(2):
            piece = rows_of(blocks[c], i)
            step3[c].append(push(piece, piece, s3.at[c, i], r3.at[c, i], first[c]))
        for c in range(2):
            piece = rows_of(blocks[c], i)
            own[c].append(push(piece, piece, s4.at[c, i], r4.at[c, i], partner))

    cols = 512

    def multiply(k, fresh=False):
        wo_copy(k).wait()
        lhs = jnp.concatenate([att[k, i * seqs:(i + 1) * seqs, :] for i in range(per)], axis=1).astype(jnp.bfloat16)
        for i in range(model // cols):
            off = slice(i * cols, (i + 1) * cols)
            y = jnp.dot(lhs, wov[k, :, off], preferred_element_type=jnp.float32)
            res[:, off] = y if fresh else res[:, off] + y

    def multiply_pair(base, i, last=False):
        ks = [base + give[c] for c in range(2)]
        if i == 0:
            for k in ks:
                wo_copy(k).wait()
        depth = slice(i * (k_rows // PIECES), (i + 1) * (k_rows // PIECES))
        lhs = jnp.concatenate([att[k, h * seqs:(h + 1) * seqs, :] for k in ks for h in range(i * hp, (i + 1) * hp)], axis=1).astype(jnp.bfloat16)
        for j in range(model // cols):
            off = slice(j * cols, (j + 1) * cols)
            rhs = jnp.concatenate([wov[k, depth, off] for k in ks], axis=0)
            y = res[:, off] + jnp.dot(lhs, rhs, preferred_element_type=jnp.float32)
            if last:
                out_ref[:, off] = (tok_ref[:, off].astype(jnp.float32) + y).astype(jnp.bfloat16)
            else:
                res[:, off] = y

    multiply(blocks[0], fresh=True)
    multiply(blocks[1])
    for c in range(2):
        for i in range(PIECES):
            own[c][i].wait_recv()
        multiply(other + keep[c])
    tok_copy.wait()
    passed = []
    for i in range(PIECES):
        for c in range(2):
            step3[c][i].wait_recv()
            piece = rows_of(core * 4 + give[c], i)
            passed.append(push(piece, piece, s5.at[c, i], r5.at[c, i], partner))
        multiply_pair(core * 4, i)
        if i > 0:
            for copy in passed[2 * i - 2:2 * i]:
                copy.wait_recv()
            multiply_pair(other, i - 1)
    for copy in passed[2 * PIECES - 2:]:
        copy.wait_recv()
    multiply_pair(other, PIECES - 1, last=True)
    for copy in sent:
        copy.wait_send()


def tail_stage(part, w_o, tokens, group):
    seqs, model = tokens.shape
    head_dim = part.shape[-1]
    rows = seqs + STAT_ROWS
    per = part.shape[0] // rows // group
    vmem = pl.BlockSpec(memory_space=pltpu.VMEM)
    hbm = pl.BlockSpec(memory_space=pltpu.HBM)
    dma = pltpu.SemaphoreType.DMA
    sums = pltpu.VMEM((2, per * rows, head_dim), jnp.float32)
    return pl.pallas_call(
        tail_kernel,
        name='tail_stage',
        out_shape=pltpu.VMEM((seqs, model), jnp.bfloat16),
        in_specs=[vmem, hbm, hbm],
        out_specs=vmem,
        scratch_shapes=[
            pltpu.VMEM((seqs, model), tokens.dtype),
            dma,
            pltpu.VMEM((4, per * rows, head_dim), jnp.float32),
            sums, sums, sums, sums, sums,
            pltpu.VMEM((group, per * seqs, head_dim), jnp.float32),
            pltpu.VMEM((group, w_o.shape[0] // group, model), jnp.bfloat16),
            pltpu.VMEM((seqs, model), jnp.float32),
            dma((group,)), dma((4, PIECES)), dma((4, PIECES)),
        ] + [dma((2, PIECES))] * 10,
        compiler_params=pltpu.CompilerParams(collective_id=0, has_side_effects=True, vmem_limit_bytes=44 * 1024 * 1024),
    )(part, *in_hbm(w_o, tokens))


def solution(mesh):
    cache_spec = P('dp', 'sp', None, None)
    group = mesh.shape['sp']

    def device_step(tokens, positions, k_cache, v_cache, w_q, w_k, w_v, w_o, attn_norm, q_norm, k_norm):
        shared = project_stage(tokens, positions, k_cache, v_cache, w_q, w_k, w_v, attn_norm, q_norm, k_norm, group)
        k_upd, v_upd, new_kv, part = attend_stage(positions, *shared)
        block_out = tail_stage(part, w_o, tokens, group)
        return block_out, k_upd, v_upd, new_kv

    return jax.shard_map(device_step, mesh=mesh, in_specs=(P('dp', None), P('dp'), cache_spec, cache_spec, P(), P(), P(), P(), P(), P(), P()), out_specs=(P('dp', None), cache_spec, cache_spec, P('dp', None, None, None)), check_vma=False)
```

```python
import functools

import jax
import jax.numpy as jnp
import numpy as np
from jax import lax
from jax.experimental import pallas as pl
from jax.experimental.pallas import tpu as pltpu
from jax.sharding import PartitionSpec as P

NORM_EPS = 1e-6
ROPE_THETA = 1000000.0
NEG_FILL = -1e30
MESH = pl.DeviceIdType.MESH
STAT_ROWS = 8


def in_hbm(*arrays):
    return [pltpu.with_memory_space_constraint(jnp.asarray(a), pltpu.HBM) for a in arrays]


def rope_frequencies(head_dim):
    inv_freq = ROPE_THETA ** (-np.arange(head_dim // 2, dtype=np.float64) * 2.0 / head_dim)
    return np.concatenate([inv_freq, inv_freq])[None, :].astype(np.float32)


def norm_rope(proj, gain, cos_full, sin_full):
    values = proj.astype(jnp.bfloat16).astype(jnp.float32)
    scale = lax.rsqrt(jnp.mean(values * values, axis=-1, keepdims=True) + NORM_EPS)
    normed = values * scale * gain
    turned = pltpu.roll(normed, normed.shape[-1] // 2, 1)
    return (normed * cos_full + turned * sin_full).astype(jnp.bfloat16).astype(jnp.float32)


def ring_place():
    me = lax.axis_index('sp')
    chips = lax.axis_size('sp') // 2
    core, chip = lax.rem(me, 2), me // 2
    c_right, c_left, c_opp = lax.rem(chip + 1, chips), lax.rem(chip + chips - 1, chips), lax.rem(chip + 2, chips)
    return chips, core, chip, c_right, c_left, c_opp, chip * 2 + 1 - core, c_right * 2 + core, c_left * 2 + core


def enter(peers):
    barrier = pltpu.get_barrier_semaphore()
    for peer in peers:
        pl.semaphore_signal(barrier, inc=1, device_id={'sp': peer}, device_id_type=MESH)
    return lambda: pl.semaphore_wait(barrier, len(peers))


def send(src, dst, ss, rs, peer):
    copy = pltpu.make_async_remote_copy(src_ref=src, dst_ref=dst, send_sem=ss, recv_sem=rs,
                                        device_id={'sp': peer}, device_id_type=MESH)
    copy.start()
    return copy


def project_kernel(pos_in, tok_in, freq_in, an_in, qn_in, kn_in, wq_ref, wk_ref, wv_ref, kc_ref, vc_ref,
                   qf, kf, vf, kbuf, vbuf,
                   pos_ref, tok_ref, freq_ref, an_ref, qn_ref, kn_ref, hid, wbuf, cosb, sinb, insem, wsem, csem, ss, rs):
    seqs, model = tok_ref.shape
    head_dim = qn_ref.shape[-1]
    blocks, _, blk = hid.shape
    width = wbuf.shape[-1]
    heads = width // head_dim
    chips, core, chip, c_right, c_left, c_opp, partner, right, left = ring_place()
    mine_k = core * chips + chip

    smalls = [pltpu.make_async_copy(src, dst, insem.at[j]) for j, (src, dst) in enumerate((
        (tok_in, tok_ref), (pos_in, pos_ref), (freq_in, freq_ref), (an_in, an_ref), (qn_in, qn_ref), (kn_in, kn_ref)))]
    for copy in smalls:
        copy.start()
    bulk = []
    k_left, k_right, k_opp = core * chips + c_left, core * chips + c_right, core * chips + c_opp
    for j, (ref, col) in enumerate(((wq_ref, mine_k), (wq_ref, k_opp), (wk_ref, core), (wv_ref, core))):
        for i in range(blocks):
            src = ref.at[pl.ds(i * blk, blk), pl.ds(pl.multiple_of(col * width, width), width)]
            bulk.append(pltpu.make_async_copy(src, wbuf.at[j, i], wsem.at[j, i]))
    pieces = csem.shape[1]
    per = seqs // pieces
    for g in range(pieces):
        for j, (ref, buf) in enumerate(((kc_ref, kbuf), (vc_ref, vbuf))):
            rows = pl.ds(g * per, per)
            bulk.append(pltpu.make_async_copy(ref.at[rows], buf.at[rows], csem.at[j, g]))
    issued = 0

    def issue(count):
        nonlocal issued
        for copy in bulk[issued:issued + count]:
            copy.start()
        issued += count

    issue(8)
    arrived = enter((partner, right, left))
    for copy in smalls:
        copy.wait()

    lanes = an_ref.shape[1]
    total = jnp.zeros((seqs, lanes), jnp.float32)
    for i in range(model // lanes):
        xf = tok_ref[:, i * lanes:(i + 1) * lanes].astype(jnp.float32)
        total = total + xf * xf
    inv = lax.rsqrt(jnp.sum(total, axis=-1, keepdims=True) / model + NORM_EPS)
    per_blk = blk // lanes
    for i in range(model // lanes):
        xf = tok_ref[:, i * lanes:(i + 1) * lanes].astype(jnp.float32)
        gain = an_ref[i:i + 1, :].astype(jnp.float32)
        hid[i // per_blk, :, (i % per_blk) * lanes:(i % per_blk + 1) * lanes] = (xf * inv * gain).astype(jnp.bfloat16)

    for b in range(seqs):
        cosb[b:b + 1, :] = jnp.full((1, head_dim), pos_ref[b], jnp.int32).astype(jnp.float32)
    angles = cosb[...] * freq_ref[...]
    sign = jnp.where(lax.broadcasted_iota(jnp.int32, angles.shape, 1) < head_dim // 2, -1.0, 1.0)
    sinb[...] = jnp.sin(angles) * sign
    cosb[...] = jnp.cos(angles)
    cos_full, sin_full = cosb[...], sinb[...]

    def project(j, more):
        y = None
        for i in range(blocks):
            bulk[j * blocks + i].wait()
            issue(more)
            part = jnp.dot(hid[i], wbuf[j, i], preferred_element_type=jnp.float32)
            y = part if y is None else y + part
        return [y[:, h * head_dim:(h + 1) * head_dim] for h in range(heads)]

    def put(dst, base, values):
        for h, value in enumerate(values):
            dst[pl.ds(pl.multiple_of(base + h * seqs, seqs), seqs), :] = value

    half_rows = heads // 2 * seqs

    def q_half(k, h):
        return qf.at[pl.ds(pl.multiple_of(k * heads * seqs + h * half_rows, half_rows), half_rows)]

    q_gain = qn_ref[...].astype(jnp.float32)
    put(qf, mine_k * heads * seqs, [norm_rope(p, q_gain, cos_full, sin_full) for p in project(0, 2)])
    arrived()
    count = 0
    sent = []

    def push(ref, peer):
        nonlocal count
        sent.append(send(ref, ref, ss.at[count], rs.at[count], peer))
        count += 1
        return sent[-1]

    own = [[push(q_half(mine_k, h), peer) for peer in (right, left)] for h in range(2)]
    push(q_half(mine_k, 0), partner)
    push(q_half(mine_k, 1), partner)
    put(qf, k_opp * heads * seqs, [norm_rope(p, q_gain, cos_full, sin_full) for p in project(1, 4)])
    push(q_half(k_opp, 0), partner)
    push(q_half(k_opp, 1), partner)

    kv_rows = heads * seqs
    kv_base = core * kv_rows
    kv_part = pl.ds(pl.multiple_of(kv_base, kv_rows), kv_rows)
    k_gain = kn_ref[...].astype(jnp.float32)
    put(kf, kv_base, [norm_rope(p, k_gain, cos_full, sin_full) for p in project(2, 2)])
    push(kf.at[kv_part], partner)
    put(vf, kv_base, [p.astype(jnp.bfloat16).astype(jnp.float32) for p in project(3, 2)])
    push(vf.at[kv_part], partner)
    issue(len(bulk) - issued)

    for h in range(2):
        for from_peer, k in zip(own[h], (k_left, k_right)):
            from_peer.wait_recv()
            push(q_half(k, h), partner)
    waited = own[0] + own[1]
    for copy in sent:
        if not any(copy is w for w in waited):
            copy.wait_recv()
        copy.wait_send()
    for copy in bulk[4 * blocks:]:
        copy.wait()


def project_stage(tokens, positions, k_cache, v_cache, w_q, w_k, w_v, attn_norm, q_norm, k_norm, group):
    seqs, model = tokens.shape
    kv_heads, head_dim = k_cache.shape[2:]
    q_heads = w_q.shape[1] // head_dim
    width = w_q.shape[1] // group
    blocks = 4
    vmem = pl.BlockSpec(memory_space=pltpu.VMEM)
    hbm = pl.BlockSpec(memory_space=pltpu.HBM)
    dma = pltpu.SemaphoreType.DMA
    return pl.pallas_call(
        project_kernel,
        name='project_stage',
        out_shape=(
            pltpu.VMEM((q_heads * seqs, head_dim), jnp.float32),
            pltpu.VMEM((kv_heads * seqs, head_dim), jnp.float32),
            pltpu.VMEM((kv_heads * seqs, head_dim), jnp.float32),
            pltpu.VMEM(k_cache.shape, k_cache.dtype),
            pltpu.VMEM(v_cache.shape, v_cache.dtype),
        ),
        in_specs=[hbm] * 11,
        out_specs=(vmem,) * 5,
        scratch_shapes=[
            pltpu.SMEM(positions.shape, jnp.int32),
            pltpu.VMEM(tokens.shape, tokens.dtype),
            pltpu.VMEM((1, head_dim), jnp.float32),
            pltpu.VMEM((model // 128, 128), attn_norm.dtype),
            pltpu.VMEM((1, head_dim), q_norm.dtype),
            pltpu.VMEM((1, head_dim), k_norm.dtype),
            pltpu.VMEM((blocks, seqs, model // blocks), jnp.bfloat16),
            pltpu.VMEM((4, blocks, model // blocks, width), jnp.bfloat16),
            pltpu.VMEM((seqs, head_dim), jnp.float32),
            pltpu.VMEM((seqs, head_dim), jnp.float32),
            dma((6,)), dma((4, blocks)), dma((2, 8)), dma((16,)), dma((16,)),
        ],
        compiler_params=pltpu.CompilerParams(collective_id=1, has_side_effects=True, vmem_limit_bytes=24 * 1024 * 1024),
    )(*in_hbm(positions, tokens, rope_frequencies(head_dim), attn_norm.reshape(-1, 128), q_norm[None, :], k_norm[None, :],
              w_q, w_k, w_v, k_cache, v_cache))


def attend_kernel(pos_in, qf, kf, vf, k_in, v_in, ko_ref, vo_ref, new_out, part_ref, kbuf, vbuf,
                  pos_ref, new_ref, mstat, lstat, sbuf, ebuf, possem, newsem, kosem, vosem):
    seqs, slots, kv_heads, head_dim = kbuf.shape
    groups = kosem.shape[0]
    per_group = seqs // groups
    q_heads = qf.shape[0] // seqs
    start = lax.axis_index('sp') * slots
    pos_copy = pltpu.make_async_copy(pos_in, pos_ref, possem)
    pos_copy.start()
    pos_copy.wait()

    def write_step(g, carry):
        for bb in range(per_group):
            b = g * per_group + bb
            local = pos_ref[b] - start
            here = (local >= 0) & (local < slots)
            at = jnp.clip(local, 0, slots - 1)
            k_new = kf[pl.ds(b, kv_heads, stride=seqs), :]
            v_new = vf[pl.ds(b, kv_heads, stride=seqs), :]
            new_ref[b, 0] = k_new.astype(jnp.bfloat16)
            new_ref[b, 1] = v_new.astype(jnp.bfloat16)
            kbuf[b, at] = jnp.where(here, k_new, kbuf[b, at].astype(jnp.float32)).astype(jnp.bfloat16)
            vbuf[b, at] = jnp.where(here, v_new, vbuf[b, at].astype(jnp.float32)).astype(jnp.bfloat16)
        for copy in writes(g):
            copy.start()
        return carry

    def writes(g):
        rows = pl.ds(g * per_group, per_group)
        return (pltpu.make_async_copy(kbuf.at[rows], ko_ref.at[rows], kosem.at[g]),
                pltpu.make_async_copy(vbuf.at[rows], vo_ref.at[rows], vosem.at[g]),
                pltpu.make_async_copy(new_ref.at[rows], new_out.at[rows], newsem.at[g]))

    lax.fori_loop(0, groups, write_step, 0)

    cols = slots * kv_heads
    row_id = lax.broadcasted_iota(jnp.int32, (q_heads, cols), 0)
    col_id = lax.broadcasted_iota(jnp.int32, (q_heads, cols), 1)
    head_ok = row_id % kv_heads == col_id % kv_heads
    q_per = q_heads // kv_heads
    block_rows = STAT_ROWS + q_per * seqs
    slot_key = jnp.where(head_ok, col_id // kv_heads, slots * 1024)
    lane = lax.broadcasted_iota(jnp.int32, (q_heads, 128), 1)
    score_scale = head_dim ** -0.5
    mstat[...] = jnp.zeros_like(mstat)
    lstat[...] = jnp.zeros_like(lstat)

    def group_step(g, carry):
        m_acc, l_acc = mstat[...], lstat[...]
        members = [g * per_group + bb for bb in range(per_group)]
        for bb, b in enumerate(members):
            q_b = jnp.concatenate([qf[pl.ds(b + j * seqs, kv_heads, stride=q_per * seqs), :] for j in range(q_per)], axis=0).astype(jnp.bfloat16)
            k_b = kbuf[b].reshape(cols, head_dim)
            sbuf[bb] = lax.dot_general(q_b, k_b, (((1,), (1,)), ((), ())), preferred_element_type=jnp.float32)
        for bb, b in enumerate(members):
            live = slot_key <= pos_ref[b] - start
            s = jnp.where(live, sbuf[bb] * score_scale, NEG_FILL)
            m = jnp.max(s, axis=-1, keepdims=True)
            e = jnp.where(live, jnp.exp(s - m), 0.0)
            l = jnp.sum(e, axis=-1, keepdims=True)
            ebuf[bb] = e.astype(jnp.bfloat16)
            m_acc = jnp.where(lane == b, m, m_acc)
            l_acc = jnp.where(lane == b, l, l_acc)
        for bb, b in enumerate(members):
            o = jnp.dot(ebuf[bb], vbuf[b].reshape(cols, head_dim), preferred_element_type=jnp.float32)
            for j in range(q_per):
                part_ref[pl.ds(b + STAT_ROWS + j * seqs, kv_heads, stride=block_rows), :] = o[j * kv_heads:(j + 1) * kv_heads, :]
        mstat[...] = m_acc
        lstat[...] = l_acc
        return carry

    lax.fori_loop(0, groups, group_step, 0)

    for k in range(kv_heads):
        for j in range(q_per):
            row = k * block_rows + j
            part_ref[row:row + 1, :] = mstat[j * kv_heads + k:j * kv_heads + k + 1, :]
            part_ref[row + q_per:row + q_per + 1, :] = lstat[j * kv_heads + k:j * kv_heads + k + 1, :]
    for g in range(groups):
        for copy in writes(g):
            copy.wait()


def attend_stage(positions, qf, kf, vf, k_vm, v_vm):
    seqs, slots, kv_heads, head_dim = k_vm.shape
    q_heads = qf.shape[0] // seqs
    groups = 4
    vmem = pl.BlockSpec(memory_space=pltpu.VMEM)
    anyspec = pl.BlockSpec(memory_space=pl.ANY)
    hbm = pl.BlockSpec(memory_space=pltpu.HBM)
    dma = pltpu.SemaphoreType.DMA
    outs = pl.pallas_call(
        attend_kernel,
        name='attend_stage',
        out_shape=(
            jax.ShapeDtypeStruct(k_vm.shape, k_vm.dtype),
            jax.ShapeDtypeStruct(v_vm.shape, v_vm.dtype),
            jax.ShapeDtypeStruct((seqs, 2, kv_heads, head_dim), jnp.bfloat16),
            pltpu.VMEM((kv_heads * STAT_ROWS + q_heads * seqs, head_dim), jnp.float32),
            pltpu.VMEM(k_vm.shape, k_vm.dtype),
            pltpu.VMEM(v_vm.shape, v_vm.dtype),
        ),
        in_specs=[hbm] + [vmem] * 5,
        out_specs=(anyspec, anyspec, anyspec, vmem, vmem, vmem),
        input_output_aliases={4: 4, 5: 5},
        scratch_shapes=[
            pltpu.SMEM(positions.shape, jnp.int32),
            pltpu.VMEM((seqs, 2, kv_heads, head_dim), jnp.bfloat16),
            pltpu.VMEM((q_heads, 128), jnp.float32),
            pltpu.VMEM((q_heads, 128), jnp.float32),
            pltpu.VMEM((seqs // groups, q_heads, slots * kv_heads), jnp.float32),
            pltpu.VMEM((seqs // groups, q_heads, slots * kv_heads), jnp.bfloat16),
            dma, dma((groups,)), dma((groups,)), dma((groups,)),
        ],
        compiler_params=pltpu.CompilerParams(vmem_limit_bytes=16 * 1024 * 1024),
    )(*in_hbm(positions), qf, kf, vf, k_vm, v_vm)
    return outs[:4]


def weigh(tiles, seqs):
    per = STAT_ROWS // 2
    stats = [jnp.transpose(tile, (1, 0))[:seqs] for tile in tiles]
    peak = functools.reduce(jnp.maximum, [t[:, :per] for t in stats])
    factors = [jnp.exp(t[:, :per] - peak) for t in stats]
    return factors, peak, functools.reduce(jnp.add, [f * t[:, per:] for f, t in zip(factors, stats)])


def stat_tile(peak, total):
    both = jnp.concatenate([peak, total], axis=1)
    both = jnp.concatenate([both, jnp.zeros((128 - both.shape[0], STAT_ROWS), jnp.float32)], axis=0)
    return jnp.transpose(both, (1, 0))


def tail_kernel(mine, wo_ref, tok_in, out_ref, tok_ref, toksem, pin, away, in1, out2, in2, att, wov, res,
                wsem, s0, r0, s1, r1, s2, r2, s3, r3, s4, r4, s5, r5):
    seqs, model = tok_ref.shape
    size = away.shape[1]
    per = (size - STAT_ROWS) // seqs
    tok_copy = pltpu.make_async_copy(tok_in, tok_ref, toksem)
    tok_copy.start()
    chips, core, chip, _, _, _, partner, _, _ = ring_place()
    near, far = chip + 1 - 2 * lax.rem(chip, 2), chips - 1 - chip
    first = (near * 2 + core, far * 2 + core)
    second = (first[1], first[0])
    sel = (lax.rem((chip + 1) // 2, 2), chip // 2)
    keep = [2 * c + sel[c] for c in range(2)]
    give = [2 * c + 1 - sel[c] for c in range(2)]
    arrived = enter((partner, first[0], first[1]))
    k_rows = wov.shape[1]

    def wo_copy(k):
        return pltpu.make_async_copy(wo_ref.at[pl.ds(pl.multiple_of(k * k_rows, k_rows), k_rows)], wov.at[k], wsem.at[k])

    other = (1 - core) * 4
    for k in [core * 4 + q for q in keep] + [other + q for q in keep] + [core * 4 + q for q in give] + [other + q for q in give]:
        wo_copy(k).start()
    arrived()
    sent = []

    def push(src, dst, ss, rs, peer):
        sent.append(send(src, dst, ss, rs, peer))
        return sent[-1]

    def block_of(k):
        return mine.at[pl.ds(pl.multiple_of(k * size, 8), size)]

    def piece_of(ref, i):
        return ref.at[pl.ds(STAT_ROWS + i * seqs, seqs)] if i else ref.at[pl.ds(0, STAT_ROWS + seqs)]

    def trade(q, slot, i):
        return push(piece_of(block_of((1 - core) * 4 + q), i), piece_of(pin.at[slot], i), s0.at[slot, i], r0.at[slot, i], partner)

    pair = [[trade(give[c], c, i) for c in range(2)] for i in range(per)]
    pair_keep = [[trade(keep[c], 2 + c, i) for c in range(2)] for i in range(per)]

    def stat(ref):
        return ref[0:STAT_ROWS, :]

    def blend(refs, factors, h):
        rows = slice(STAT_ROWS + h * seqs, STAT_ROWS + (h + 1) * seqs)
        return functools.reduce(jnp.add, [ref[rows, :] * f[:, h:h + 1] for ref, f in zip(refs, factors)])

    def exchange(sources, out, waits, dst, ss, rs, peers):
        started, factors = [[], []], [None, None]
        for i in range(per):
            for c in range(2):
                for copy in waits(c, i):
                    copy.wait_recv()
            for c in range(2):
                if i == 0:
                    factors[c], peak, total = weigh([stat(ref) for ref in sources[c]], seqs)
                    out[c, 0:STAT_ROWS, :] = stat_tile(peak, total)
                out[c, STAT_ROWS + i * seqs:STAT_ROWS + (i + 1) * seqs, :] = blend(sources[c], factors[c], i)
            for c in range(2):
                started[c].append(push(piece_of(out.at[c], i), piece_of(dst.at[c], i), ss.at[c, i], rs.at[c, i], peers[c]))
        return started

    step1 = exchange([[block_of(core * 4 + give[c]), pin.at[c]] for c in range(2)], away,
                     lambda c, i: (pair[i][c],), in1, s1, r1, first)
    step2 = exchange([[block_of(core * 4 + keep[c]), pin.at[2 + c], in1.at[c]] for c in range(2)], out2,
                     lambda c, i: (pair_keep[i][c], step1[c][i]), in2, s2, r2, second)
    step3, own, factors = [[], []], [[], []], [None, None]
    blocks = [core * 4 + keep[c] for c in range(2)]

    def rows_of(k, i):
        return att.at[k, pl.ds(i * seqs, seqs)]

    for i in range(per):
        for c in range(2):
            step2[c][i].wait_recv()
        for c in range(2):
            refs = [out2.at[c], in2.at[c]]
            if i == 0:
                weights, _, total = weigh([stat(ref) for ref in refs], seqs)
                factors[c] = [f / total for f in weights]
            att[blocks[c], i * seqs:(i + 1) * seqs, :] = blend(refs, factors[c], i).astype(jnp.bfloat16).astype(jnp.float32)
        for c in range(2):
            piece = rows_of(blocks[c], i)
            step3[c].append(push(piece, piece, s3.at[c, i], r3.at[c, i], first[c]))
        for c in range(2):
            piece = rows_of(blocks[c], i)
            own[c].append(push(piece, piece, s4.at[c, i], r4.at[c, i], partner))

    cols = 512

    def multiply(k, fresh=False):
        wo_copy(k).wait()
        lhs = jnp.concatenate([att[k, i * seqs:(i + 1) * seqs, :] for i in range(per)], axis=1).astype(jnp.bfloat16)
        for i in range(model // cols):
            off = slice(i * cols, (i + 1) * cols)
            y = jnp.dot(lhs, wov[k, :, off], preferred_element_type=jnp.float32)
            res[:, off] = y if fresh else res[:, off] + y

    def multiply_pair(base, i, last=False):
        ks = [base + give[c] for c in range(2)]
        if i == 0:
            for k in ks:
                wo_copy(k).wait()
        part = slice(i * seqs, (i + 1) * seqs)
        depth = slice(i * (k_rows // per), (i + 1) * (k_rows // per))
        lhs = jnp.concatenate([att[k, part, :] for k in ks], axis=1).astype(jnp.bfloat16)
        for j in range(model // cols):
            off = slice(j * cols, (j + 1) * cols)
            rhs = jnp.concatenate([wov[k, depth, off] for k in ks], axis=0)
            y = res[:, off] + jnp.dot(lhs, rhs, preferred_element_type=jnp.float32)
            if last:
                out_ref[:, off] = (tok_ref[:, off].astype(jnp.float32) + y).astype(jnp.bfloat16)
            else:
                res[:, off] = y

    multiply(blocks[0], fresh=True)
    multiply(blocks[1])
    for c in range(2):
        for i in range(per):
            own[c][i].wait_recv()
        multiply(other + keep[c])
    tok_copy.wait()
    passed = []
    for i in range(per):
        for c in range(2):
            step3[c][i].wait_recv()
            piece = rows_of(core * 4 + give[c], i)
            passed.append(push(piece, piece, s5.at[c, i], r5.at[c, i], partner))
        multiply_pair(core * 4, i)
        if i > 0:
            for copy in passed[2 * i - 2:2 * i]:
                copy.wait_recv()
            multiply_pair(other, i - 1)
    for copy in passed[2 * per - 2:]:
        copy.wait_recv()
    multiply_pair(other, per - 1, last=True)
    for copy in sent:
        copy.wait_send()


def tail_stage(part, w_o, tokens, group):
    seqs, model = tokens.shape
    head_dim = part.shape[-1]
    rows = part.shape[0] // group
    per = (rows - STAT_ROWS) // seqs
    vmem = pl.BlockSpec(memory_space=pltpu.VMEM)
    hbm = pl.BlockSpec(memory_space=pltpu.HBM)
    dma = pltpu.SemaphoreType.DMA
    sums = pltpu.VMEM((2, rows, head_dim), jnp.float32)
    return pl.pallas_call(
        tail_kernel,
        name='tail_stage',
        out_shape=pltpu.VMEM((seqs, model), jnp.bfloat16),
        in_specs=[vmem, hbm, hbm],
        out_specs=vmem,
        scratch_shapes=[
            pltpu.VMEM((seqs, model), tokens.dtype),
            dma,
            pltpu.VMEM((4, rows, head_dim), jnp.float32),
            sums, sums, sums, sums,
            pltpu.VMEM((group, per * seqs, head_dim), jnp.float32),
            pltpu.VMEM((group, w_o.shape[0] // group, model), jnp.bfloat16),
            pltpu.VMEM((seqs, model), jnp.float32),
            dma((group,)), dma((4, per)), dma((4, per)),
        ] + [dma((2, per))] * 10,
        compiler_params=pltpu.CompilerParams(collective_id=0, has_side_effects=True, vmem_limit_bytes=44 * 1024 * 1024),
    )(part, *in_hbm(w_o, tokens))


def solution(mesh):
    cache_spec = P('dp', 'sp', None, None)
    group = mesh.shape['sp']

    def device_step(tokens, positions, k_cache, v_cache, w_q, w_k, w_v, w_o, attn_norm, q_norm, k_norm):
        shared = project_stage(tokens, positions, k_cache, v_cache, w_q, w_k, w_v, attn_norm, q_norm, k_norm, group)
        k_upd, v_upd, new_kv, part = attend_stage(positions, *shared)
        block_out = tail_stage(part, w_o, tokens, group)
        return block_out, k_upd, v_upd, new_kv

    return jax.shard_map(device_step, mesh=mesh, in_specs=(P('dp', None), P('dp'), cache_spec, cache_spec, P(), P(), P(), P(), P(), P(), P()), out_specs=(P('dp', None), cache_spec, cache_spec, P('dp', None, None, None)), check_vma=False)
```

```python
import functools

import jax
import jax.numpy as jnp
import numpy as np
from jax import lax
from jax.experimental import pallas as pl
from jax.experimental.pallas import tpu as pltpu
from jax.sharding import PartitionSpec as P

NORM_EPS = 1e-6
ROPE_THETA = 1000000.0
NEG_FILL = -1e30
MESH = pl.DeviceIdType.MESH
STAT_ROWS = 8


def in_hbm(*arrays):
    return [pltpu.with_memory_space_constraint(jnp.asarray(a), pltpu.HBM) for a in arrays]


def rope_frequencies(head_dim):
    inv_freq = ROPE_THETA ** (-np.arange(head_dim // 2, dtype=np.float64) * 2.0 / head_dim)
    return np.concatenate([inv_freq, inv_freq])[None, :].astype(np.float32)


def norm_rope(proj, gain, cos_full, sin_full):
    values = proj.astype(jnp.bfloat16).astype(jnp.float32)
    scale = lax.rsqrt(jnp.mean(values * values, axis=-1, keepdims=True) + NORM_EPS)
    normed = values * scale * gain
    turned = pltpu.roll(normed, normed.shape[-1] // 2, 1)
    return (normed * cos_full + turned * sin_full).astype(jnp.bfloat16).astype(jnp.float32)


def ring_place():
    me = lax.axis_index('sp')
    chips = lax.axis_size('sp') // 2
    core, chip = lax.rem(me, 2), me // 2
    c_right, c_left, c_opp = lax.rem(chip + 1, chips), lax.rem(chip + chips - 1, chips), lax.rem(chip + 2, chips)
    return chips, core, chip, c_right, c_left, c_opp, chip * 2 + 1 - core, c_right * 2 + core, c_left * 2 + core


def enter(peers):
    barrier = pltpu.get_barrier_semaphore()
    for peer in peers:
        pl.semaphore_signal(barrier, inc=1, device_id={'sp': peer}, device_id_type=MESH)
    return lambda: pl.semaphore_wait(barrier, len(peers))


def send(src, dst, ss, rs, peer):
    copy = pltpu.make_async_remote_copy(src_ref=src, dst_ref=dst, send_sem=ss, recv_sem=rs,
                                        device_id={'sp': peer}, device_id_type=MESH)
    copy.start()
    return copy


def project_kernel(pos_in, tok_in, freq_in, an_in, qn_in, kn_in, wq_ref, wk_ref, wv_ref, kc_ref, vc_ref,
                   qf, kf, vf, kbuf, vbuf,
                   pos_ref, tok_ref, freq_ref, an_ref, qn_ref, kn_ref, hid, wbuf, cosb, sinb, insem, wsem, csem, ss, rs):
    seqs, model = tok_ref.shape
    head_dim = qn_ref.shape[-1]
    blocks, _, blk = hid.shape
    width = wbuf.shape[-1]
    heads = width // head_dim
    chips, core, chip, c_right, c_left, c_opp, partner, right, left = ring_place()
    mine_k = core * chips + chip

    smalls = [pltpu.make_async_copy(src, dst, insem.at[j]) for j, (src, dst) in enumerate((
        (tok_in, tok_ref), (pos_in, pos_ref), (freq_in, freq_ref), (an_in, an_ref), (qn_in, qn_ref), (kn_in, kn_ref)))]
    for copy in smalls:
        copy.start()
    bulk = []
    k_left, k_right, k_opp = core * chips + c_left, core * chips + c_right, core * chips + c_opp
    for j, (ref, col) in enumerate(((wq_ref, mine_k), (wq_ref, k_opp), (wk_ref, core), (wv_ref, core))):
        for i in range(blocks):
            src = ref.at[pl.ds(i * blk, blk), pl.ds(pl.multiple_of(col * width, width), width)]
            bulk.append(pltpu.make_async_copy(src, wbuf.at[j, i], wsem.at[j, i]))
    pieces = csem.shape[1]
    per = seqs // pieces
    for g in range(pieces):
        for j, (ref, buf) in enumerate(((kc_ref, kbuf), (vc_ref, vbuf))):
            rows = pl.ds(g * per, per)
            bulk.append(pltpu.make_async_copy(ref.at[rows], buf.at[rows], csem.at[j, g]))
    issued = 0

    def issue(count):
        nonlocal issued
        for copy in bulk[issued:issued + count]:
            copy.start()
        issued += count

    issue(8)
    arrived = enter((partner, right, left))
    for copy in smalls:
        copy.wait()

    lanes = an_ref.shape[1]
    total = jnp.zeros((seqs, lanes), jnp.float32)
    for i in range(model // lanes):
        xf = tok_ref[:, i * lanes:(i + 1) * lanes].astype(jnp.float32)
        total = total + xf * xf
    inv = lax.rsqrt(jnp.sum(total, axis=-1, keepdims=True) / model + NORM_EPS)
    per_blk = blk // lanes
    for i in range(model // lanes):
        xf = tok_ref[:, i * lanes:(i + 1) * lanes].astype(jnp.float32)
        gain = an_ref[i:i + 1, :].astype(jnp.float32)
        hid[i // per_blk, :, (i % per_blk) * lanes:(i % per_blk + 1) * lanes] = (xf * inv * gain).astype(jnp.bfloat16)

    for b in range(seqs):
        cosb[b:b + 1, :] = jnp.full((1, head_dim), pos_ref[b], jnp.int32).astype(jnp.float32)
    angles = cosb[...] * freq_ref[...]
    sign = jnp.where(lax.broadcasted_iota(jnp.int32, angles.shape, 1) < head_dim // 2, -1.0, 1.0)
    sinb[...] = jnp.sin(angles) * sign
    cosb[...] = jnp.cos(angles)
    cos_full, sin_full = cosb[...], sinb[...]

    def project(j, more):
        y = None
        for i in range(blocks):
            bulk[j * blocks + i].wait()
            issue(more)
            part = jnp.dot(hid[i], wbuf[j, i], preferred_element_type=jnp.float32)
            y = part if y is None else y + part
        return [y[:, h * head_dim:(h + 1) * head_dim] for h in range(heads)]

    def put(dst, base, values):
        for h, value in enumerate(values):
            dst[pl.ds(pl.multiple_of(base + h * seqs, seqs), seqs), :] = value

    half_rows = heads // 2 * seqs

    def q_half(k, h):
        return qf.at[pl.ds(pl.multiple_of(k * heads * seqs + h * half_rows, half_rows), half_rows)]

    q_gain = qn_ref[...].astype(jnp.float32)
    put(qf, mine_k * heads * seqs, [norm_rope(p, q_gain, cos_full, sin_full) for p in project(0, 2)])
    arrived()
    count = 0
    sent = []

    def push(ref, peer):
        nonlocal count
        sent.append(send(ref, ref, ss.at[count], rs.at[count], peer))
        count += 1
        return sent[-1]

    own = [[push(q_half(mine_k, h), peer) for peer in (right, left)] for h in range(2)]
    push(q_half(mine_k, 0), partner)
    push(q_half(mine_k, 1), partner)
    put(qf, k_opp * heads * seqs, [norm_rope(p, q_gain, cos_full, sin_full) for p in project(1, 4)])
    push(q_half(k_opp, 0), partner)
    push(q_half(k_opp, 1), partner)

    kv_rows = heads * seqs
    kv_base = core * kv_rows
    kv_part = pl.ds(pl.multiple_of(kv_base, kv_rows), kv_rows)
    k_gain = kn_ref[...].astype(jnp.float32)
    put(kf, kv_base, [norm_rope(p, k_gain, cos_full, sin_full) for p in project(2, 2)])
    push(kf.at[kv_part], partner)
    put(vf, kv_base, [p.astype(jnp.bfloat16).astype(jnp.float32) for p in project(3, 2)])
    push(vf.at[kv_part], partner)
    issue(len(bulk) - issued)

    for h in range(2):
        for from_peer, k in zip(own[h], (k_left, k_right)):
            from_peer.wait_recv()
            push(q_half(k, h), partner)
    waited = own[0] + own[1]
    for copy in sent:
        if not any(copy is w for w in waited):
            copy.wait_recv()
        copy.wait_send()
    for copy in bulk[4 * blocks:]:
        copy.wait()


def project_stage(tokens, positions, k_cache, v_cache, w_q, w_k, w_v, attn_norm, q_norm, k_norm, group):
    seqs, model = tokens.shape
    kv_heads, head_dim = k_cache.shape[2:]
    q_heads = w_q.shape[1] // head_dim
    width = w_q.shape[1] // group
    blocks = 4
    vmem = pl.BlockSpec(memory_space=pltpu.VMEM)
    hbm = pl.BlockSpec(memory_space=pltpu.HBM)
    dma = pltpu.SemaphoreType.DMA
    return pl.pallas_call(
        project_kernel,
        name='project_stage',
        out_shape=(
            pltpu.VMEM((q_heads * seqs, head_dim), jnp.float32),
            pltpu.VMEM((kv_heads * seqs, head_dim), jnp.float32),
            pltpu.VMEM((kv_heads * seqs, head_dim), jnp.float32),
            pltpu.VMEM(k_cache.shape, k_cache.dtype),
            pltpu.VMEM(v_cache.shape, v_cache.dtype),
        ),
        in_specs=[hbm] * 11,
        out_specs=(vmem,) * 5,
        scratch_shapes=[
            pltpu.SMEM(positions.shape, jnp.int32),
            pltpu.VMEM(tokens.shape, tokens.dtype),
            pltpu.VMEM((1, head_dim), jnp.float32),
            pltpu.VMEM((model // 128, 128), attn_norm.dtype),
            pltpu.VMEM((1, head_dim), q_norm.dtype),
            pltpu.VMEM((1, head_dim), k_norm.dtype),
            pltpu.VMEM((blocks, seqs, model // blocks), jnp.bfloat16),
            pltpu.VMEM((4, blocks, model // blocks, width), jnp.bfloat16),
            pltpu.VMEM((seqs, head_dim), jnp.float32),
            pltpu.VMEM((seqs, head_dim), jnp.float32),
            dma((6,)), dma((4, blocks)), dma((2, 8)), dma((16,)), dma((16,)),
        ],
        compiler_params=pltpu.CompilerParams(collective_id=1, has_side_effects=True, vmem_limit_bytes=24 * 1024 * 1024),
    )(*in_hbm(positions, tokens, rope_frequencies(head_dim), attn_norm.reshape(-1, 128), q_norm[None, :], k_norm[None, :],
              w_q, w_k, w_v, k_cache, v_cache))


def attend_kernel(pos_in, qf, kf, vf, k_in, v_in, ko_ref, vo_ref, new_out, part_ref, kbuf, vbuf,
                  pos_ref, new_ref, mstat, lstat, sbuf, ebuf, possem, newsem, kosem, vosem):
    seqs, slots, kv_heads, head_dim = kbuf.shape
    groups = kosem.shape[0]
    per_group = seqs // groups
    q_heads = qf.shape[0] // seqs
    start = lax.axis_index('sp') * slots
    pos_copy = pltpu.make_async_copy(pos_in, pos_ref, possem)
    pos_copy.start()
    pos_copy.wait()

    def write_step(g, carry):
        for bb in range(per_group):
            b = g * per_group + bb
            local = pos_ref[b] - start
            here = (local >= 0) & (local < slots)
            at = jnp.clip(local, 0, slots - 1)
            k_new = kf[pl.ds(b, kv_heads, stride=seqs), :]
            v_new = vf[pl.ds(b, kv_heads, stride=seqs), :]
            new_ref[b, 0] = k_new.astype(jnp.bfloat16)
            new_ref[b, 1] = v_new.astype(jnp.bfloat16)
            kbuf[b, at] = jnp.where(here, k_new, kbuf[b, at].astype(jnp.float32)).astype(jnp.bfloat16)
            vbuf[b, at] = jnp.where(here, v_new, vbuf[b, at].astype(jnp.float32)).astype(jnp.bfloat16)
        for copy in writes(g):
            copy.start()
        return carry

    def writes(g):
        rows = pl.ds(g * per_group, per_group)
        return (pltpu.make_async_copy(kbuf.at[rows], ko_ref.at[rows], kosem.at[g]),
                pltpu.make_async_copy(vbuf.at[rows], vo_ref.at[rows], vosem.at[g]),
                pltpu.make_async_copy(new_ref.at[rows], new_out.at[rows], newsem.at[g]))

    lax.fori_loop(0, groups, write_step, 0)

    cols = slots * kv_heads
    row_id = lax.broadcasted_iota(jnp.int32, (q_heads, cols), 0)
    col_id = lax.broadcasted_iota(jnp.int32, (q_heads, cols), 1)
    head_ok = row_id % kv_heads == col_id % kv_heads
    q_per = q_heads // kv_heads
    block_rows = STAT_ROWS + q_per * seqs
    slot_key = jnp.where(head_ok, col_id // kv_heads, slots * 1024)
    lane = lax.broadcasted_iota(jnp.int32, (q_heads, 128), 1)
    score_scale = head_dim ** -0.5
    mstat[...] = jnp.zeros_like(mstat)
    lstat[...] = jnp.zeros_like(lstat)

    def group_step(g, carry):
        m_acc, l_acc = mstat[...], lstat[...]
        members = [g * per_group + bb for bb in range(per_group)]
        for bb, b in enumerate(members):
            q_b = jnp.concatenate([qf[pl.ds(b + j * seqs, kv_heads, stride=q_per * seqs), :] for j in range(q_per)], axis=0).astype(jnp.bfloat16)
            k_b = kbuf[b].reshape(cols, head_dim)
            sbuf[bb] = lax.dot_general(q_b, k_b, (((1,), (1,)), ((), ())), preferred_element_type=jnp.float32)
        for bb, b in enumerate(members):
            live = slot_key <= pos_ref[b] - start
            s = jnp.where(live, sbuf[bb] * score_scale, NEG_FILL)
            m = jnp.max(s, axis=-1, keepdims=True)
            e = jnp.where(live, jnp.exp(s - m), 0.0)
            l = jnp.sum(e, axis=-1, keepdims=True)
            ebuf[bb] = e.astype(jnp.bfloat16)
            m_acc = jnp.where(lane == b, m, m_acc)
            l_acc = jnp.where(lane == b, l, l_acc)
        for bb, b in enumerate(members):
            o = jnp.dot(ebuf[bb], vbuf[b].reshape(cols, head_dim), preferred_element_type=jnp.float32)
            for j in range(q_per):
                part_ref[pl.ds(b + STAT_ROWS + j * seqs, kv_heads, stride=block_rows), :] = o[j * kv_heads:(j + 1) * kv_heads, :]
        mstat[...] = m_acc
        lstat[...] = l_acc
        return carry

    lax.fori_loop(0, groups, group_step, 0)

    for k in range(kv_heads):
        for j in range(q_per):
            row = k * block_rows + j
            part_ref[row:row + 1, :] = mstat[j * kv_heads + k:j * kv_heads + k + 1, :]
            part_ref[row + q_per:row + q_per + 1, :] = lstat[j * kv_heads + k:j * kv_heads + k + 1, :]
    for g in range(groups):
        for copy in writes(g):
            copy.wait()


def attend_stage(positions, qf, kf, vf, k_vm, v_vm):
    seqs, slots, kv_heads, head_dim = k_vm.shape
    q_heads = qf.shape[0] // seqs
    groups = 4
    vmem = pl.BlockSpec(memory_space=pltpu.VMEM)
    anyspec = pl.BlockSpec(memory_space=pl.ANY)
    hbm = pl.BlockSpec(memory_space=pltpu.HBM)
    dma = pltpu.SemaphoreType.DMA
    outs = pl.pallas_call(
        attend_kernel,
        name='attend_stage',
        out_shape=(
            jax.ShapeDtypeStruct(k_vm.shape, k_vm.dtype),
            jax.ShapeDtypeStruct(v_vm.shape, v_vm.dtype),
            jax.ShapeDtypeStruct((seqs, 2, kv_heads, head_dim), jnp.bfloat16),
            pltpu.VMEM((kv_heads * STAT_ROWS + q_heads * seqs, head_dim), jnp.float32),
            pltpu.VMEM(k_vm.shape, k_vm.dtype),
            pltpu.VMEM(v_vm.shape, v_vm.dtype),
        ),
        in_specs=[hbm] + [vmem] * 5,
        out_specs=(anyspec, anyspec, anyspec, vmem, vmem, vmem),
        input_output_aliases={4: 4, 5: 5},
        scratch_shapes=[
            pltpu.SMEM(positions.shape, jnp.int32),
            pltpu.VMEM((seqs, 2, kv_heads, head_dim), jnp.bfloat16),
            pltpu.VMEM((q_heads, 128), jnp.float32),
            pltpu.VMEM((q_heads, 128), jnp.float32),
            pltpu.VMEM((seqs // groups, q_heads, slots * kv_heads), jnp.float32),
            pltpu.VMEM((seqs // groups, q_heads, slots * kv_heads), jnp.bfloat16),
            dma, dma((groups,)), dma((groups,)), dma((groups,)),
        ],
        compiler_params=pltpu.CompilerParams(vmem_limit_bytes=16 * 1024 * 1024),
    )(*in_hbm(positions), qf, kf, vf, k_vm, v_vm)
    return outs[:4]


def weigh(tiles, seqs):
    per = STAT_ROWS // 2
    stats = [jnp.transpose(tile, (1, 0))[:seqs] for tile in tiles]
    peak = functools.reduce(jnp.maximum, [t[:, :per] for t in stats])
    factors = [jnp.exp(t[:, :per] - peak) for t in stats]
    return factors, peak, functools.reduce(jnp.add, [f * t[:, per:] for f, t in zip(factors, stats)])


def stat_tile(peak, total):
    both = jnp.concatenate([peak, total], axis=1)
    both = jnp.concatenate([both, jnp.zeros((128 - both.shape[0], STAT_ROWS), jnp.float32)], axis=0)
    return jnp.transpose(both, (1, 0))


def tail_kernel(mine, wo_ref, tok_in, out_ref, tok_ref, toksem, pin, away, in1, out2, in2, att, wov, res,
                wsem, s0, r0, s1, r1, s2, r2, s3, r3, s4, r4, s5, r5):
    seqs, model = tok_ref.shape
    size = away.shape[1]
    per = (size - STAT_ROWS) // seqs
    tok_copy = pltpu.make_async_copy(tok_in, tok_ref, toksem)
    tok_copy.start()
    chips, core, chip, _, _, _, partner, _, _ = ring_place()
    near, far = chip + 1 - 2 * lax.rem(chip, 2), chips - 1 - chip
    first = (near * 2 + core, far * 2 + core)
    second = (first[1], first[0])
    sel = (lax.rem((chip + 1) // 2, 2), chip // 2)
    keep = [2 * c + sel[c] for c in range(2)]
    give = [2 * c + 1 - sel[c] for c in range(2)]
    arrived = enter((partner, first[0], first[1]))
    k_rows = wov.shape[1]

    def wo_copy(k):
        return pltpu.make_async_copy(wo_ref.at[pl.ds(pl.multiple_of(k * k_rows, k_rows), k_rows)], wov.at[k], wsem.at[k])

    other = (1 - core) * 4
    for k in [core * 4 + q for q in keep] + [other + q for q in keep] + [core * 4 + q for q in give] + [other + q for q in give]:
        wo_copy(k).start()
    arrived()
    sent = []

    def push(src, dst, ss, rs, peer):
        sent.append(send(src, dst, ss, rs, peer))
        return sent[-1]

    def block_of(k):
        return mine.at[pl.ds(pl.multiple_of(k * size, 8), size)]

    def piece_of(ref, i):
        return ref.at[pl.ds(STAT_ROWS + i * seqs, seqs)] if i else ref.at[pl.ds(0, STAT_ROWS + seqs)]

    def trade(q, slot, i):
        return push(piece_of(block_of((1 - core) * 4 + q), i), piece_of(pin.at[slot], i), s0.at[slot, i], r0.at[slot, i], partner)

    pair = [[trade(give[c], c, i) for c in range(2)] for i in range(per)]
    pair_keep = [[trade(keep[c], 2 + c, i) for c in range(2)] for i in range(per)]

    part_rows = seqs // 2

    def bit_of(ref, i):
        return ref.at[pl.ds(STAT_ROWS + i * part_rows, part_rows)] if i else ref.at[pl.ds(0, STAT_ROWS + part_rows)]

    def stat(ref):
        return ref[0:STAT_ROWS, :]

    def blend(refs, factors, i):
        rows = slice(STAT_ROWS + i * part_rows, STAT_ROWS + (i + 1) * part_rows)
        seq = slice(i % 2 * part_rows, (i % 2 + 1) * part_rows)
        return functools.reduce(jnp.add, [ref[rows, :] * f[seq, i // 2:i // 2 + 1] for ref, f in zip(refs, factors)])

    def exchange(sources, out, waits, dst, ss, rs, peers):
        started, factors = [[], []], [None, None]
        for i in range(2 * per):
            for c in range(2):
                for copy in waits(c, i):
                    copy.wait_recv()
            for c in range(2):
                if i == 0:
                    factors[c], peak, total = weigh([stat(ref) for ref in sources[c]], seqs)
                    out[c, 0:STAT_ROWS, :] = stat_tile(peak, total)
                out[c, STAT_ROWS + i * part_rows:STAT_ROWS + (i + 1) * part_rows, :] = blend(sources[c], factors[c], i)
            for c in range(2):
                started[c].append(push(bit_of(out.at[c], i), bit_of(dst.at[c], i), ss.at[c, i], rs.at[c, i], peers[c]))
        return started

    step1 = exchange([[block_of(core * 4 + give[c]), pin.at[c]] for c in range(2)], away,
                     lambda c, i: () if i % 2 else (pair[i // 2][c],), in1, s1, r1, first)
    step2 = exchange([[block_of(core * 4 + keep[c]), pin.at[2 + c], in1.at[c]] for c in range(2)], out2,
                     lambda c, i: (step1[c][i],) if i % 2 else (pair_keep[i // 2][c], step1[c][i]), in2, s2, r2, second)
    step3, own, factors = [[], []], [[], []], [None, None]
    blocks = [core * 4 + keep[c] for c in range(2)]

    def rows_of(k, i):
        return att.at[k, pl.ds(i * seqs, seqs)]

    for i in range(2 * per):
        for c in range(2):
            step2[c][i].wait_recv()
        rows = slice(i * part_rows, (i + 1) * part_rows)
        for c in range(2):
            refs = [out2.at[c], in2.at[c]]
            if i == 0:
                weights, _, total = weigh([stat(ref) for ref in refs], seqs)
                factors[c] = [f / total for f in weights]
            att[blocks[c], rows, :] = blend(refs, factors[c], i).astype(jnp.bfloat16).astype(jnp.float32)
        for c in range(2):
            piece = att.at[blocks[c], pl.ds(i * part_rows, part_rows)]
            step3[c].append(push(piece, piece, s3.at[c, i], r3.at[c, i], first[c]))
        if i % 2:
            for c in range(2):
                piece = rows_of(blocks[c], i // 2)
                own[c].append(push(piece, piece, s4.at[c, i // 2], r4.at[c, i // 2], partner))

    cols = 512

    def multiply(k, fresh=False):
        wo_copy(k).wait()
        lhs = jnp.concatenate([att[k, i * seqs:(i + 1) * seqs, :] for i in range(per)], axis=1).astype(jnp.bfloat16)
        for i in range(model // cols):
            off = slice(i * cols, (i + 1) * cols)
            y = jnp.dot(lhs, wov[k, :, off], preferred_element_type=jnp.float32)
            res[:, off] = y if fresh else res[:, off] + y

    def multiply_pair(base, i, last=False):
        ks = [base + give[c] for c in range(2)]
        if i == 0:
            for k in ks:
                wo_copy(k).wait()
        part = slice(i * seqs, (i + 1) * seqs)
        depth = slice(i * (k_rows // per), (i + 1) * (k_rows // per))
        lhs = jnp.concatenate([att[k, part, :] for k in ks], axis=1).astype(jnp.bfloat16)
        for j in range(model // cols):
            off = slice(j * cols, (j + 1) * cols)
            rhs = jnp.concatenate([wov[k, depth, off] for k in ks], axis=0)
            y = res[:, off] + jnp.dot(lhs, rhs, preferred_element_type=jnp.float32)
            if last:
                out_ref[:, off] = (tok_ref[:, off].astype(jnp.float32) + y).astype(jnp.bfloat16)
            else:
                res[:, off] = y

    multiply(blocks[0], fresh=True)
    multiply(blocks[1])
    for c in range(2):
        for i in range(per):
            own[c][i].wait_recv()
        multiply(other + keep[c])
    tok_copy.wait()
    passed = []
    for i in range(per):
        for c in range(2):
            step3[c][2 * i].wait_recv()
            step3[c][2 * i + 1].wait_recv()
            piece = rows_of(core * 4 + give[c], i)
            passed.append(push(piece, piece, s5.at[c, i], r5.at[c, i], partner))
        multiply_pair(core * 4, i)
        if i > 0:
            for copy in passed[2 * i - 2:2 * i]:
                copy.wait_recv()
            multiply_pair(other, i - 1)
    for copy in passed[2 * per - 2:]:
        copy.wait_recv()
    multiply_pair(other, per - 1, last=True)
    for copy in sent:
        copy.wait_send()


def tail_stage(part, w_o, tokens, group):
    seqs, model = tokens.shape
    head_dim = part.shape[-1]
    rows = part.shape[0] // group
    per = (rows - STAT_ROWS) // seqs
    vmem = pl.BlockSpec(memory_space=pltpu.VMEM)
    hbm = pl.BlockSpec(memory_space=pltpu.HBM)
    dma = pltpu.SemaphoreType.DMA
    sums = pltpu.VMEM((2, rows, head_dim), jnp.float32)
    return pl.pallas_call(
        tail_kernel,
        name='tail_stage',
        out_shape=pltpu.VMEM((seqs, model), jnp.bfloat16),
        in_specs=[vmem, hbm, hbm],
        out_specs=vmem,
        scratch_shapes=[
            pltpu.VMEM((seqs, model), tokens.dtype),
            dma,
            pltpu.VMEM((4, rows, head_dim), jnp.float32),
            sums, sums, sums, sums,
            pltpu.VMEM((group, per * seqs, head_dim), jnp.float32),
            pltpu.VMEM((group, w_o.shape[0] // group, model), jnp.bfloat16),
            pltpu.VMEM((seqs, model), jnp.float32),
            dma((group,)), dma((4, per)), dma((4, per)),
        ] + [dma((2, 2 * per))] * 10,
        compiler_params=pltpu.CompilerParams(collective_id=0, has_side_effects=True, vmem_limit_bytes=44 * 1024 * 1024),
    )(part, *in_hbm(w_o, tokens))


def solution(mesh):
    cache_spec = P('dp', 'sp', None, None)
    group = mesh.shape['sp']

    def device_step(tokens, positions, k_cache, v_cache, w_q, w_k, w_v, w_o, attn_norm, q_norm, k_norm):
        shared = project_stage(tokens, positions, k_cache, v_cache, w_q, w_k, w_v, attn_norm, q_norm, k_norm, group)
        k_upd, v_upd, new_kv, part = attend_stage(positions, *shared)
        block_out = tail_stage(part, w_o, tokens, group)
        return block_out, k_upd, v_upd, new_kv

    return jax.shard_map(device_step, mesh=mesh, in_specs=(P('dp', None), P('dp'), cache_spec, cache_spec, P(), P(), P(), P(), P(), P(), P()), out_specs=(P('dp', None), cache_spec, cache_spec, P('dp', None, None, None)), check_vma=False)
```
